32 devices in a mesh: rows: 8 (over y, x, core), cols: 4 (over z).
Axes of the slice: x: 2, y: 2, z: 4, core: 2. Of those that a mesh axis runs over, the one named last changes fastest.
Arguments:
- fmap1: bfloat16 [2, 256, 256, 256], P(None, 'rows', 'cols'), may hold values from -6 to 6
- fmap2: bfloat16 [2, 256, 256, 256], P(None, 'rows', 'cols'), may hold values from -6 to 6
- target_owner: int32 [2, 2048, 1], P(None, ('rows', 'cols')), may hold values from 0 to 31; in each aligned block of 64 rows (0 to 63, 64 to 127, ..., all dimensions but the last counted through in order) at most 4 rows name the same one
- target_tile: int32 [2, 2048], P(None, ('rows', 'cols')), may hold values from 0 to 31
Outputs:
- corr: float32 [2, 81, 131072], P(None, None, ('rows', 'cols'))
The draws below stay inside these ranges and needn't reach their ends.
Inputs may be any that keep to these rules, and one draw needn't show every extreme that they name: `target_owner`: at each level, the 64 query blocks of one region (aligned blocks of rows) name any one owner at most 4 times, a bound that some block reaches. `target_tile`: tile of the owner's region in the query block's frame, numbered row-major; level l uses it modulo that level's tile count.
All inputs are finite; a program needn't handle non-finite values.
Results may differ from the reference program's by a relative error of at most 0.0013.
Values may be sent and summed in bfloat16 or wider, within the bound.
A program may use at most 128 MiB of HBM per device.

```python
import math
import jax
import jax.numpy as jnp
import numpy as np
from jax import lax

C = 256
RADIUS = 4
LEVELS = 2
BATCH = 2
QH = 32
QW = 64
H0 = 256
W0 = 256
TILES = 32
QB_DEV = 64
CAP = 4
QBLK = 2048
N_ROWS = 8
N_COLS = 4


def with_ends(entries, stream_key, low, high):
    place = [jax.random.randint(jax.random.fold_in(stream_key, axis), (), 0, length) for axis, length in enumerate(entries.shape)]
    longest = entries.shape.index(max(entries.shape))
    neighbour = place[:longest] + [(place[longest] + 1) % entries.shape[longest]] + place[longest + 1:]
    return entries.at[tuple(place)].set(low).at[tuple(neighbour)].set(high)


def block_scale(key, extent, shards, low, largest):
    loudness, own = 1.0, jax.random.fold_in(key, 6)
    for axis_at, parts in shards:
        steps = jnp.exp(jax.random.uniform(jax.random.fold_in(own, axis_at), (parts,), jnp.float32, low / len(shards), largest / len(shards)))
        loudness = loudness * jnp.repeat(steps, extent[axis_at] // parts).reshape([-1 if axis == axis_at else 1 for axis in range(len(extent))])
    return loudness


def routed_block(own_key, own, number, rows, amount, top, reach, skew):
    order = jax.random.permutation(own_key, amount)
    packed, common = portions_of(amount, rows * top, reach, skew, True), portions_of(amount, rows * top, reach, skew, False)
    places = jnp.arange(amount)

    def named(tallies, offset_by):
        used = int((tallies > 0).sum())
        fixed = max(1, used // 4)
        passed = fixed + (places - fixed + offset_by * (used - fixed)) % max(1, amount - fixed)
        return jnp.zeros((amount,), jnp.int32).at[order[jnp.where(places < fixed, places, passed)]].set(jnp.asarray(tallies, jnp.int32))

    tallies = jnp.where(number % 4 == 0, named(packed, number // 4), named(common, number - number // 4 - 1))
    mixed = jax.random.permutation(jax.random.fold_in(own, 3), amount)
    source_of, receiver = mixed[0:amount // 2 * 2:2], mixed[1:amount // 2 * 2:2]
    margin = jnp.minimum(tallies[source_of] - 1, reach - tallies[receiver]) // 2
    margin = jnp.where((source_of == order[0]) | (receiver == order[0]) | (tallies[receiver] == 0), 0, jnp.maximum(margin, 0))
    passed = jax.random.randint(jax.random.fold_in(own, 4), (amount // 2,), 0, 1 << 20) % (margin + 1)
    tallies = tallies.at[source_of].add(-passed).at[receiver].add(passed)
    members = jnp.searchsorted(jnp.cumsum(tallies), jnp.arange(rows * top), side="right").astype(jnp.int32)
    table = members.reshape(top, rows).T
    table = table[jax.random.permutation(jax.random.fold_in(own, 1), rows)]
    offset_by = jax.random.randint(jax.random.fold_in(own, 2), (rows, 1), 0, top)
    return jnp.take_along_axis(table, (jnp.arange(top)[None, :] + offset_by) % top, axis=1)


def portions_of(number_of, total, reach, skew, full):
    weights = [(1 << 20) // math.isqrt(standing ** skew) + 1 for standing in range(1, number_of + 1)]
    largest = reach if full else min(reach, max(-(-total // number_of), total * weights[0] // sum(weights)))
    least = 1 if total - largest >= number_of - 1 else 0
    holding, rest = [largest] + [least] * (number_of - 1), total - largest - least * (number_of - 1)
    while rest > 0:
        candidates = [i for i in range(1, number_of) if holding[i] < largest] or [i for i in range(1, number_of) if holding[i] < reach]
        whole, remaining = sum([weights[i] for i in candidates]), rest
        for i in candidates:
            extra = min(reach - holding[i], max(1, remaining * weights[i] // whole), rest)
            holding[i] = holding[i] + extra
            rest = rest - extra
    return np.array(holding)


def noise(key, shape, spread, most, shards=(), kind=jnp.bfloat16):
    array = jax.random.normal(key, shape, jnp.float32) * spread
    if len(shards) > 0:
        array = block_scale(key, shape, shards, -0.22, 0.18) * array
    return jnp.clip(array, min=-most, max=most).astype(kind)


def setup_inputs(seed: int = 0) -> dict:
    key_list = jax.random.split(jax.random.key(seed), 5)
    fmap1 = noise(key_list[0], (BATCH, H0, W0, C), 1.0, 6.0, ((1, 8), (2, 4)))
    fmap2 = noise(key_list[1], (BATCH, H0, W0, C), 1.0, 6.0, ((1, 8), (2, 4)))
    target_owner_keys = jax.random.split(jax.random.fold_in(key_list[2], 1), LEVELS * QBLK // QB_DEV)
    target_owner_turns = jax.random.permutation(jax.random.fold_in(key_list[2], 3), LEVELS * QBLK // QB_DEV)
    target_owner = jax.vmap(lambda own, number: routed_block(jax.random.fold_in(key_list[2], 2), own, number, QB_DEV, N_ROWS * N_COLS, 1, CAP, 2))(target_owner_keys, target_owner_turns).reshape((LEVELS, QBLK, 1))
    target_tile = with_ends(jax.random.randint(key_list[3], (LEVELS, QBLK), 0, TILES), jax.random.fold_in(key_list[3], 1), 0, TILES - 1).astype(jnp.int32)
    return dict(fmap1=fmap1, fmap2=fmap2, target_owner=target_owner, target_tile=target_tile)


def window_index():
    tile_side = 2 * RADIUS
    span_side = 4 * RADIUS
    window_side = 2 * RADIUS + 1
    query_ids = jnp.arange(tile_side * tile_side, dtype=jnp.int32)
    offset_ids = jnp.arange(window_side * window_side, dtype=jnp.int32)
    row_part = query_ids[:, None] // tile_side + offset_ids[None, :] // window_side
    col_part = query_ids[:, None] % tile_side + offset_ids[None, :] % window_side
    return row_part * span_side + col_part


def pool_level(level_map):
    frame_count, rows_in, cols_in, channels = level_map.shape
    pooled = level_map.astype(jnp.float32).reshape(frame_count, rows_in // 2, 2, cols_in // 2, 2, channels)
    return jnp.mean(pooled, axis=(2, 4)).astype(jnp.bfloat16)


def reference(fmap1, fmap2, target_owner, target_tile):
    tile_side = 2 * RADIUS
    span_side = 4 * RADIUS
    window_side = 2 * RADIUS + 1
    device_count = N_ROWS * N_COLS
    levels = [fmap2]
    for level in range(1, LEVELS):
        levels.append(pool_level(levels[-1]))
    padded = [jnp.pad(level_map, ((0, 0), (RADIUS, RADIUS), (RADIUS, RADIUS), (0, 0))) for level_map in levels]
    window_ids = window_index()
    tiles_across = QW // tile_side
    per_frame = (QH // tile_side) * tiles_across
    block_ids = jnp.arange(QB_DEV, dtype=jnp.int32)
    frame_ids = block_ids // per_frame
    block_rows = (block_ids % per_frame) // tiles_across * tile_side
    block_cols = block_ids % tiles_across * tile_side
    owner_table = target_owner[:, :, 0].reshape(LEVELS, device_count, QB_DEV)
    tile_table = target_tile.reshape(LEVELS, device_count, QB_DEV)
    gather_ids = jnp.broadcast_to(window_ids[None], (QB_DEV,) + window_ids.shape)

    def one_device(device):
        first_row = device // N_COLS * QH + block_rows
        first_col = device % N_COLS * QW + block_cols

        def query_block(frame_id, row_at, col_at):
            return lax.dynamic_slice(fmap1, (frame_id, row_at, col_at, 0 * frame_id), (1, tile_side, tile_side, C)).reshape(tile_side * tile_side, C)

        queries = jax.vmap(query_block)(frame_ids, first_row, first_col).astype(jnp.float32)
        results = []
        for level in range(LEVELS):
            level_rows = QH >> level
            level_cols = QW >> level
            level_across = level_cols // tile_side
            tile_count = (level_rows // tile_side) * level_across
            owner_ids = owner_table[level, device]
            tile_ids = tile_table[level, device] % tile_count
            target_rows = owner_ids // N_COLS * level_rows + tile_ids // level_across * tile_side
            target_cols = owner_ids % N_COLS * level_cols + tile_ids % level_across * tile_side

            def target_block(frame_id, row_at, col_at, source=padded[level]):
                return lax.dynamic_slice(source, (frame_id, row_at, col_at, 0 * frame_id), (1, span_side, span_side, C)).reshape(span_side * span_side, C)

            targets = jax.vmap(target_block)(frame_ids, target_rows, target_cols).astype(jnp.float32)
            scores = jnp.einsum("bqc,bpc->bqp", queries, targets, precision=lax.Precision.HIGHEST) * C ** -0.5
            results.append(jnp.take_along_axis(scores, gather_ids, axis=2))
        return jnp.stack(results)

    stacked = lax.map(one_device, jnp.arange(device_count, dtype=jnp.int32))
    return stacked.transpose(1, 4, 0, 2, 3).reshape(LEVELS, window_side * window_side, device_count * QB_DEV * tile_side * tile_side)
```

```python
import functools

import jax
import jax.numpy as jnp
from jax import lax
from jax.experimental import pallas as pl
from jax.experimental.pallas import tpu as pltpu
from jax.sharding import PartitionSpec as P

RADIUS = 4
LEVELS = 2
STEP_SLOTS = 16


def padded_2(block, sides, width):
    for axis, dim in sides:
        count = lax.axis_size(axis)
        forward = [(i, i + 1) for i in range(count - 1)]
        backward = [(target, source) for source, target in forward]
        low = lax.ppermute(
            lax.slice_in_dim(block, block.shape[dim] - width, None, axis=dim), axis, forward
        )
        high = lax.ppermute(lax.slice_in_dim(block, 0, width, axis=dim), axis, backward)
        block = jnp.concatenate([low, block, high], axis=dim)
    return block


def pool_level(level_map):
    frame_count, rows_in, cols_in, channels = level_map.shape
    pooled = level_map.astype(jnp.float32).reshape(
        frame_count, rows_in // 2, 2, cols_in // 2, 2, channels
    )
    return jnp.mean(pooled, axis=(2, 4)).astype(jnp.bfloat16)


def dispatch_kernel(slot_count, block_ref, query_ref, sent_ref):
    base = pl.program_id(0) * slot_count
    for slot in range(slot_count):
        sent_ref[slot] = query_ref[block_ref[base + slot]]


def correlate_kernel(plan, scale, label_ref, query_ref, map_ref, reply_ref):
    per_frame, col_count, padded_rows, across = plan
    tile_side = 2 * RADIUS
    span_side = 4 * RADIUS
    window_side = 2 * RADIUS + 1
    block_cells = tile_side * tile_side
    base = pl.program_id(0) * STEP_SLOTS
    lane = lax.broadcasted_iota(jnp.int32, (1, 1, 2 * block_cells), 2)
    query_row = lane % block_cells // tile_side
    query_col = lane[0] % tile_side
    is_first = lane[0] < block_cells

    def window(slot):
        label = label_ref[base + slot]
        tile = label % per_frame
        region = label // per_frame
        row = region // col_count * padded_rows + tile // across * tile_side
        col = (region % col_count * across + tile % across) * tile_side
        col = pl.multiple_of(col, tile_side)
        cells = map_ref[pl.ds(row, span_side), pl.ds(col, span_side), :]
        return cells.reshape(span_side * span_side, -1).astype(jnp.bfloat16)

    for pair in range(STEP_SLOTS // 2):
        queries = query_ref[2 * pair : 2 * pair + 2].reshape(2 * block_cells, -1)
        first, second = [
            lax.dot_general(
                window(2 * pair + half),
                queries,
                (((1,), (1,)), ((), ())),
                preferred_element_type=jnp.float32,
            )
            for half in range(2)
        ]
        scores = jnp.where(is_first, first, second)
        scores = scores.reshape(span_side, span_side, 2 * block_cells)
        for bit in (1, 2, 4):
            scores = jnp.where((query_row & bit) != 0, scores[bit:], scores[:-bit])
        flat = scores.reshape(window_side * span_side, 2 * block_cells)
        for bit in (1, 2, 4):
            moved = pltpu.roll(flat, flat.shape[0] - bit, 0)
            flat = jnp.where((query_col & bit) != 0, moved, flat)
        flat = flat * scale
        for a in range(window_side):
            at = (pair * window_side + a) * window_side
            reply_ref[at : at + window_side, :] = flat[
                a * span_side : a * span_side + window_side
            ]


def assemble_kernel(pair_count, source_ref, half_ref, *refs):
    reply_refs, out_ref = refs[:-1], refs[-1]
    window_cells, lanes = out_ref.shape[1], reply_refs[0].shape[1]
    is_first = lax.broadcasted_iota(jnp.int32, (window_cells, lanes), 1) < lanes // 2
    for level in range(LEVELS):

        def step(m, carry, level=level):
            at = 2 * (level * pair_count + m)
            picked = []
            for side in range(2):
                first_row = source_ref[at + side] * window_cells
                rows = reply_refs[level][pl.ds(first_row, window_cells), :]
                moved = pltpu.roll(rows, lanes // 2, 1)
                picked.append(jnp.where(half_ref[at + side] == side, rows, moved))
            spot = pl.ds(pl.multiple_of(m * lanes, lanes), lanes)
            out_ref[level, :, spot] = jnp.where(is_first, picked[0], picked[1])
            return carry

        lax.fori_loop(0, pair_count, step, 0)


def body(fmap1, fmap2, target_owner, target_tile):
    tile_side = 2 * RADIUS
    window_side = 2 * RADIUS + 1
    block_cells = tile_side * tile_side
    frame_count, band_rows, band_cols, channels = fmap1.shape
    row_count = lax.axis_size("rows")
    col_count = lax.axis_size("cols")
    device_count = row_count * col_count
    tiles_across = band_cols // tile_side
    per_frame = band_rows // tile_side * tiles_across
    block_count = frame_count * per_frame
    owner_slots = max(2, (2 * block_count + device_count - 1) // device_count)
    row_slots = -(-owner_slots * col_count // STEP_SLOTS) * STEP_SLOTS
    pair_slots = row_slots // 2
    queries = fmap1.reshape(
        frame_count, band_rows // tile_side, tile_side, tiles_across, tile_side, channels
    )
    queries = queries.transpose(0, 1, 3, 2, 4, 5).reshape(block_count, block_cells, channels)
    owner_ids = target_owner[:, :, 0]
    owner_rows = owner_ids // col_count
    peer_ids = jnp.arange(row_count, dtype=jnp.int32)
    owner_hits = (owner_rows[:, :, None] == peer_ids[None, None, :]).astype(jnp.int32)
    slot_rank = jnp.sum(owner_hits * (jnp.cumsum(owner_hits, axis=1) - 1), axis=2)
    block_ids = jnp.arange(block_count, dtype=jnp.int32)
    label_rows = []
    for level in range(LEVELS):
        tile_count = (band_rows >> level) // tile_side * ((band_cols >> level) // tile_side)
        regions = block_ids // per_frame * col_count + owner_ids[level] % col_count
        label_rows.append(regions * per_frame + target_tile[level] % tile_count)
    rank_ids = jnp.arange(row_slots, dtype=jnp.int32)
    rank_hits = (slot_rank[:, :, None] == rank_ids[None, None, :]).astype(jnp.int32)
    slot_hits = owner_hits[:, :, :, None] * rank_hits[:, :, None, :]

    def by_slot(values):
        table = jnp.sum(slot_hits * values[:, :, None, None], axis=1)
        return table.transpose(1, 0, 2)

    labels_sent = by_slot(jnp.stack(label_rows))
    blocks_sent = by_slot(jnp.broadcast_to(block_ids[None], owner_ids.shape))
    slot_block = (row_slots, block_cells, channels)
    slot_total = row_count * row_slots
    label_part = lax.all_to_all(labels_sent, "rows", split_axis=0, concat_axis=0, tiled=True)
    levels = [fmap2]
    for level in range(1, LEVELS):
        levels.append(pool_level(levels[-1]))
    window_cells = window_side * window_side
    step_block = (STEP_SLOTS, block_cells, channels)
    reply_block = (STEP_SLOTS // 2 * window_cells, 2 * block_cells)
    reply_tables = [None] * LEVELS
    earlier = None
    for level in reversed(range(LEVELS)):
        queries_sent = pl.pallas_call(
            functools.partial(dispatch_kernel, row_slots),
            out_shape=jax.ShapeDtypeStruct((slot_total,) + slot_block[1:], jnp.bfloat16),
            grid_spec=pltpu.PrefetchScalarGridSpec(
                num_scalar_prefetch=1,
                grid=(row_count,),
                in_specs=[pl.BlockSpec(queries.shape, lambda d, *_: (0, 0, 0))],
                out_specs=pl.BlockSpec(slot_block, lambda d, *_: (d, 0, 0)),
            ),
        )(blocks_sent[:, level].reshape(-1), queries)
        query_part = lax.all_to_all(
            queries_sent.reshape((row_count,) + slot_block),
            "rows",
            split_axis=0,
            concat_axis=0,
            tiled=True,
        )
        band = lax.all_gather(levels[level], "cols", axis=2, tiled=True)
        if earlier is not None:
            band = lax.optimization_barrier((band, earlier, query_part))[0]
        padded = padded_2(band, (("rows", 1),), RADIUS).astype(jnp.float32)
        padded = jnp.pad(padded, ((0, 0), (0, 0), (RADIUS, RADIUS), (0, 0)))
        level_map = padded.reshape((-1,) + padded.shape[2:])
        plan = (per_frame, col_count, padded.shape[1], levels[level].shape[2] // tile_side)
        replies = pl.pallas_call(
            functools.partial(correlate_kernel, plan, channels ** (-0.5)),
            out_shape=jax.ShapeDtypeStruct(
                (row_count * pair_slots * window_cells, 2 * block_cells), jnp.float32
            ),
            grid_spec=pltpu.PrefetchScalarGridSpec(
                num_scalar_prefetch=1,
                grid=(slot_total // STEP_SLOTS,),
                in_specs=[
                    pl.BlockSpec(step_block, lambda d, *_: (d, 0, 0)),
                    pl.BlockSpec(
                        level_map.shape, lambda d, *_: (0, 0, 0), pipeline_mode=pl.Buffered(1)
                    ),
                ],
                out_specs=pl.BlockSpec(reply_block, lambda d, *_: (d, 0)),
            ),
        )(
            label_part[:, level].reshape(-1),
            query_part.reshape((slot_total,) + slot_block[1:]),
            level_map,
        )
        returned = lax.all_to_all(
            replies.reshape(row_count, pair_slots * window_cells, 2 * block_cells),
            "rows",
            split_axis=0,
            concat_axis=0,
            tiled=True,
        )
        earlier = returned
        reply_tables[level] = returned.reshape(-1, 2 * block_cells)
    source_ids = owner_rows * pair_slots + slot_rank // 2
    return pl.pallas_call(
        functools.partial(assemble_kernel, block_count // 2),
        out_shape=jax.ShapeDtypeStruct(
            (LEVELS, window_cells, block_count * block_cells), jnp.float32
        ),
        in_specs=[
            pl.BlockSpec(memory_space=pltpu.SMEM),
            pl.BlockSpec(memory_space=pltpu.SMEM),
        ]
        + [pl.BlockSpec(memory_space=pltpu.VMEM)] * LEVELS,
        out_specs=pl.BlockSpec(memory_space=pltpu.VMEM),
    )(source_ids.reshape(-1), (slot_rank % 2).reshape(-1), *reply_tables)


MESH = pl.DeviceIdType.MESH


def flipped(index, bit):
    return index + bit - 2 * bit * (index // bit % 2)


def chosen(index, values):
    result = jnp.int32(values[0])
    for at in range(1, len(values)):
        result = jnp.where(index == at, values[at], result)
    return result


def plane_plan(count):
    order, done = [], []
    for here in range(count):
        need = [
            max(abs(near - here) for near in range(max(b - 1, 0), min(b + 2, count)))
            for b in range(count)
        ]
        ranked = sorted(range(count), key=lambda b: (need[b], abs(b - here)))
        order.append(ranked)
        done.append([sum(n <= step for n in need) for step in range(count)])
    return order, done


def lookup_kernel(
    plan,
    f2_hbm,
    q_hbm,
    tab_hbm,
    rep_out,
    f2x,
    f1a,
    tabv,
    tabs,
    map0,
    map1,
    p1x,
    tmp,
    reps,
    loc_sem,
    zs_sem,
    zr_sem,
    hs_sem,
    hr_sem,
    fs_sem,
    fr_sem,
    ts_sem,
    tr_sem,
    tl_sem,
    rs_sem,
    rr_sem,
):
    row_count, plane_count, slots, scale = plan
    frame_count, band_rows, band_cols, channels = f2_hbm.shape
    block_count, block_cells, _ = q_hbm.shape
    side = 2 * RADIUS
    span = 4 * RADIUS
    wside = 2 * RADIUS + 1
    subs = band_rows // side
    across = band_cols // side
    half_blocks = block_count // 2
    r = lax.axis_index("rows")
    c = lax.axis_index("cols")
    last_r, last_c = row_count - 1, plane_count - 1
    order, done = plane_plan(plane_count)
    sub_order = [0, subs - 1] + list(range(1, subs - 1))

    barrier = pltpu.get_barrier_semaphore()
    for k in range(1, row_count):
        pl.semaphore_signal(
            barrier, inc=1, device_id=((r + k) % row_count, c), device_id_type=MESH
        )

    @pl.when(c > 0)
    def _():
        pl.semaphore_signal(barrier, inc=1, device_id=(r, c - 1), device_id_type=MESH)

    @pl.when(c < last_c)
    def _():
        pl.semaphore_signal(barrier, inc=1, device_id=(r, c + 1), device_id_type=MESH)

    has_left = jnp.where(c > 0, 1, 0)
    has_right = jnp.where(c < last_c, 1, 0)
    pl.semaphore_wait(barrier, row_count - 1 + has_left + has_right)

    def center(b, sub):
        return f2x.at[b, :, pl.ds(side + sub * side, side)]

    def z_copy(b, sub, way, own=False):
        source = f2_hbm.at[:, pl.ds(sub * side, side)] if own else center(b, sub)
        return pltpu.make_async_remote_copy(
            src_ref=source,
            dst_ref=center(b, sub),
            send_sem=zs_sem.at[way, b, sub],
            recv_sem=zr_sem.at[b, sub],
            device_id=(r, c - 1 if way == 0 else c + 1),
            device_id_type=MESH,
        )

    def halo_copy(b, way, own=False):
        sub = 0 if way == 0 else subs - 1
        at = band_rows + side if way == 0 else 0
        source = f2_hbm.at[:, pl.ds(sub * side, side)] if own else center(b, sub)
        return pltpu.make_async_remote_copy(
            src_ref=source,
            dst_ref=f2x.at[b, :, pl.ds(at, side)],
            send_sem=hs_sem.at[way, b],
            recv_sem=hr_sem.at[way, b],
            device_id=(r - 1 if way == 0 else r + 1, c),
            device_id_type=MESH,
        )

    def send_halo(b, sub, own=False):
        if sub == 0:

            @pl.when(r > 0)
            def _():
                halo_copy(b, 0, own).start()

        if sub == subs - 1:

            @pl.when(r < last_r)
            def _():
                halo_copy(b, 1, own).start()

    def f1_copy(index, row, half, bit, own=False):
        part = pl.ds(half * half_blocks, half_blocks)
        source = q_hbm.at[part] if own else f1a.at[row, part]
        return pltpu.make_async_remote_copy(
            src_ref=source,
            dst_ref=f1a.at[row, part],
            send_sem=fs_sem.at[index],
            recv_sem=fr_sem.at[row, half],
            device_id=(flipped(r, bit), c),
            device_id_type=MESH,
        )

    def tab_copy(k):
        return pltpu.make_async_remote_copy(
            src_ref=tab_hbm.at[(r + k) % row_count],
            dst_ref=tabv.at[r],
            send_sem=ts_sem.at[k],
            recv_sem=tr_sem.at[k],
            device_id=((r + k) % row_count, c),
            device_id_type=MESH,
        )

    def rep_copy(b, k):
        s = (r + k) % row_count
        return pltpu.make_async_remote_copy(
            src_ref=reps.at[b, s],
            dst_ref=rep_out.at[:, r, b],
            send_sem=rs_sem.at[b, k],
            recv_sem=rr_sem.at[b, k],
            device_id=(s, c),
            device_id_type=MESH,
        )

    def rep_local(b):
        return pltpu.make_async_copy(reps.at[b, r], rep_out.at[:, r, b], rs_sem.at[b, 0])

    x_row, y_row, d_row = flipped(r, 2), flipped(r, 4), flipped(flipped(r, 2), 4)
    f1_first = [(0, r, 0, 2), (1, r, 0, 4), (2, r, 1, 2), (3, r, 1, 4), (4, r, 0, 1), (5, r, 1, 1)]
    f1_second = [
        (6, x_row, 0, 4),
        (7, y_row, 1, 2),
        (8, x_row, 0, 1),
        (9, x_row, 1, 1),
        (10, y_row, 0, 1),
        (11, y_row, 1, 1),
    ]
    f1_third = [(12, d_row, 0, 1), (13, d_row, 1, 1)]

    loc_f2 = pltpu.make_async_copy(f2_hbm, f2x.at[c, :, pl.ds(side, band_rows)], loc_sem.at[0])
    loc_q = pltpu.make_async_copy(q_hbm, f1a.at[r], loc_sem.at[1])
    loc_tab = pltpu.make_async_copy(tab_hbm.at[r], tabv.at[r], loc_sem.at[2])
    loc_f2.start()
    loc_q.start()
    loc_tab.start()
    for sub in sub_order:

        @pl.when(c > 0)
        def _():
            z_copy(c, sub, 0, True).start()

        @pl.when(c < last_c)
        def _():
            z_copy(c, sub, 1, True).start()

    for item in f1_first:
        f1_copy(*item, own=True).start()
    for k in range(1, row_count):
        tab_copy(k).start()
    for sub in (0, subs - 1):
        send_halo(c, sub, True)

    @pl.when(r == 0)
    def _():
        f2x[:, :, 0:side] = jnp.zeros((plane_count, frame_count, side) + f2x.shape[3:], f2x.dtype)

    @pl.when(r == last_r)
    def _():
        f2x[:, :, band_rows + side :] = jnp.zeros(
            (plane_count, frame_count, side) + f2x.shape[3:], f2x.dtype
        )

    def each_side(step, act):
        @pl.when(c + step <= last_c)
        def _():
            act(c + step, 0)

        if step > 0:

            @pl.when(c - step >= 0)
            def _():
                act(c - step, 1)

    def take(step, sub):
        def act(b, way):
            z_copy(b, sub, way).wait_recv()

            @pl.when(c > 0 if way == 0 else c < last_c)
            def _():
                z_copy(b, sub, way).start()

            send_halo(b, sub)

        each_side(step, act)

    def pool(b, way):
        @pl.when(r > 0)
        def _():
            halo_copy(b, 1).wait_recv()

        @pl.when(r < last_r)
        def _():
            halo_copy(b, 0).wait_recv()

        rows = p1x.shape[2]

        def pool_row(t, carry):
            f, i = t // rows, t % rows
            pair = f2x[b, f, pl.ds(2 * i, 2)].astype(jnp.float32)
            both = pair[0] + pair[1]
            for lane in range(channels // 128):
                tmp[lane] = both[:, lane * 128 : (lane + 1) * 128]
            for lane in range(channels // 128):
                even = tmp[lane, pl.ds(0, band_cols // 2, stride=2), :]
                odd = tmp[lane, pl.ds(1, band_cols // 2, stride=2), :]
                p1x[b, f, i, :, lane * 128 : (lane + 1) * 128] = (even + odd) * 0.25
            return carry

        lax.fori_loop(0, frame_count * rows, pool_row, 0)

    lane_id = lax.broadcasted_iota(jnp.int32, (1, 1, 2 * block_cells), 2)
    query_row = lane_id % block_cells // side
    query_col = lane_id[0] % side
    is_first = lane_id[0] < block_cells

    def build(b, level):
        into = (map0, map1)[level]
        width = band_cols >> level
        rows = into.shape[0] // frame_count
        left_b, right_b = jnp.maximum(b - 1, 0), jnp.minimum(b + 1, last_c)

        def build_row(t, carry):
            f, y = t // rows, t % rows
            if level == 0:
                at = y + RADIUS
                left = f2x[left_b, f, at, width - 2 * side :, :].astype(jnp.float32)[side:]
                middle = f2x[b, f, at].astype(jnp.float32)
                right = f2x[right_b, f, at, : 2 * side, :].astype(jnp.float32)[:side]
            else:
                left = p1x[left_b, f, y, width - side :, :]
                middle = p1x[b, f, y]
                right = p1x[right_b, f, y, :side, :]
            left = jnp.where(b > 0, left, 0.0)
            right = jnp.where(b < last_c, right, 0.0)
            whole = jnp.concatenate([left, middle, right], axis=0)
            whole = pltpu.roll(whole, whole.shape[0] - RADIUS, 0)
            into[t] = whole[: width + side].reshape(into.shape[1:])
            return carry

        lax.fori_loop(0, into.shape[0], build_row, 0)

    def score_pair(b, s, level, pair):
        from_map = (map0, map1)[level]
        windows, queries = [], []
        for half in range(2):
            at = (b * LEVELS + level) * slots + 2 * pair + half
            k, row = tabs[s, 0, at], tabs[s, 1, at]
            cells = from_map[pl.ds(row, span), pl.ds(tabs[s, 2, at], 2)]
            windows.append(cells.reshape(span * span, channels).astype(jnp.bfloat16))
            queries.append(f1a[s, k])
        queries = jnp.concatenate(queries, axis=0)
        first, second = [
            lax.dot_general(
                window, queries, (((1,), (1,)), ((), ())), preferred_element_type=jnp.float32
            )
            for window in windows
        ]
        scores = jnp.where(is_first, first, second).reshape(span, span, 2 * block_cells)
        for bit in (1, 2, 4):
            scores = jnp.where((query_row & bit) != 0, scores[bit:], scores[:-bit])
        flat = scores.reshape(wside * span, 2 * block_cells)
        for bit in (1, 2, 4):
            moved = pltpu.roll(flat, flat.shape[0] - bit, 0)
            flat = jnp.where((query_col & bit) != 0, moved, flat)
        flat = flat * scale
        for a in range(wside):
            reps[b, s, level, pair, a * wside : (a + 1) * wside, :] = flat[
                a * span : a * span + wside
            ]

    code = chosen(c, [sum(b * plane_count**i for i, b in enumerate(row)) for row in order])

    def process(i, carry):
        power = chosen(i, [plane_count**n for n in range(plane_count)])
        b = code // power % plane_count
        for level in range(LEVELS):
            build(b, level)

        def source(k, inner):
            s = (r + k) % row_count
            for level in range(LEVELS):
                for pair in range(slots // 2):
                    score_pair(b, s, level, pair)

            @pl.when(k == 0)
            def _():
                rep_local(b).start()

            @pl.when(k > 0)
            def _():
                rep_copy(b, k).start()

            return inner

        lax.fori_loop(0, row_count, source, 0)
        return carry

    def process_ready(step):
        low = chosen(c, [row[step - 1] for row in done])
        high = chosen(c, [row[step] for row in done])
        lax.fori_loop(low, high, process, 0)

    for sub in sub_order:
        take(1, sub)
    for item in f1_second:
        index, row, half, bit = item
        if index in (6, 7, 9, 10):
            f1_copy(*item).wait_recv()
        f1_copy(*item).start()
    if plane_count > 2:
        for sub in sub_order[:2]:
            take(2, sub)
    for item in f1_third:
        f1_copy(*item).wait_recv()
        f1_copy(*item).start()
    for bits in ((1,), (1, 2), (1, 4), (1, 2, 4)):
        row = r
        for bit in bits:
            row = flipped(row, bit)
        for half in range(2):
            f1_copy(0, row, half, 1).wait_recv()
    for k in range(1, row_count):
        tab_copy(k).wait_recv()
    loc_tab.wait()
    loc_q.wait()
    loc_f2.wait()
    tab_smem = pltpu.make_async_copy(tabv, tabs, tl_sem)
    tab_smem.start()
    tab_smem.wait()
    each_side(0, pool)
    each_side(1, pool)
    process_ready(1)
    for step in range(2, plane_count):
        for sub in sub_order[2:] if step == 2 else sub_order:
            take(step, sub)
        each_side(step, pool)
        process_ready(step)

    for step in range(plane_count):
        for sub in range(subs):

            def sent(b, way):
                @pl.when(c > 0 if way == 0 else c < last_c)
                def _():
                    z_copy(b, sub, way).wait_send()

            each_side(step, sent)
            if step == 0:

                @pl.when(c < last_c)
                def _():
                    z_copy(c, sub, 1).wait_send()

    def plane_end(b, carry):
        @pl.when(r > 0)
        def _():
            halo_copy(b, 0).wait_send()

        @pl.when(r < last_r)
        def _():
            halo_copy(b, 1).wait_send()

        rep_local(b).wait()

        def peer_end(k, inner):
            rep_copy(b, k).wait_send()
            rep_copy(b, k).wait_recv()
            return inner

        lax.fori_loop(1, row_count, peer_end, 0)
        return carry

    lax.fori_loop(0, plane_count, plane_end, 0)
    for item in f1_first + f1_second + f1_third:
        f1_copy(*item).wait_send()
    for k in range(1, row_count):
        tab_copy(k).wait_send()


def join_kernel(pair_count, source_ref, half_ref, reply_ref, out_ref):
    level = pl.program_id(0)
    window_cells, lanes = out_ref.shape[1], reply_ref.shape[-1]
    is_first = lax.broadcasted_iota(jnp.int32, (window_cells, lanes), 1) < lanes // 2

    def step(m, carry):
        at = 2 * (level * pair_count + m)
        picked = []
        for side in range(2):
            rows = reply_ref[0, source_ref[at + side], :window_cells, :]
            moved = pltpu.roll(rows, lanes // 2, 1)
            picked.append(jnp.where(half_ref[at + side] == side, rows, moved))
        spot = pl.ds(pl.multiple_of(m * lanes, lanes), lanes)
        out_ref[0, :, spot] = jnp.where(is_first, picked[0], picked[1])
        return carry

    lax.fori_loop(0, pair_count, step, 0)


def gathered_body(fmap1, fmap2, target_owner, target_tile):
    side = 2 * RADIUS
    window_cells = (2 * RADIUS + 1) ** 2
    frame_count, band_rows, band_cols, channels = fmap1.shape
    row_count = lax.axis_size("rows")
    plane_count = lax.axis_size("cols")
    device_count = row_count * plane_count
    subs, across = band_rows // side, band_cols // side
    per_frame = subs * across
    block_count = frame_count * per_frame
    block_cells = side * side
    slots = max(2, (2 * block_count + device_count - 1) // device_count)
    queries = fmap1.reshape(frame_count, subs, side, across, side, channels)
    queries = queries.transpose(0, 1, 3, 2, 4, 5).reshape(block_count, block_cells, channels)

    owner = target_owner[:, :, 0]
    owner_ids = jnp.arange(device_count, dtype=jnp.int32)
    hits = (owner[:, :, None] == owner_ids).astype(jnp.int32)
    rank = jnp.sum(hits * (jnp.cumsum(hits, axis=1) - 1), axis=2)
    block_ids = jnp.arange(block_count, dtype=jnp.int32)
    entries = []
    for level in range(LEVELS):
        level_across = across >> level
        tile = target_tile[level] % ((subs >> level) * level_across)
        map_rows = (band_rows >> level) + side
        row = block_ids // per_frame * map_rows + tile // level_across * side
        entries.append(jnp.stack([block_ids, row, tile % level_across]))
    entries = jnp.stack(entries, axis=1)
    ranked = (rank[:, :, None] == jnp.arange(slots, dtype=jnp.int32)).astype(jnp.int32)
    table = jnp.sum(
        hits[:, :, :, None] * ranked[:, :, None, :] * entries[:, :, :, None, None], axis=2
    )
    table = table.reshape(3, LEVELS, row_count, plane_count, slots).transpose(2, 0, 3, 1, 4)
    used = plane_count * LEVELS * slots
    table = table.reshape(row_count, 3, used)
    table = jnp.pad(table, ((0, 0), (0, 5), (0, -used % 128)))

    padded_rows = -(-window_cells // 8) * 8
    pairs = slots // 2
    reply_shape = (LEVELS, row_count, plane_count, pairs, padded_rows, 2 * block_cells)
    ext_rows = band_rows + 2 * side
    dma = pltpu.SemaphoreType.DMA
    replies = pl.pallas_call(
        functools.partial(lookup_kernel, (row_count, plane_count, slots, channels**-0.5)),
        out_shape=jax.ShapeDtypeStruct(reply_shape, jnp.float32),
        in_specs=[pl.BlockSpec(memory_space=pl.ANY)] * 3,
        out_specs=pl.BlockSpec(memory_space=pl.ANY),
        scratch_shapes=[
            pltpu.VMEM((plane_count, frame_count, ext_rows, band_cols, channels), jnp.bfloat16),
            pltpu.VMEM((row_count, block_count, block_cells, channels), jnp.bfloat16),
            pltpu.VMEM(table.shape, jnp.int32),
            pltpu.SMEM(table.shape, jnp.int32),
            pltpu.VMEM((frame_count * (band_rows + side), across + 1, side, channels), jnp.float32),
            pltpu.VMEM(
                (frame_count * (band_rows // 2 + side), across // 2 + 1, side, channels),
                jnp.float32,
            ),
            pltpu.VMEM(
                (plane_count, frame_count, ext_rows // 2, band_cols // 2, channels), jnp.float32
            ),
            pltpu.VMEM((channels // 128, band_cols, 128), jnp.float32),
            pltpu.VMEM(
                (plane_count, row_count, LEVELS, pairs, padded_rows, 2 * block_cells), jnp.float32
            ),
            dma((3,)),
            dma((2, plane_count, subs)),
            dma((plane_count, subs)),
            dma((2, plane_count)),
            dma((2, plane_count)),
            dma((14,)),
            dma((row_count, 2)),
            dma((row_count,)),
            dma((row_count,)),
            dma,
            dma((plane_count, row_count)),
            dma((plane_count, row_count)),
        ],
        compiler_params=pltpu.CompilerParams(
            collective_id=0, has_side_effects=True, vmem_limit_bytes=62 * 2**20
        ),
    )(fmap2, queries, table)
    spots = row_count * plane_count * pairs
    source_ids = owner * pairs + rank // 2
    return pl.pallas_call(
        functools.partial(join_kernel, block_count // 2),
        out_shape=jax.ShapeDtypeStruct(
            (LEVELS, window_cells, block_count * block_cells), jnp.float32
        ),
        grid_spec=pltpu.PrefetchScalarGridSpec(
            num_scalar_prefetch=2,
            grid=(LEVELS,),
            in_specs=[
                pl.BlockSpec(
                    (1, spots, padded_rows, 2 * block_cells), lambda l, *_: (l, 0, 0, 0)
                )
            ],
            out_specs=pl.BlockSpec(
                (1, window_cells, block_count * block_cells), lambda l, *_: (l, 0, 0)
            ),
        ),
    )(
        source_ids.reshape(-1),
        (rank % 2).reshape(-1),
        replies.reshape(LEVELS, spots, padded_rows, 2 * block_cells),
    )


def solution(mesh):
    in_specs = (
        P(None, "rows", "cols", None),
        P(None, "rows", "cols", None),
        P(None, ("rows", "cols"), None),
        P(None, ("rows", "cols")),
    )
    out_specs = P(None, None, ("rows", "cols"))
    chosen_body = gathered_body if mesh.shape["rows"] == 8 else body
    return jax.shard_map(
        chosen_body, mesh=mesh, in_specs=in_specs, out_specs=out_specs, check_vma=False
    )
```

```python
import functools

import jax
import jax.numpy as jnp
from jax import lax
from jax.experimental import pallas as pl
from jax.experimental.pallas import tpu as pltpu
from jax.sharding import PartitionSpec as P

RADIUS = 4
LEVELS = 2
STEP_SLOTS = 16


def padded_2(block, sides, width):
    for axis, dim in sides:
        count = lax.axis_size(axis)
        forward = [(i, i + 1) for i in range(count - 1)]
        backward = [(target, source) for source, target in forward]
        low = lax.ppermute(
            lax.slice_in_dim(block, block.shape[dim] - width, None, axis=dim), axis, forward
        )
        high = lax.ppermute(lax.slice_in_dim(block, 0, width, axis=dim), axis, backward)
        block = jnp.concatenate([low, block, high], axis=dim)
    return block


def pool_level(level_map):
    frame_count, rows_in, cols_in, channels = level_map.shape
    pooled = level_map.astype(jnp.float32).reshape(
        frame_count, rows_in // 2, 2, cols_in // 2, 2, channels
    )
    return jnp.mean(pooled, axis=(2, 4)).astype(jnp.bfloat16)


def dispatch_kernel(slot_count, block_ref, query_ref, sent_ref):
    base = pl.program_id(0) * slot_count
    for slot in range(slot_count):
        sent_ref[slot] = query_ref[block_ref[base + slot]]


def correlate_kernel(plan, scale, label_ref, query_ref, map_ref, reply_ref):
    per_frame, col_count, padded_rows, across = plan
    tile_side = 2 * RADIUS
    span_side = 4 * RADIUS
    window_side = 2 * RADIUS + 1
    block_cells = tile_side * tile_side
    base = pl.program_id(0) * STEP_SLOTS
    lane = lax.broadcasted_iota(jnp.int32, (1, 1, 2 * block_cells), 2)
    query_row = lane % block_cells // tile_side
    query_col = lane[0] % tile_side
    is_first = lane[0] < block_cells

    def window(slot):
        label = label_ref[base + slot]
        tile = label % per_frame
        region = label // per_frame
        row = region // col_count * padded_rows + tile // across * tile_side
        col = (region % col_count * across + tile % across) * tile_side
        col = pl.multiple_of(col, tile_side)
        cells = map_ref[pl.ds(row, span_side), pl.ds(col, span_side), :]
        return cells.reshape(span_side * span_side, -1).astype(jnp.bfloat16)

    for pair in range(STEP_SLOTS // 2):
        queries = query_ref[2 * pair : 2 * pair + 2].reshape(2 * block_cells, -1)
        first, second = [
            lax.dot_general(
                window(2 * pair + half),
                queries,
                (((1,), (1,)), ((), ())),
                preferred_element_type=jnp.float32,
            )
            for half in range(2)
        ]
        scores = jnp.where(is_first, first, second)
        scores = scores.reshape(span_side, span_side, 2 * block_cells)
        for bit in (1, 2, 4):
            scores = jnp.where((query_row & bit) != 0, scores[bit:], scores[:-bit])
        flat = scores.reshape(window_side * span_side, 2 * block_cells)
        for bit in (1, 2, 4):
            moved = pltpu.roll(flat, flat.shape[0] - bit, 0)
            flat = jnp.where((query_col & bit) != 0, moved, flat)
        flat = flat * scale
        for a in range(window_side):
            at = (pair * window_side + a) * window_side
            reply_ref[at : at + window_side, :] = flat[
                a * span_side : a * span_side + window_side
            ]


def assemble_kernel(pair_count, source_ref, half_ref, *refs):
    reply_refs, out_ref = refs[:-1], refs[-1]
    window_cells, lanes = out_ref.shape[1], reply_refs[0].shape[1]
    is_first = lax.broadcasted_iota(jnp.int32, (window_cells, lanes), 1) < lanes // 2
    for level in range(LEVELS):

        def step(m, carry, level=level):
            at = 2 * (level * pair_count + m)
            picked = []
            for side in range(2):
                first_row = source_ref[at + side] * window_cells
                rows = reply_refs[level][pl.ds(first_row, window_cells), :]
                moved = pltpu.roll(rows, lanes // 2, 1)
                picked.append(jnp.where(half_ref[at + side] == side, rows, moved))
            spot = pl.ds(pl.multiple_of(m * lanes, lanes), lanes)
            out_ref[level, :, spot] = jnp.where(is_first, picked[0], picked[1])
            return carry

        lax.fori_loop(0, pair_count, step, 0)


def body(fmap1, fmap2, target_owner, target_tile):
    tile_side = 2 * RADIUS
    window_side = 2 * RADIUS + 1
    block_cells = tile_side * tile_side
    frame_count, band_rows, band_cols, channels = fmap1.shape
    row_count = lax.axis_size("rows")
    col_count = lax.axis_size("cols")
    device_count = row_count * col_count
    tiles_across = band_cols // tile_side
    per_frame = band_rows // tile_side * tiles_across
    block_count = frame_count * per_frame
    owner_slots = max(2, (2 * block_count + device_count - 1) // device_count)
    row_slots = -(-owner_slots * col_count // STEP_SLOTS) * STEP_SLOTS
    pair_slots = row_slots // 2
    queries = fmap1.reshape(
        frame_count, band_rows // tile_side, tile_side, tiles_across, tile_side, channels
    )
    queries = queries.transpose(0, 1, 3, 2, 4, 5).reshape(block_count, block_cells, channels)
    owner_ids = target_owner[:, :, 0]
    owner_rows = owner_ids // col_count
    peer_ids = jnp.arange(row_count, dtype=jnp.int32)
    owner_hits = (owner_rows[:, :, None] == peer_ids[None, None, :]).astype(jnp.int32)
    slot_rank = jnp.sum(owner_hits * (jnp.cumsum(owner_hits, axis=1) - 1), axis=2)
    block_ids = jnp.arange(block_count, dtype=jnp.int32)
    label_rows = []
    for level in range(LEVELS):
        tile_count = (band_rows >> level) // tile_side * ((band_cols >> level) // tile_side)
        regions = block_ids // per_frame * col_count + owner_ids[level] % col_count
        label_rows.append(regions * per_frame + target_tile[level] % tile_count)
    rank_ids = jnp.arange(row_slots, dtype=jnp.int32)
    rank_hits = (slot_rank[:, :, None] == rank_ids[None, None, :]).astype(jnp.int32)
    slot_hits = owner_hits[:, :, :, None] * rank_hits[:, :, None, :]

    def by_slot(values):
        table = jnp.sum(slot_hits * values[:, :, None, None], axis=1)
        return table.transpose(1, 0, 2)

    labels_sent = by_slot(jnp.stack(label_rows))
    blocks_sent = by_slot(jnp.broadcast_to(block_ids[None], owner_ids.shape))
    slot_block = (row_slots, block_cells, channels)
    slot_total = row_count * row_slots
    label_part = lax.all_to_all(labels_sent, "rows", split_axis=0, concat_axis=0, tiled=True)
    levels = [fmap2]
    for level in range(1, LEVELS):
        levels.append(pool_level(levels[-1]))
    window_cells = window_side * window_side
    step_block = (STEP_SLOTS, block_cells, channels)
    reply_block = (STEP_SLOTS // 2 * window_cells, 2 * block_cells)
    reply_tables = [None] * LEVELS
    earlier = None
    for level in reversed(range(LEVELS)):
        queries_sent = pl.pallas_call(
            functools.partial(dispatch_kernel, row_slots),
            out_shape=jax.ShapeDtypeStruct((slot_total,) + slot_block[1:], jnp.bfloat16),
            grid_spec=pltpu.PrefetchScalarGridSpec(
                num_scalar_prefetch=1,
                grid=(row_count,),
                in_specs=[pl.BlockSpec(queries.shape, lambda d, *_: (0, 0, 0))],
                out_specs=pl.BlockSpec(slot_block, lambda d, *_: (d, 0, 0)),
            ),
        )(blocks_sent[:, level].reshape(-1), queries)
        query_part = lax.all_to_all(
            queries_sent.reshape((row_count,) + slot_block),
            "rows",
            split_axis=0,
            concat_axis=0,
            tiled=True,
        )
        band = lax.all_gather(levels[level], "cols", axis=2, tiled=True)
        if earlier is not None:
            band = lax.optimization_barrier((band, earlier, query_part))[0]
        padded = padded_2(band, (("rows", 1),), RADIUS).astype(jnp.float32)
        padded = jnp.pad(padded, ((0, 0), (0, 0), (RADIUS, RADIUS), (0, 0)))
        level_map = padded.reshape((-1,) + padded.shape[2:])
        plan = (per_frame, col_count, padded.shape[1], levels[level].shape[2] // tile_side)
        replies = pl.pallas_call(
            functools.partial(correlate_kernel, plan, channels ** (-0.5)),
            out_shape=jax.ShapeDtypeStruct(
                (row_count * pair_slots * window_cells, 2 * block_cells), jnp.float32
            ),
            grid_spec=pltpu.PrefetchScalarGridSpec(
                num_scalar_prefetch=1,
                grid=(slot_total // STEP_SLOTS,),
                in_specs=[
                    pl.BlockSpec(step_block, lambda d, *_: (d, 0, 0)),
                    pl.BlockSpec(
                        level_map.shape, lambda d, *_: (0, 0, 0), pipeline_mode=pl.Buffered(1)
                    ),
                ],
                out_specs=pl.BlockSpec(reply_block, lambda d, *_: (d, 0)),
            ),
        )(
            label_part[:, level].reshape(-1),
            query_part.reshape((slot_total,) + slot_block[1:]),
            level_map,
        )
        returned = lax.all_to_all(
            replies.reshape(row_count, pair_slots * window_cells, 2 * block_cells),
            "rows",
            split_axis=0,
            concat_axis=0,
            tiled=True,
        )
        earlier = returned
        reply_tables[level] = returned.reshape(-1, 2 * block_cells)
    source_ids = owner_rows * pair_slots + slot_rank // 2
    return pl.pallas_call(
        functools.partial(assemble_kernel, block_count // 2),
        out_shape=jax.ShapeDtypeStruct(
            (LEVELS, window_cells, block_count * block_cells), jnp.float32
        ),
        in_specs=[
            pl.BlockSpec(memory_space=pltpu.SMEM),
            pl.BlockSpec(memory_space=pltpu.SMEM),
        ]
        + [pl.BlockSpec(memory_space=pltpu.VMEM)] * LEVELS,
        out_specs=pl.BlockSpec(memory_space=pltpu.VMEM),
    )(source_ids.reshape(-1), (slot_rank % 2).reshape(-1), *reply_tables)


MESH = pl.DeviceIdType.MESH
TOP = 32767.0


def flipped(index, bit):
    return index + bit - 2 * bit * (index // bit % 2)


def lookup_kernel(
    plan,
    f2_hbm,
    q_hbm,
    tab_hbm,
    rep_out,
    f2x,
    f1a,
    tabv,
    tabs,
    map0,
    map1,
    p1x,
    tmp,
    line,
    reps,
    loc_sem,
    zs_sem,
    zr_sem,
    hs_sem,
    hr_sem,
    fs_sem,
    fr_sem,
    ts_sem,
    tr_sem,
    tl_sem,
    rs_sem,
    rr_sem,
):
    row_count, plane_count, slots, scale = plan
    frame_count, band_rows, band_cols, channels = f2_hbm.shape
    block_count, block_cells, _ = q_hbm.shape
    side = 2 * RADIUS
    span = 4 * RADIUS
    wside = 2 * RADIUS + 1
    wide = 2 * side
    strips = band_cols // wide
    half_blocks = block_count // 2
    r = lax.axis_index("rows")
    c = lax.axis_index("cols")
    last_r, last_c = row_count - 1, plane_count - 1

    barrier = pltpu.get_barrier_semaphore()
    for k in range(1, row_count):
        pl.semaphore_signal(
            barrier, inc=1, device_id=((r + k) % row_count, c), device_id_type=MESH
        )

    @pl.when(c > 0)
    def _():
        pl.semaphore_signal(barrier, inc=1, device_id=(r, c - 1), device_id_type=MESH)

    @pl.when(c < last_c)
    def _():
        pl.semaphore_signal(barrier, inc=1, device_id=(r, c + 1), device_id_type=MESH)

    has_left = jnp.where(c > 0, 1, 0)
    has_right = jnp.where(c < last_c, 1, 0)
    pl.semaphore_wait(barrier, row_count - 1 + has_left + has_right)

    def strip(at, way):
        return at if way == 0 else strips - 1 - at

    def z_copy(b, at, way, own=False):
        cols = pl.ds(strip(at, way) * wide, wide)
        here = f2x.at[b, :, pl.ds(side, band_rows), cols]
        return pltpu.make_async_remote_copy(
            src_ref=f2_hbm.at[:, :, cols] if own else here,
            dst_ref=here,
            send_sem=zs_sem.at[way, b, at],
            recv_sem=zr_sem.at[b, at],
            device_id=(r, c - 1 if way == 0 else c + 1),
            device_id_type=MESH,
        )

    def halo_copy(b, at, way, up, own=False):
        cols = pl.ds(strip(at, way) * wide, wide)
        first = 0 if up else band_rows - side
        into = band_rows + side if up else 0
        if own:
            source = f2_hbm.at[:, pl.ds(first, side), cols]
        else:
            source = f2x.at[b, :, pl.ds(first + side, side), cols]
        lane = 0 if up else 1
        return pltpu.make_async_remote_copy(
            src_ref=source,
            dst_ref=f2x.at[b, :, pl.ds(into, side), cols],
            send_sem=hs_sem.at[lane, b, at],
            recv_sem=hr_sem.at[lane, b, at],
            device_id=(r - 1 if up else r + 1, c),
            device_id_type=MESH,
        )

    def send_halo(b, at, way, own=False):
        @pl.when(r > 0)
        def _():
            halo_copy(b, at, way, True, own).start()

        @pl.when(r < last_r)
        def _():
            halo_copy(b, at, way, False, own).start()

    def f1_copy(index, row, half, bit, own=False):
        part = pl.ds(half * half_blocks, half_blocks)
        source = q_hbm.at[part] if own else f1a.at[row, part]
        return pltpu.make_async_remote_copy(
            src_ref=source,
            dst_ref=f1a.at[row, part],
            send_sem=fs_sem.at[index],
            recv_sem=fr_sem.at[row, half],
            device_id=(flipped(r, bit), c),
            device_id_type=MESH,
        )

    def tab_copy(k):
        return pltpu.make_async_remote_copy(
            src_ref=tab_hbm.at[(r + k) % row_count],
            dst_ref=tabv.at[r],
            send_sem=ts_sem.at[k],
            recv_sem=tr_sem.at[k],
            device_id=((r + k) % row_count, c),
            device_id_type=MESH,
        )

    def rep_copy(b, k):
        s = (r + k) % row_count
        return pltpu.make_async_remote_copy(
            src_ref=reps.at[b, s],
            dst_ref=rep_out.at[:, r, b],
            send_sem=rs_sem.at[b, k],
            recv_sem=rr_sem.at[b, k],
            device_id=(s, c),
            device_id_type=MESH,
        )

    def rep_local(b):
        return pltpu.make_async_copy(reps.at[b, r], rep_out.at[:, r, b], rs_sem.at[b, 0])

    x_row, y_row, d_row = flipped(r, 2), flipped(r, 4), flipped(flipped(r, 2), 4)
    f1_first = [(0, r, 0, 2), (1, r, 0, 4), (2, r, 1, 2), (3, r, 1, 4), (4, r, 0, 1), (5, r, 1, 1)]
    f1_second = [
        (6, x_row, 0, 4),
        (7, y_row, 1, 2),
        (8, x_row, 0, 1),
        (9, x_row, 1, 1),
        (10, y_row, 0, 1),
        (11, y_row, 1, 1),
    ]
    f1_third = [(12, d_row, 0, 1), (13, d_row, 1, 1)]

    loc_f2 = pltpu.make_async_copy(f2_hbm, f2x.at[c, :, pl.ds(side, band_rows)], loc_sem.at[0])
    loc_q = pltpu.make_async_copy(q_hbm, f1a.at[r], loc_sem.at[1])
    loc_tab = pltpu.make_async_copy(tab_hbm.at[r], tabv.at[r], loc_sem.at[2])
    loc_f2.start()
    loc_q.start()
    loc_tab.start()
    for at in range(strips):

        @pl.when(c > 0)
        def _():
            z_copy(c, at, 0, True).start()

        @pl.when(c < last_c)
        def _():
            z_copy(c, at, 1, True).start()

    for item in f1_first:
        f1_copy(*item, own=True).start()
    for k in range(1, row_count):
        tab_copy(k).start()
    for at in range(strips):
        send_halo(c, at, 0, True)

    @pl.when(r == 0)
    def _():
        f2x[:, :, 0:side] = jnp.zeros((plane_count, frame_count, side) + f2x.shape[3:], f2x.dtype)

    @pl.when(r == last_r)
    def _():
        f2x[:, :, band_rows + side :] = jnp.zeros(
            (plane_count, frame_count, side) + f2x.shape[3:], f2x.dtype
        )

    def each_side(step, act):
        @pl.when(c + step <= last_c)
        def _():
            act(c + step, 0)

        if step > 0:

            @pl.when(c - step >= 0)
            def _():
                act(c - step, 1)

    def take(step, at):
        def act(b, way):
            z_copy(b, at, way).wait_recv()

            @pl.when(c > 0 if way == 0 else c < last_c)
            def _():
                z_copy(b, at, way).start()

            send_halo(b, at, way)

        each_side(step, act)

    def pool(step, ats):
        def act(b, way):
            for at in ats:

                @pl.when(r > 0)
                def _():
                    halo_copy(b, at, way, False).wait_recv()

                @pl.when(r < last_r)
                def _():
                    halo_copy(b, at, way, True).wait_recv()

            rows = p1x.shape[2]
            for at in ats:
                col = strip(at, way)

                def pool_row(t, carry):
                    f, i = t // rows, t % rows
                    pair = f2x[b, f, pl.ds(2 * i, 2), col * wide : (col + 1) * wide]
                    pair = pair.astype(jnp.float32)
                    both = pair[0] + pair[1]
                    for lane in range(channels // 128):
                        tmp[lane, pl.ds(i * wide, wide), :] = both[:, lane * 128 : (lane + 1) * 128]
                    for lane in range(channels // 128):
                        even = tmp[lane, pl.ds(i * wide, side, stride=2), :]
                        odd = tmp[lane, pl.ds(i * wide + 1, side, stride=2), :]
                        p1x[
                            b, f, i, col * side : (col + 1) * side, lane * 128 : (lane + 1) * 128
                        ] = (even + odd) * 0.25
                    return carry

                lax.fori_loop(0, frame_count * rows, pool_row, 0, unroll=4)

        each_side(step, act)

    lane_id = lax.broadcasted_iota(jnp.int32, (1, 1, 2 * block_cells), 2)
    query_row = lane_id % block_cells // side
    query_col = lane_id[0] % side
    is_first = lane_id[0] < block_cells
    row_id = lax.broadcasted_iota(jnp.int32, line.shape[1:], 0)
    line[...] = jnp.zeros(line.shape, line.dtype)

    def build(b, level):
        into = (map0, map1)[level]
        width = band_cols >> level
        rows = into.shape[0] // frame_count
        left_b, right_b = jnp.maximum(b - 1, 0), jnp.minimum(b + 1, last_c)

        def build_row(t, carry):
            f, y = t // rows, t % rows
            if level == 0:
                at = y + RADIUS
                left = f2x[left_b, f, at, width - 2 * side :, :].astype(jnp.float32)[side:]
                middle = f2x[b, f, at].astype(jnp.float32)
                right = f2x[right_b, f, at, : 2 * side, :].astype(jnp.float32)[:side]
            else:
                left = p1x[left_b, f, y, width - side :, :]
                middle = p1x[b, f, y]
                right = p1x[right_b, f, y, :side, :]
            left = jnp.where(b > 0, left, 0.0)
            right = jnp.where(b < last_c, right, 0.0)
            whole = jnp.concatenate([left, middle, right], axis=0)
            whole = pltpu.roll(whole, whole.shape[0] - RADIUS, 0)
            into[t] = whole[: width + side].reshape(into.shape[1:])
            return carry

        lax.fori_loop(0, into.shape[0], build_row, 0)

    def score_pair(b, s, level, pair):
        from_map = (map0, map1)[level]
        windows, queries = [], []
        for half in range(2):
            at = (b * LEVELS + level) * slots + 2 * pair + half
            k, row = tabs[s, 0, at], tabs[s, 1, at]
            cells = from_map[pl.ds(row, span), pl.ds(tabs[s, 2, at], 2)]
            windows.append(cells.reshape(span * span, channels).astype(jnp.bfloat16))
            queries.append(f1a[s, k])
        queries = jnp.concatenate(queries, axis=0)
        first, second = [
            lax.dot_general(
                window, queries, (((1,), (1,)), ((), ())), preferred_element_type=jnp.float32
            )
            for window in windows
        ]
        scores = jnp.where(is_first, first, second).reshape(span, span, 2 * block_cells)
        for bit in (1, 2, 4):
            scores = jnp.where((query_row & bit) != 0, scores[bit:], scores[:-bit])
        flat = scores.reshape(wside * span, 2 * block_cells)
        for bit in (1, 2, 4):
            moved = pltpu.roll(flat, flat.shape[0] - bit, 0)
            flat = jnp.where((query_col & bit) != 0, moved, flat)
        flat = flat * scale
        for a in range(wside):
            line[pair, a * wside : (a + 1) * wside, :] = flat[a * span : a * span + wside]
        found = line[pair]
        top = jnp.max(jnp.abs(found), axis=0, keepdims=True)
        power = jnp.maximum(jnp.ceil(jnp.log2(top)), -100.0)
        coded = jnp.floor(found * (TOP * jnp.exp2(-power)) + 0.5)
        coded = jnp.clip(coded, -TOP, TOP)
        coded = jnp.where(row_id == wside * wside, power, coded)
        reps[b, s, level, pair] = coded.astype(jnp.int32).astype(jnp.int16)

    def process(b, way):
        for level in range(LEVELS):
            build(b, level)

        def source(k, inner):
            s = (r + k) % row_count
            for level in range(LEVELS):
                for pair in range(slots // 2):
                    score_pair(b, s, level, pair)

            @pl.when(k == 0)
            def _():
                rep_local(b).start()

            @pl.when(k > 0)
            def _():
                rep_copy(b, k).start()

            return inner

        lax.fori_loop(0, row_count, source, 0)

    for at in range(strips):
        take(1, at)
    for item in f1_second:
        index, row, half, bit = item
        if index in (6, 7, 9, 10):
            f1_copy(*item).wait_recv()
        f1_copy(*item).start()
    for at in range(strips - 1):
        take(2, at)
    for item in f1_third:
        f1_copy(*item).wait_recv()
        f1_copy(*item).start()
    for bits in ((1,), (1, 2), (1, 4), (1, 2, 4)):
        row = r
        for bit in bits:
            row = flipped(row, bit)
        for half in range(2):
            f1_copy(0, row, half, 1).wait_recv()
    for k in range(1, row_count):
        tab_copy(k).wait_recv()
    loc_tab.wait()
    loc_q.wait()
    loc_f2.wait()
    tab_smem = pltpu.make_async_copy(tabv, tabs, tl_sem)
    tab_smem.start()
    tab_smem.wait()
    near, rest = [0], list(range(1, strips))
    pool(0, near + rest)
    pool(1, near)
    each_side(0, process)
    take(2, strips - 1)
    for step in range(1, plane_count):
        if step > 2:
            for at in rest:
                take(step, at)
        if step >= 2 and step + 1 < plane_count:
            take(step + 1, 0)
        pool(step, rest)
        if step + 1 < plane_count:
            pool(step + 1, near)
        each_side(step, process)

    for at in range(strips):

        @pl.when(c < last_c)
        def _():
            z_copy(c, at, 1).wait_send()

    for step in range(plane_count):

        def sent(b, way):
            for at in range(strips):

                @pl.when(c > 0 if way == 0 else c < last_c)
                def _():
                    z_copy(b, at, way).wait_send()

                @pl.when(r > 0)
                def _():
                    halo_copy(b, at, way, True).wait_send()

                @pl.when(r < last_r)
                def _():
                    halo_copy(b, at, way, False).wait_send()

        each_side(step, sent)

    def plane_end(b, carry):
        rep_local(b).wait()

        def peer_end(k, inner):
            rep_copy(b, k).wait_send()
            rep_copy(b, k).wait_recv()
            return inner

        lax.fori_loop(1, row_count, peer_end, 0)
        return carry

    lax.fori_loop(0, plane_count, plane_end, 0)
    for item in f1_first + f1_second + f1_third:
        f1_copy(*item).wait_send()
    for k in range(1, row_count):
        tab_copy(k).wait_send()


def join_kernel(pair_count, window_cells, source_ref, half_ref, reply_ref, out_ref):
    level = pl.program_id(0)
    padded_rows, lanes = reply_ref.shape[-2:]
    is_first = lax.broadcasted_iota(jnp.int32, (padded_rows, lanes), 1) < lanes // 2

    def step(m, carry):
        at = 2 * (level * pair_count + m)
        picked = []
        for side in range(2):
            rows = reply_ref[0, source_ref[at + side]].astype(jnp.int32).astype(jnp.float32)
            moved = pltpu.roll(rows, lanes // 2, 1)
            picked.append(jnp.where(half_ref[at + side] == side, rows, moved))
        both = jnp.where(is_first, picked[0], picked[1])
        unit = jnp.exp2(both[window_cells : window_cells + 1]) * (1.0 / TOP)
        spot = pl.ds(m * LEVELS + level, window_cells, stride=pair_count * LEVELS)
        out_ref[spot, :] = both[:window_cells] * unit
        return carry

    lax.fori_loop(0, pair_count, step, 0, unroll=2)


def gathered_body(fmap1, fmap2, target_owner, target_tile):
    side = 2 * RADIUS
    window_cells = (2 * RADIUS + 1) ** 2
    frame_count, band_rows, band_cols, channels = fmap1.shape
    row_count = lax.axis_size("rows")
    plane_count = lax.axis_size("cols")
    device_count = row_count * plane_count
    subs, across = band_rows // side, band_cols // side
    per_frame = subs * across
    block_count = frame_count * per_frame
    block_cells = side * side
    slots = max(2, (2 * block_count + device_count - 1) // device_count)
    queries = fmap1.reshape(frame_count, subs, side, across, side, channels)
    queries = queries.transpose(0, 1, 3, 2, 4, 5).reshape(block_count, block_cells, channels)

    owner = target_owner[:, :, 0]
    block_ids = jnp.arange(block_count, dtype=jnp.int32)
    earlier = block_ids[:, None] > block_ids[None, :]
    same = owner[:, :, None] == owner[:, None, :]
    rank = jnp.sum((same & earlier).astype(jnp.int32), axis=2)
    values, places = [], []
    for level in range(LEVELS):
        level_across = across >> level
        tile = target_tile[level] % ((subs >> level) * level_across)
        map_rows = (band_rows >> level) + side
        row = block_ids // per_frame * map_rows + tile // level_across * side
        values.append(jnp.stack([block_ids, row, tile % level_across]))
        places.append((owner[level] % plane_count * LEVELS + level) * slots + rank[level])
    values = jnp.pad(jnp.concatenate(values, axis=1), ((0, 5), (0, 0)))
    places = jnp.concatenate(places)
    towards = owner.reshape(-1) // plane_count
    lanes_used = -(-plane_count * LEVELS * slots // 128) * 128
    named = towards == jnp.arange(row_count, dtype=jnp.int32)[:, None]
    left = jnp.where(named[:, None, :], values[None], 0).astype(jnp.float32)
    right = (places[:, None] == jnp.arange(lanes_used, dtype=jnp.int32)).astype(jnp.float32)
    table = lax.dot_general(
        left, right, (((2,), (0,)), ((), ())), precision=lax.Precision.HIGHEST
    ).astype(jnp.int32)

    padded_rows = -(-(window_cells + 1) // 16) * 16
    pairs = slots // 2
    strips = across // 2
    reply_shape = (LEVELS, row_count, plane_count, pairs, padded_rows, 2 * block_cells)
    ext_rows = band_rows + 2 * side
    dma = pltpu.SemaphoreType.DMA
    replies = pl.pallas_call(
        functools.partial(lookup_kernel, (row_count, plane_count, slots, channels**-0.5)),
        out_shape=jax.ShapeDtypeStruct(reply_shape, jnp.int16),
        in_specs=[pl.BlockSpec(memory_space=pl.ANY)] * 3,
        out_specs=pl.BlockSpec(memory_space=pl.ANY),
        scratch_shapes=[
            pltpu.VMEM((plane_count, frame_count, ext_rows, band_cols, channels), jnp.bfloat16),
            pltpu.VMEM((row_count, block_count, block_cells, channels), jnp.bfloat16),
            pltpu.VMEM(table.shape, jnp.int32),
            pltpu.SMEM(table.shape, jnp.int32),
            pltpu.VMEM((frame_count * (band_rows + side), across + 1, side, channels), jnp.float32),
            pltpu.VMEM(
                (frame_count * (band_rows // 2 + side), across // 2 + 1, side, channels),
                jnp.float32,
            ),
            pltpu.VMEM(
                (plane_count, frame_count, ext_rows // 2, band_cols // 2, channels), jnp.float32
            ),
            pltpu.VMEM((channels // 128, ext_rows // 2 * 2 * side, 128), jnp.float32),
            pltpu.VMEM((pairs, padded_rows, 2 * block_cells), jnp.float32),
            pltpu.VMEM(
                (plane_count, row_count, LEVELS, pairs, padded_rows, 2 * block_cells), jnp.int16
            ),
            dma((3,)),
            dma((2, plane_count, strips)),
            dma((plane_count, strips)),
            dma((2, plane_count, strips)),
            dma((2, plane_count, strips)),
            dma((14,)),
            dma((row_count, 2)),
            dma((row_count,)),
            dma((row_count,)),
            dma,
            dma((plane_count, row_count)),
            dma((plane_count, row_count)),
        ],
        compiler_params=pltpu.CompilerParams(
            collective_id=0, has_side_effects=True, vmem_limit_bytes=62 * 2**20
        ),
    )(fmap2, queries, table)
    spots = row_count * plane_count * pairs
    source_ids = owner * pairs + rank // 2
    joined = pl.pallas_call(
        functools.partial(join_kernel, block_count // 2, window_cells),
        out_shape=jax.ShapeDtypeStruct(
            (window_cells * block_count // 2 * LEVELS, 2 * block_cells), jnp.float32
        ),
        grid_spec=pltpu.PrefetchScalarGridSpec(
            num_scalar_prefetch=2,
            grid=(LEVELS,),
            in_specs=[
                pl.BlockSpec((1, spots, padded_rows, 2 * block_cells), lambda l, *_: (l, 0, 0, 0))
            ],
            out_specs=pl.BlockSpec(
                (window_cells * block_count // 2 * LEVELS, 2 * block_cells), lambda l, *_: (0, 0)
            ),
        ),
    )(
        source_ids.reshape(-1),
        (rank % 2).reshape(-1),
        replies.reshape(LEVELS, spots, padded_rows, 2 * block_cells),
    )
    joined = joined.reshape(window_cells, block_count // 2, LEVELS, 2 * block_cells)
    return joined.transpose(2, 0, 1, 3).reshape(LEVELS, window_cells, block_count * block_cells)


def solution(mesh):
    in_specs = (
        P(None, "rows", "cols", None),
        P(None, "rows", "cols", None),
        P(None, ("rows", "cols"), None),
        P(None, ("rows", "cols")),
    )
    out_specs = P(None, None, ("rows", "cols"))
    chosen_body = gathered_body if mesh.shape["rows"] == 8 else body
    return jax.shard_map(
        chosen_body, mesh=mesh, in_specs=in_specs, out_specs=out_specs, check_vma=False
    )
```

```python
import functools

import jax
import jax.numpy as jnp
from jax import lax
from jax.experimental import pallas as pl
from jax.experimental.pallas import tpu as pltpu
from jax.sharding import PartitionSpec as P

RADIUS = 4
LEVELS = 2
STEP_SLOTS = 16


def padded_2(block, sides, width):
    for axis, dim in sides:
        count = lax.axis_size(axis)
        forward = [(i, i + 1) for i in range(count - 1)]
        backward = [(target, source) for source, target in forward]
        low = lax.ppermute(
            lax.slice_in_dim(block, block.shape[dim] - width, None, axis=dim), axis, forward
        )
        high = lax.ppermute(lax.slice_in_dim(block, 0, width, axis=dim), axis, backward)
        block = jnp.concatenate([low, block, high], axis=dim)
    return block


def pool_level(level_map):
    frame_count, rows_in, cols_in, channels = level_map.shape
    pooled = level_map.astype(jnp.float32).reshape(
        frame_count, rows_in // 2, 2, cols_in // 2, 2, channels
    )
    return jnp.mean(pooled, axis=(2, 4)).astype(jnp.bfloat16)


def dispatch_kernel(slot_count, block_ref, query_ref, sent_ref):
    base = pl.program_id(0) * slot_count
    for slot in range(slot_count):
        sent_ref[slot] = query_ref[block_ref[base + slot]]


def correlate_kernel(plan, scale, label_ref, query_ref, map_ref, reply_ref):
    per_frame, col_count, padded_rows, across = plan
    tile_side = 2 * RADIUS
    span_side = 4 * RADIUS
    window_side = 2 * RADIUS + 1
    block_cells = tile_side * tile_side
    base = pl.program_id(0) * STEP_SLOTS
    lane = lax.broadcasted_iota(jnp.int32, (1, 1, 2 * block_cells), 2)
    query_row = lane % block_cells // tile_side
    query_col = lane[0] % tile_side
    is_first = lane[0] < block_cells

    def window(slot):
        label = label_ref[base + slot]
        tile = label % per_frame
        region = label // per_frame
        row = region // col_count * padded_rows + tile // across * tile_side
        col = (region % col_count * across + tile % across) * tile_side
        col = pl.multiple_of(col, tile_side)
        cells = map_ref[pl.ds(row, span_side), pl.ds(col, span_side), :]
        return cells.reshape(span_side * span_side, -1).astype(jnp.bfloat16)

    for pair in range(STEP_SLOTS // 2):
        queries = query_ref[2 * pair : 2 * pair + 2].reshape(2 * block_cells, -1)
        first, second = [
            lax.dot_general(
                window(2 * pair + half),
                queries,
                (((1,), (1,)), ((), ())),
                preferred_element_type=jnp.float32,
            )
            for half in range(2)
        ]
        scores = jnp.where(is_first, first, second)
        scores = scores.reshape(span_side, span_side, 2 * block_cells)
        for bit in (1, 2, 4):
            scores = jnp.where((query_row & bit) != 0, scores[bit:], scores[:-bit])
        flat = scores.reshape(window_side * span_side, 2 * block_cells)
        for bit in (1, 2, 4):
            moved = pltpu.roll(flat, flat.shape[0] - bit, 0)
            flat = jnp.where((query_col & bit) != 0, moved, flat)
        flat = flat * scale
        for a in range(window_side):
            at = (pair * window_side + a) * window_side
            reply_ref[at : at + window_side, :] = flat[
                a * span_side : a * span_side + window_side
            ]


def assemble_kernel(pair_count, source_ref, half_ref, *refs):
    reply_refs, out_ref = refs[:-1], refs[-1]
    window_cells, lanes = out_ref.shape[1], reply_refs[0].shape[1]
    is_first = lax.broadcasted_iota(jnp.int32, (window_cells, lanes), 1) < lanes // 2
    for level in range(LEVELS):

        def step(m, carry, level=level):
            at = 2 * (level * pair_count + m)
            picked = []
            for side in range(2):
                first_row = source_ref[at + side] * window_cells
                rows = reply_refs[level][pl.ds(first_row, window_cells), :]
                moved = pltpu.roll(rows, lanes // 2, 1)
                picked.append(jnp.where(half_ref[at + side] == side, rows, moved))
            spot = pl.ds(pl.multiple_of(m * lanes, lanes), lanes)
            out_ref[level, :, spot] = jnp.where(is_first, picked[0], picked[1])
            return carry

        lax.fori_loop(0, pair_count, step, 0)


def body(fmap1, fmap2, target_owner, target_tile):
    tile_side = 2 * RADIUS
    window_side = 2 * RADIUS + 1
    block_cells = tile_side * tile_side
    frame_count, band_rows, band_cols, channels = fmap1.shape
    row_count = lax.axis_size("rows")
    col_count = lax.axis_size("cols")
    device_count = row_count * col_count
    tiles_across = band_cols // tile_side
    per_frame = band_rows // tile_side * tiles_across
    block_count = frame_count * per_frame
    owner_slots = max(2, (2 * block_count + device_count - 1) // device_count)
    row_slots = -(-owner_slots * col_count // STEP_SLOTS) * STEP_SLOTS
    pair_slots = row_slots // 2
    queries = fmap1.reshape(
        frame_count, band_rows // tile_side, tile_side, tiles_across, tile_side, channels
    )
    queries = queries.transpose(0, 1, 3, 2, 4, 5).reshape(block_count, block_cells, channels)
    owner_ids = target_owner[:, :, 0]
    owner_rows = owner_ids // col_count
    peer_ids = jnp.arange(row_count, dtype=jnp.int32)
    owner_hits = (owner_rows[:, :, None] == peer_ids[None, None, :]).astype(jnp.int32)
    slot_rank = jnp.sum(owner_hits * (jnp.cumsum(owner_hits, axis=1) - 1), axis=2)
    block_ids = jnp.arange(block_count, dtype=jnp.int32)
    label_rows = []
    for level in range(LEVELS):
        tile_count = (band_rows >> level) // tile_side * ((band_cols >> level) // tile_side)
        regions = block_ids // per_frame * col_count + owner_ids[level] % col_count
        label_rows.append(regions * per_frame + target_tile[level] % tile_count)
    rank_ids = jnp.arange(row_slots, dtype=jnp.int32)
    rank_hits = (slot_rank[:, :, None] == rank_ids[None, None, :]).astype(jnp.int32)
    slot_hits = owner_hits[:, :, :, None] * rank_hits[:, :, None, :]

    def by_slot(values):
        table = jnp.sum(slot_hits * values[:, :, None, None], axis=1)
        return table.transpose(1, 0, 2)

    labels_sent = by_slot(jnp.stack(label_rows))
    blocks_sent = by_slot(jnp.broadcast_to(block_ids[None], owner_ids.shape))
    slot_block = (row_slots, block_cells, channels)
    slot_total = row_count * row_slots
    label_part = lax.all_to_all(labels_sent, "rows", split_axis=0, concat_axis=0, tiled=True)
    levels = [fmap2]
    for level in range(1, LEVELS):
        levels.append(pool_level(levels[-1]))
    window_cells = window_side * window_side
    step_block = (STEP_SLOTS, block_cells, channels)
    reply_block = (STEP_SLOTS // 2 * window_cells, 2 * block_cells)
    reply_tables = [None] * LEVELS
    earlier = None
    for level in reversed(range(LEVELS)):
        queries_sent = pl.pallas_call(
            functools.partial(dispatch_kernel, row_slots),
            out_shape=jax.ShapeDtypeStruct((slot_total,) + slot_block[1:], jnp.bfloat16),
            grid_spec=pltpu.PrefetchScalarGridSpec(
                num_scalar_prefetch=1,
                grid=(row_count,),
                in_specs=[pl.BlockSpec(queries.shape, lambda d, *_: (0, 0, 0))],
                out_specs=pl.BlockSpec(slot_block, lambda d, *_: (d, 0, 0)),
            ),
        )(blocks_sent[:, level].reshape(-1), queries)
        query_part = lax.all_to_all(
            queries_sent.reshape((row_count,) + slot_block),
            "rows",
            split_axis=0,
            concat_axis=0,
            tiled=True,
        )
        band = lax.all_gather(levels[level], "cols", axis=2, tiled=True)
        if earlier is not None:
            band = lax.optimization_barrier((band, earlier, query_part))[0]
        padded = padded_2(band, (("rows", 1),), RADIUS).astype(jnp.float32)
        padded = jnp.pad(padded, ((0, 0), (0, 0), (RADIUS, RADIUS), (0, 0)))
        level_map = padded.reshape((-1,) + padded.shape[2:])
        plan = (per_frame, col_count, padded.shape[1], levels[level].shape[2] // tile_side)
        replies = pl.pallas_call(
            functools.partial(correlate_kernel, plan, channels ** (-0.5)),
            out_shape=jax.ShapeDtypeStruct(
                (row_count * pair_slots * window_cells, 2 * block_cells), jnp.float32
            ),
            grid_spec=pltpu.PrefetchScalarGridSpec(
                num_scalar_prefetch=1,
                grid=(slot_total // STEP_SLOTS,),
                in_specs=[
                    pl.BlockSpec(step_block, lambda d, *_: (d, 0, 0)),
                    pl.BlockSpec(
                        level_map.shape, lambda d, *_: (0, 0, 0), pipeline_mode=pl.Buffered(1)
                    ),
                ],
                out_specs=pl.BlockSpec(reply_block, lambda d, *_: (d, 0)),
            ),
        )(
            label_part[:, level].reshape(-1),
            query_part.reshape((slot_total,) + slot_block[1:]),
            level_map,
        )
        returned = lax.all_to_all(
            replies.reshape(row_count, pair_slots * window_cells, 2 * block_cells),
            "rows",
            split_axis=0,
            concat_axis=0,
            tiled=True,
        )
        earlier = returned
        reply_tables[level] = returned.reshape(-1, 2 * block_cells)
    source_ids = owner_rows * pair_slots + slot_rank // 2
    return pl.pallas_call(
        functools.partial(assemble_kernel, block_count // 2),
        out_shape=jax.ShapeDtypeStruct(
            (LEVELS, window_cells, block_count * block_cells), jnp.float32
        ),
        in_specs=[
            pl.BlockSpec(memory_space=pltpu.SMEM),
            pl.BlockSpec(memory_space=pltpu.SMEM),
        ]
        + [pl.BlockSpec(memory_space=pltpu.VMEM)] * LEVELS,
        out_specs=pl.BlockSpec(memory_space=pltpu.VMEM),
    )(source_ids.reshape(-1), (slot_rank % 2).reshape(-1), *reply_tables)


MESH = pl.DeviceIdType.MESH
TOP = 32000.0


def flipped(index, bit):
    return index + bit - 2 * bit * (index // bit % 2)


def lookup_kernel(
    plan,
    f2_hbm,
    q_hbm,
    owner_ref,
    tile_ref,
    rep_out,
    idx_out,
    f2x,
    f1a,
    tab_made,
    tabv,
    tabs,
    map0,
    map1,
    p1x,
    tmp,
    line,
    reps,
    loc_sem,
    zs_sem,
    zr_sem,
    hs_sem,
    hr_sem,
    fs_sem,
    fr_sem,
    ts_sem,
    tr_sem,
    tl_sem,
    rs_sem,
    rr_sem,
):
    row_count, plane_count, slots, scale = plan
    frame_count, band_rows, band_cols, channels = f2_hbm.shape
    side = 2 * RADIUS
    subs, across = band_rows // side, band_cols // side
    per_frame = subs * across
    block_count, block_cells = frame_count * per_frame, side * side
    span = 4 * RADIUS
    wside = 2 * RADIUS + 1
    wide = 2 * side
    strips = band_cols // wide
    half_blocks = block_count // 2
    r = lax.axis_index("rows")
    c = lax.axis_index("cols")
    last_r, last_c = row_count - 1, plane_count - 1

    barrier = pltpu.get_barrier_semaphore()
    for k in range(1, row_count):
        pl.semaphore_signal(
            barrier, inc=1, device_id=((r + k) % row_count, c), device_id_type=MESH
        )

    @pl.when(c > 0)
    def _():
        pl.semaphore_signal(barrier, inc=1, device_id=(r, c - 1), device_id_type=MESH)

    @pl.when(c < last_c)
    def _():
        pl.semaphore_signal(barrier, inc=1, device_id=(r, c + 1), device_id_type=MESH)

    has_left = jnp.where(c > 0, 1, 0)
    has_right = jnp.where(c < last_c, 1, 0)
    pl.semaphore_wait(barrier, row_count - 1 + has_left + has_right)

    def strip(at, way):
        return at if way == 0 else strips - 1 - at

    def z_copy(b, at, way, own=False):
        cols = pl.ds(strip(at, way) * wide, wide)
        here = f2x.at[b, :, pl.ds(side, band_rows), cols]
        return pltpu.make_async_remote_copy(
            src_ref=f2_hbm.at[:, :, cols] if own else here,
            dst_ref=here,
            send_sem=zs_sem.at[way, b, at],
            recv_sem=zr_sem.at[b, at],
            device_id=(r, c - 1 if way == 0 else c + 1),
            device_id_type=MESH,
        )

    def halo_copy(b, at, way, up, own=False):
        cols = pl.ds(strip(at, way) * wide, wide)
        first = 0 if up else band_rows - side
        into = band_rows + side if up else 0
        if own:
            source = f2_hbm.at[:, pl.ds(first, side), cols]
        else:
            source = f2x.at[b, :, pl.ds(first + side, side), cols]
        lane = 0 if up else 1
        return pltpu.make_async_remote_copy(
            src_ref=source,
            dst_ref=f2x.at[b, :, pl.ds(into, side), cols],
            send_sem=hs_sem.at[lane, b, at],
            recv_sem=hr_sem.at[lane, b, at],
            device_id=(r - 1 if up else r + 1, c),
            device_id_type=MESH,
        )

    def send_halo(b, at, way, own=False):
        @pl.when(r > 0)
        def _():
            halo_copy(b, at, way, True, own).start()

        @pl.when(r < last_r)
        def _():
            halo_copy(b, at, way, False, own).start()

    def f1_copy(index, row, half, bit):
        part = pl.ds(half * half_blocks, half_blocks)
        return pltpu.make_async_remote_copy(
            src_ref=f1a.at[row, part],
            dst_ref=f1a.at[row, part],
            send_sem=fs_sem.at[index],
            recv_sem=fr_sem.at[row, half],
            device_id=(flipped(r, bit), c),
            device_id_type=MESH,
        )

    def tab_copy(k):
        return pltpu.make_async_remote_copy(
            src_ref=tab_made.at[(r + k) % row_count],
            dst_ref=tabv.at[r],
            send_sem=ts_sem.at[k],
            recv_sem=tr_sem.at[k],
            device_id=((r + k) % row_count, c),
            device_id_type=MESH,
        )

    def rep_copy(b, k):
        s = (r + k) % row_count
        return pltpu.make_async_remote_copy(
            src_ref=reps.at[b, s],
            dst_ref=rep_out.at[:, r, b],
            send_sem=rs_sem.at[b, k],
            recv_sem=rr_sem.at[b, k],
            device_id=(s, c),
            device_id_type=MESH,
        )

    def rep_local(b):
        return pltpu.make_async_copy(reps.at[b, r], rep_out.at[:, r, b], rs_sem.at[b, 0])

    x_row, y_row, d_row = flipped(r, 2), flipped(r, 4), flipped(flipped(r, 2), 4)
    f1_first = [(0, r, 0, 2), (1, r, 0, 4), (2, r, 1, 2), (3, r, 1, 4), (4, r, 0, 1), (5, r, 1, 1)]
    f1_second = [
        (6, x_row, 0, 4),
        (7, y_row, 1, 2),
        (8, x_row, 0, 1),
        (9, x_row, 1, 1),
        (10, y_row, 0, 1),
        (11, y_row, 1, 1),
    ]
    f1_third = [(12, d_row, 0, 1), (13, d_row, 1, 1)]

    def whole_part(values, unit):
        return jnp.floor((values + 0.5) * (1.0 / unit))

    def make_tables():
        ids = lax.broadcasted_iota(jnp.int32, (block_count, block_count), 0).astype(jnp.float32)
        lanes = lax.broadcasted_iota(jnp.int32, (block_count, block_count), 1).astype(jnp.float32)
        block = lanes[:1]
        spots = lax.broadcasted_iota(
            jnp.int32, (block_count, tab_made.shape[2]), 1
        ).astype(jnp.float32)
        peers = lax.broadcasted_iota(jnp.int32, (row_count, block_count), 0).astype(jnp.float32)

        def upright(line_values):
            return jnp.sum(jnp.where(ids == lanes, line_values, 0.0), axis=1, keepdims=True)

        tab_made[...] = jnp.zeros(tab_made.shape, tab_made.dtype)
        idx_out[...] = jnp.zeros(idx_out.shape, idx_out.dtype)
        totals = [0.0, 0.0, 0.0]
        for level in range(LEVELS):
            owner = owner_ref[level].astype(jnp.float32)
            tile = tile_ref[level : level + 1].astype(jnp.float32)
            level_across = across >> level
            tiles = (subs >> level) * level_across
            tile = tile - whole_part(tile, tiles) * tiles
            tile_row = whole_part(tile, level_across)
            same = jnp.where((upright(owner) == owner) & (ids < lanes), 1.0, 0.0)
            rank = jnp.sum(same, axis=0, keepdims=True)
            towards = whole_part(owner, plane_count)
            plane = owner - towards * plane_count
            place = (plane * LEVELS + level) * slots + rank
            map_rows = (band_rows >> level) + side
            values = [
                block,
                whole_part(block, per_frame) * map_rows + tile_row * side,
                tile - tile_row * level_across,
            ]
            place = jnp.where(rank < slots, place, -1.0)
            chosen = jnp.where(upright(place) == spots, 1.0, 0.0).astype(jnp.bfloat16)
            for at, value in enumerate(values):
                named = jnp.where(peers == towards, value, 0.0).astype(jnp.bfloat16)
                totals[at] += jnp.dot(named, chosen, preferred_element_type=jnp.float32)
            rank = jnp.minimum(rank, slots - 1.0)
            pair = whole_part(rank, 2)
            source = (owner * (slots // 2) + pair).astype(jnp.int32)
            idx_out[level : level + 1, :block_count] = source
            half = (rank - 2 * pair).astype(jnp.int32)
            idx_out[LEVELS + level : LEVELS + level + 1, :block_count] = half
        for at, total in enumerate(totals):
            total = total.astype(jnp.int32)
            for peer in range(row_count):
                tab_made[peer, at : at + 1, :] = total[peer : peer + 1]

    loc_f2 = pltpu.make_async_copy(f2_hbm, f2x.at[c, :, pl.ds(side, band_rows)], loc_sem.at[0])
    loc_tab = pltpu.make_async_copy(tab_made.at[r], tabv.at[r], loc_sem.at[2])

    def loc_q(k):
        f, at = k // per_frame, k % per_frame
        cut = q_hbm.at[f, at // across, :, at % across]
        return pltpu.make_async_copy(cut, f1a.at[r, k], loc_sem.at[1])

    def start_q(k, carry):
        loc_q(k).start()
        return carry

    for at in range(strips):

        @pl.when(c > 0)
        def _():
            z_copy(c, at, 0, True).start()

        @pl.when(c < last_c)
        def _():
            z_copy(c, at, 1, True).start()

    lax.fori_loop(0, block_count, start_q, 0)
    loc_f2.start()
    make_tables()
    pltpu.make_async_copy(f1a.at[r], f1a.at[r], loc_sem.at[1]).wait()
    for item in f1_first:
        f1_copy(*item).start()
    for at in range(strips):
        send_halo(c, at, 0, True)
    for k in range(1, row_count):
        tab_copy(k).start()
    loc_tab.start()

    @pl.when(r == 0)
    def _():
        f2x[:, :, 0:side] = jnp.zeros((plane_count, frame_count, side) + f2x.shape[3:], f2x.dtype)

    @pl.when(r == last_r)
    def _():
        f2x[:, :, band_rows + side :] = jnp.zeros(
            (plane_count, frame_count, side) + f2x.shape[3:], f2x.dtype
        )

    def each_side(step, act):
        @pl.when(c + step <= last_c)
        def _():
            act(c + step, 0)

        if step > 0:

            @pl.when(c - step >= 0)
            def _():
                act(c - step, 1)

    def take(step, at):
        def act(b, way):
            z_copy(b, at, way).wait_recv()

            @pl.when(c > 0 if way == 0 else c < last_c)
            def _():
                z_copy(b, at, way).start()

            send_halo(b, at, way)

        each_side(step, act)

    def pool(step, ats):
        def act(b, way):
            for at in ats:

                @pl.when(r > 0)
                def _():
                    halo_copy(b, at, way, False).wait_recv()

                @pl.when(r < last_r)
                def _():
                    halo_copy(b, at, way, True).wait_recv()

            rows = p1x.shape[2]
            for at in ats:
                col = strip(at, way)

                def pool_row(t, carry):
                    f, i = t // rows, t % rows
                    pair = f2x[b, f, pl.ds(2 * i, 2), col * wide : (col + 1) * wide]
                    pair = pair.astype(jnp.float32)
                    both = pair[0] + pair[1]
                    for lane in range(channels // 128):
                        tmp[lane, pl.ds(i * wide, wide), :] = both[:, lane * 128 : (lane + 1) * 128]
                    for lane in range(channels // 128):
                        even = tmp[lane, pl.ds(i * wide, side, stride=2), :]
                        odd = tmp[lane, pl.ds(i * wide + 1, side, stride=2), :]
                        p1x[
                            b, f, i, col * side : (col + 1) * side, lane * 128 : (lane + 1) * 128
                        ] = (even + odd) * 0.25
                    return carry

                lax.fori_loop(0, frame_count * rows, pool_row, 0, unroll=4)

        each_side(step, act)

    lane_id = lax.broadcasted_iota(jnp.int32, (1, 1, 2 * block_cells), 2)
    query_row = lane_id % block_cells // side
    query_col = lane_id[0] % side
    is_first = lane_id[0] < block_cells
    row_id = lax.broadcasted_iota(jnp.int32, line.shape[2:], 0)
    line[...] = jnp.zeros(line.shape, line.dtype)

    def build(b, level):
        into = (map0, map1)[level]
        width = band_cols >> level
        rows = into.shape[0] // frame_count
        left_b, right_b = jnp.maximum(b - 1, 0), jnp.minimum(b + 1, last_c)

        def build_row(t, carry):
            f, y = t // rows, t % rows
            if level == 0:
                at = y + RADIUS
                left = f2x[left_b, f, at, width - 2 * side :, :].astype(jnp.float32)[side:]
                middle = f2x[b, f, at].astype(jnp.float32)
                right = f2x[right_b, f, at, : 2 * side, :].astype(jnp.float32)[:side]
            else:
                left = p1x[left_b, f, y, width - side :, :]
                middle = p1x[b, f, y]
                right = p1x[right_b, f, y, :side, :]
            left = jnp.where(b > 0, left, 0.0)
            right = jnp.where(b < last_c, right, 0.0)
            whole = jnp.concatenate([left, middle, right], axis=0)
            whole = pltpu.roll(whole, whole.shape[0] - RADIUS, 0)
            into[t] = whole[: width + side].reshape(into.shape[1:])
            return carry

        lax.fori_loop(0, into.shape[0], build_row, 0)

    def score_pair(b, s, level, pair):
        from_map = (map0, map1)[level]
        windows, queries = [], []
        for half in range(2):
            at = (b * LEVELS + level) * slots + 2 * pair + half
            k, row = jnp.clip(tabs[s, 0, at], 0, block_count - 1), jnp.clip(tabs[s, 1, at], 0, from_map.shape[0] - span)
            cells = from_map[pl.ds(row, span), pl.ds(jnp.clip(tabs[s, 2, at], 0, from_map.shape[1] - 2), 2)]
            windows.append(cells.reshape(span * span, channels).astype(jnp.bfloat16))
            queries.append(f1a[s, k].astype(jnp.float32).reshape(block_cells, channels))
        queries = jnp.concatenate(queries, axis=0).astype(jnp.bfloat16)
        first, second = [
            lax.dot_general(
                window, queries, (((1,), (1,)), ((), ())), preferred_element_type=jnp.float32
            )
            for window in windows
        ]
        scores = jnp.where(is_first, first, second).reshape(span, span, 2 * block_cells)
        for bit in (1, 2, 4):
            scores = jnp.where((query_row & bit) != 0, scores[bit:], scores[:-bit])
        flat = scores.reshape(wside * span, 2 * block_cells)
        for bit in (1, 2, 4):
            moved = pltpu.roll(flat, flat.shape[0] - bit, 0)
            flat = jnp.where((query_col & bit) != 0, moved, flat)
        flat = flat * scale
        for a in range(wside):
            line[level, pair, a * wside : (a + 1) * wside, :] = flat[a * span : a * span + wside]
        found = line[level, pair]
        top = jnp.max(jnp.abs(found), axis=0, keepdims=True)
        power = jnp.maximum(jnp.ceil(jnp.log2(top)), -100.0)
        coded = jnp.floor(found * (TOP * jnp.exp2(-power)) + 0.5)
        coded = jnp.where(row_id == wside * wside, power, coded)
        reps[b, s, level, pair] = coded.astype(jnp.int32).astype(jnp.int16)

    def process(b, way):
        for level in range(LEVELS):
            build(b, level)

        def source(k, inner):
            s = (r + k) % row_count
            for level in range(LEVELS):
                for pair in range(slots // 2):
                    score_pair(b, s, level, pair)

            @pl.when(k == 0)
            def _():
                rep_local(b).start()

            @pl.when(k > 0)
            def _():
                rep_copy(b, k).start()

            return inner

        lax.fori_loop(0, row_count, source, 0)

    for at in range(strips):
        take(1, at)
    for item in f1_second:
        index, row, half, bit = item
        if index in (6, 7, 9, 10):
            f1_copy(*item).wait_recv()
        f1_copy(*item).start()
    for at in range(strips - 1):
        take(2, at)
    for item in f1_third:
        f1_copy(*item).wait_recv()
        f1_copy(*item).start()
    for bits in ((1,), (1, 2), (1, 4), (1, 2, 4)):
        row = r
        for bit in bits:
            row = flipped(row, bit)
        for half in range(2):
            f1_copy(0, row, half, 1).wait_recv()
    for k in range(1, row_count):
        tab_copy(k).wait_recv()
    loc_tab.wait()
    loc_f2.wait()
    tab_smem = pltpu.make_async_copy(tabv, tabs, tl_sem)
    tab_smem.start()
    tab_smem.wait()
    near, rest = [0], list(range(1, strips))
    pool(0, near + rest)
    pool(1, near)
    each_side(0, process)
    take(2, strips - 1)
    for step in range(1, plane_count):
        if step > 2:
            for at in rest:
                take(step, at)
        if step >= 2 and step + 1 < plane_count:
            take(step + 1, 0)
        pool(step, rest)
        if step + 1 < plane_count:
            pool(step + 1, near)
        each_side(step, process)

    for at in range(strips):

        @pl.when(c < last_c)
        def _():
            z_copy(c, at, 1).wait_send()

    for step in range(plane_count):

        def sent(b, way):
            for at in range(strips):

                @pl.when(c > 0 if way == 0 else c < last_c)
                def _():
                    z_copy(b, at, way).wait_send()

                @pl.when(r > 0)
                def _():
                    halo_copy(b, at, way, True).wait_send()

                @pl.when(r < last_r)
                def _():
                    halo_copy(b, at, way, False).wait_send()

        each_side(step, sent)

    def plane_end(b, carry):
        rep_local(b).wait()

        def peer_end(k, inner):
            rep_copy(b, k).wait_send()
            rep_copy(b, k).wait_recv()
            return inner

        lax.fori_loop(1, row_count, peer_end, 0)
        return carry

    lax.fori_loop(0, plane_count, plane_end, 0)
    for item in f1_first + f1_second + f1_third:
        f1_copy(*item).wait_send()
    for k in range(1, row_count):
        tab_copy(k).wait_send()


def join_kernel(group, index_ref, reply_ref, out_ref):
    window_cells = out_ref.shape[0]
    padded_rows, lanes = reply_ref.shape[-2:]
    is_first = lax.broadcasted_iota(jnp.int32, (padded_rows, lanes), 1) < lanes // 2
    base = pl.program_id(0) * group * 2
    for m in range(group):
        for level in range(LEVELS):
            picked = []
            for side in range(2):
                at = base + 2 * m + side
                rows = reply_ref[level, index_ref[level, at]].astype(jnp.int32)
                turn = (index_ref[LEVELS + level, at] + side) % 2 * (lanes // 2)
                picked.append(pltpu.roll(rows.astype(jnp.float32), turn, 1))
            both = jnp.where(is_first, picked[0], picked[1])
            unit = jnp.exp2(both[window_cells : window_cells + 1]) * (1.0 / TOP)
            out_ref[:, m * LEVELS + level, :] = both[:window_cells] * unit


def gathered_body(fmap1, fmap2, target_owner, target_tile):
    side = 2 * RADIUS
    window_cells = (2 * RADIUS + 1) ** 2
    frame_count, band_rows, band_cols, channels = fmap1.shape
    row_count = lax.axis_size("rows")
    plane_count = lax.axis_size("cols")
    device_count = row_count * plane_count
    subs, across = band_rows // side, band_cols // side
    per_frame = subs * across
    block_count = frame_count * per_frame
    block_cells = side * side
    slots = max(2, (2 * block_count + device_count - 1) // device_count)
    queries = fmap1.reshape(frame_count, subs, side, across, side, channels)
    owner = target_owner.transpose(0, 2, 1)
    lanes_used = -(-plane_count * LEVELS * slots // 128) * 128
    table = (row_count, 8, lanes_used)
    padded_rows = -(-(window_cells + 1) // 16) * 16
    pairs = slots // 2
    strips = across // 2
    reply_shape = (LEVELS, row_count, plane_count, pairs, padded_rows, 2 * block_cells)
    ext_rows = band_rows + 2 * side
    dma = pltpu.SemaphoreType.DMA
    replies, index = pl.pallas_call(
        functools.partial(lookup_kernel, (row_count, plane_count, slots, channels**-0.5)),
        out_shape=[
            jax.ShapeDtypeStruct(reply_shape, jnp.int16),
            jax.ShapeDtypeStruct((8, 128), jnp.int32),
        ],
        in_specs=[pl.BlockSpec(memory_space=pl.ANY)] * 2
        + [pl.BlockSpec(memory_space=pltpu.VMEM)] * 2,
        out_specs=[
            pl.BlockSpec(memory_space=pl.ANY),
            pl.BlockSpec(memory_space=pltpu.VMEM),
        ],
        scratch_shapes=[
            pltpu.VMEM((plane_count, frame_count, ext_rows, band_cols, channels), jnp.bfloat16),
            pltpu.VMEM((row_count, block_count, side, side, channels), jnp.bfloat16),
            pltpu.VMEM(table, jnp.int32),
            pltpu.VMEM(table, jnp.int32),
            pltpu.SMEM(table, jnp.int32),
            pltpu.VMEM((frame_count * (band_rows + side), across + 1, side, channels), jnp.float32),
            pltpu.VMEM(
                (frame_count * (band_rows // 2 + side), across // 2 + 1, side, channels),
                jnp.float32,
            ),
            pltpu.VMEM(
                (plane_count, frame_count, ext_rows // 2, band_cols // 2, channels), jnp.float32
            ),
            pltpu.VMEM((channels // 128, ext_rows // 2 * 2 * side, 128), jnp.float32),
            pltpu.VMEM((LEVELS, pairs, padded_rows, 2 * block_cells), jnp.float32),
            pltpu.VMEM(
                (plane_count, row_count, LEVELS, pairs, padded_rows, 2 * block_cells), jnp.int16
            ),
            dma((3,)),
            dma((2, plane_count, strips)),
            dma((plane_count, strips)),
            dma((2, plane_count, strips)),
            dma((2, plane_count, strips)),
            dma((14,)),
            dma((row_count, 2)),
            dma((row_count,)),
            dma((row_count,)),
            dma,
            dma((plane_count, row_count)),
            dma((plane_count, row_count)),
        ],
        compiler_params=pltpu.CompilerParams(
            collective_id=0, has_side_effects=True, vmem_limit_bytes=62 * 2**20
        ),
    )(fmap2, queries, owner, target_tile)
    spots = row_count * plane_count * pairs
    group = 8 // LEVELS
    joined = pl.pallas_call(
        functools.partial(join_kernel, group),
        out_shape=jax.ShapeDtypeStruct(
            (window_cells, block_count // 2 * LEVELS, 2 * block_cells), jnp.float32
        ),
        grid=(block_count // 2 // group,),
        in_specs=[
            pl.BlockSpec(memory_space=pltpu.SMEM),
            pl.BlockSpec((LEVELS, spots, padded_rows, 2 * block_cells), lambda g: (0, 0, 0, 0)),
        ],
        out_specs=pl.BlockSpec(
            (window_cells, group * LEVELS, 2 * block_cells), lambda g: (0, g, 0)
        ),
    )(index, replies.reshape(LEVELS, spots, padded_rows, 2 * block_cells))
    joined = joined.reshape(window_cells, block_count // 2, LEVELS, 2 * block_cells)
    return joined.transpose(2, 0, 1, 3).reshape(LEVELS, window_cells, block_count * block_cells)


def solution(mesh):
    in_specs = (
        P(None, "rows", "cols", None),
        P(None, "rows", "cols", None),
        P(None, ("rows", "cols"), None),
        P(None, ("rows", "cols")),
    )
    out_specs = P(None, None, ("rows", "cols"))
    chosen_body = gathered_body if mesh.shape["rows"] == 8 else body
    return jax.shard_map(
        chosen_body, mesh=mesh, in_specs=in_specs, out_specs=out_specs, check_vma=False
    )
```

```python
import functools

import jax
import jax.numpy as jnp
from jax import lax
from jax.experimental import pallas as pl
from jax.experimental.pallas import tpu as pltpu
from jax.sharding import PartitionSpec as P

RADIUS = 4
LEVELS = 2
STEP_SLOTS = 16


def padded_2(block, sides, width):
    for axis, dim in sides:
        count = lax.axis_size(axis)
        forward = [(i, i + 1) for i in range(count - 1)]
        backward = [(target, source) for source, target in forward]
        low = lax.ppermute(
            lax.slice_in_dim(block, block.shape[dim] - width, None, axis=dim), axis, forward
        )
        high = lax.ppermute(lax.slice_in_dim(block, 0, width, axis=dim), axis, backward)
        block = jnp.concatenate([low, block, high], axis=dim)
    return block


def pool_level(level_map):
    frame_count, rows_in, cols_in, channels = level_map.shape
    pooled = level_map.astype(jnp.float32).reshape(
        frame_count, rows_in // 2, 2, cols_in // 2, 2, channels
    )
    return jnp.mean(pooled, axis=(2, 4)).astype(jnp.bfloat16)


def dispatch_kernel(slot_count, block_ref, query_ref, sent_ref):
    base = pl.program_id(0) * slot_count
    for slot in range(slot_count):
        sent_ref[slot] = query_ref[block_ref[base + slot]]


def correlate_kernel(plan, scale, label_ref, query_ref, map_ref, reply_ref):
    per_frame, col_count, padded_rows, across = plan
    tile_side = 2 * RADIUS
    span_side = 4 * RADIUS
    window_side = 2 * RADIUS + 1
    block_cells = tile_side * tile_side
    base = pl.program_id(0) * STEP_SLOTS
    lane = lax.broadcasted_iota(jnp.int32, (1, 1, 2 * block_cells), 2)
    query_row = lane % block_cells // tile_side
    query_col = lane[0] % tile_side
    is_first = lane[0] < block_cells

    def window(slot):
        label = label_ref[base + slot]
        tile = label % per_frame
        region = label // per_frame
        row = region // col_count * padded_rows + tile // across * tile_side
        col = (region % col_count * across + tile % across) * tile_side
        col = pl.multiple_of(col, tile_side)
        cells = map_ref[pl.ds(row, span_side), pl.ds(col, span_side), :]
        return cells.reshape(span_side * span_side, -1).astype(jnp.bfloat16)

    for pair in range(STEP_SLOTS // 2):
        queries = query_ref[2 * pair : 2 * pair + 2].reshape(2 * block_cells, -1)
        first, second = [
            lax.dot_general(
                window(2 * pair + half),
                queries,
                (((1,), (1,)), ((), ())),
                preferred_element_type=jnp.float32,
            )
            for half in range(2)
        ]
        scores = jnp.where(is_first, first, second)
        scores = scores.reshape(span_side, span_side, 2 * block_cells)
        for bit in (1, 2, 4):
            scores = jnp.where((query_row & bit) != 0, scores[bit:], scores[:-bit])
        flat = scores.reshape(window_side * span_side, 2 * block_cells)
        for bit in (1, 2, 4):
            moved = pltpu.roll(flat, flat.shape[0] - bit, 0)
            flat = jnp.where((query_col & bit) != 0, moved, flat)
        flat = flat * scale
        for a in range(window_side):
            at = (pair * window_side + a) * window_side
            reply_ref[at : at + window_side, :] = flat[
                a * span_side : a * span_side + window_side
            ]


def assemble_kernel(pair_count, source_ref, half_ref, *refs):
    reply_refs, out_ref = refs[:-1], refs[-1]
    window_cells, lanes = out_ref.shape[1], reply_refs[0].shape[1]
    is_first = lax.broadcasted_iota(jnp.int32, (window_cells, lanes), 1) < lanes // 2
    for level in range(LEVELS):

        def step(m, carry, level=level):
            at = 2 * (level * pair_count + m)
            picked = []
            for side in range(2):
                first_row = source_ref[at + side] * window_cells
                rows = reply_refs[level][pl.ds(first_row, window_cells), :]
                moved = pltpu.roll(rows, lanes // 2, 1)
                picked.append(jnp.where(half_ref[at + side] == side, rows, moved))
            spot = pl.ds(pl.multiple_of(m * lanes, lanes), lanes)
            out_ref[level, :, spot] = jnp.where(is_first, picked[0], picked[1])
            return carry

        lax.fori_loop(0, pair_count, step, 0)


def body(fmap1, fmap2, target_owner, target_tile):
    tile_side = 2 * RADIUS
    window_side = 2 * RADIUS + 1
    block_cells = tile_side * tile_side
    frame_count, band_rows, band_cols, channels = fmap1.shape
    row_count = lax.axis_size("rows")
    col_count = lax.axis_size("cols")
    device_count = row_count * col_count
    tiles_across = band_cols // tile_side
    per_frame = band_rows // tile_side * tiles_across
    block_count = frame_count * per_frame
    owner_slots = max(2, (2 * block_count + device_count - 1) // device_count)
    row_slots = -(-owner_slots * col_count // STEP_SLOTS) * STEP_SLOTS
    pair_slots = row_slots // 2
    queries = fmap1.reshape(
        frame_count, band_rows // tile_side, tile_side, tiles_across, tile_side, channels
    )
    queries = queries.transpose(0, 1, 3, 2, 4, 5).reshape(block_count, block_cells, channels)
    owner_ids = target_owner[:, :, 0]
    owner_rows = owner_ids // col_count
    peer_ids = jnp.arange(row_count, dtype=jnp.int32)
    owner_hits = (owner_rows[:, :, None] == peer_ids[None, None, :]).astype(jnp.int32)
    slot_rank = jnp.sum(owner_hits * (jnp.cumsum(owner_hits, axis=1) - 1), axis=2)
    block_ids = jnp.arange(block_count, dtype=jnp.int32)
    label_rows = []
    for level in range(LEVELS):
        tile_count = (band_rows >> level) // tile_side * ((band_cols >> level) // tile_side)
        regions = block_ids // per_frame * col_count + owner_ids[level] % col_count
        label_rows.append(regions * per_frame + target_tile[level] % tile_count)
    rank_ids = jnp.arange(row_slots, dtype=jnp.int32)
    rank_hits = (slot_rank[:, :, None] == rank_ids[None, None, :]).astype(jnp.int32)
    slot_hits = owner_hits[:, :, :, None] * rank_hits[:, :, None, :]

    def by_slot(values):
        table = jnp.sum(slot_hits * values[:, :, None, None], axis=1)
        return table.transpose(1, 0, 2)

    labels_sent = by_slot(jnp.stack(label_rows))
    blocks_sent = by_slot(jnp.broadcast_to(block_ids[None], owner_ids.shape))
    slot_block = (row_slots, block_cells, channels)
    slot_total = row_count * row_slots
    label_part = lax.all_to_all(labels_sent, "rows", split_axis=0, concat_axis=0, tiled=True)
    levels = [fmap2]
    for level in range(1, LEVELS):
        levels.append(pool_level(levels[-1]))
    window_cells = window_side * window_side
    step_block = (STEP_SLOTS, block_cells, channels)
    reply_block = (STEP_SLOTS // 2 * window_cells, 2 * block_cells)
    reply_tables = [None] * LEVELS
    earlier = None
    for level in reversed(range(LEVELS)):
        queries_sent = pl.pallas_call(
            functools.partial(dispatch_kernel, row_slots),
            out_shape=jax.ShapeDtypeStruct((slot_total,) + slot_block[1:], jnp.bfloat16),
            grid_spec=pltpu.PrefetchScalarGridSpec(
                num_scalar_prefetch=1,
                grid=(row_count,),
                in_specs=[pl.BlockSpec(queries.shape, lambda d, *_: (0, 0, 0))],
                out_specs=pl.BlockSpec(slot_block, lambda d, *_: (d, 0, 0)),
            ),
        )(blocks_sent[:, level].reshape(-1), queries)
        query_part = lax.all_to_all(
            queries_sent.reshape((row_count,) + slot_block),
            "rows",
            split_axis=0,
            concat_axis=0,
            tiled=True,
        )
        band = lax.all_gather(levels[level], "cols", axis=2, tiled=True)
        if earlier is not None:
            band = lax.optimization_barrier((band, earlier, query_part))[0]
        padded = padded_2(band, (("rows", 1),), RADIUS).astype(jnp.float32)
        padded = jnp.pad(padded, ((0, 0), (0, 0), (RADIUS, RADIUS), (0, 0)))
        level_map = padded.reshape((-1,) + padded.shape[2:])
        plan = (per_frame, col_count, padded.shape[1], levels[level].shape[2] // tile_side)
        replies = pl.pallas_call(
            functools.partial(correlate_kernel, plan, channels ** (-0.5)),
            out_shape=jax.ShapeDtypeStruct(
                (row_count * pair_slots * window_cells, 2 * block_cells), jnp.float32
            ),
            grid_spec=pltpu.PrefetchScalarGridSpec(
                num_scalar_prefetch=1,
                grid=(slot_total // STEP_SLOTS,),
                in_specs=[
                    pl.BlockSpec(step_block, lambda d, *_: (d, 0, 0)),
                    pl.BlockSpec(
                        level_map.shape, lambda d, *_: (0, 0, 0), pipeline_mode=pl.Buffered(1)
                    ),
                ],
                out_specs=pl.BlockSpec(reply_block, lambda d, *_: (d, 0)),
            ),
        )(
            label_part[:, level].reshape(-1),
            query_part.reshape((slot_total,) + slot_block[1:]),
            level_map,
        )
        returned = lax.all_to_all(
            replies.reshape(row_count, pair_slots * window_cells, 2 * block_cells),
            "rows",
            split_axis=0,
            concat_axis=0,
            tiled=True,
        )
        earlier = returned
        reply_tables[level] = returned.reshape(-1, 2 * block_cells)
    source_ids = owner_rows * pair_slots + slot_rank // 2
    return pl.pallas_call(
        functools.partial(assemble_kernel, block_count // 2),
        out_shape=jax.ShapeDtypeStruct(
            (LEVELS, window_cells, block_count * block_cells), jnp.float32
        ),
        in_specs=[
            pl.BlockSpec(memory_space=pltpu.SMEM),
            pl.BlockSpec(memory_space=pltpu.SMEM),
        ]
        + [pl.BlockSpec(memory_space=pltpu.VMEM)] * LEVELS,
        out_specs=pl.BlockSpec(memory_space=pltpu.VMEM),
    )(source_ids.reshape(-1), (slot_rank % 2).reshape(-1), *reply_tables)


MESH = pl.DeviceIdType.MESH
TOP = 32000.0


def flipped(index, bit):
    return index + bit - 2 * bit * (index // bit % 2)


def lookup_kernel(
    plan,
    f2_hbm,
    q_hbm,
    owner_ref,
    tile_ref,
    rep_out,
    idx_out,
    f2x,
    f1a,
    tab_made,
    tabv,
    tabs,
    map0,
    map1,
    p1x,
    tmp,
    line,
    reps,
    loc_sem,
    zs_sem,
    zr_sem,
    hs_sem,
    hr_sem,
    fs_sem,
    fr_sem,
    ts_sem,
    tr_sem,
    tl_sem,
    rs_sem,
    rr_sem,
):
    row_count, plane_count, slots, scale = plan
    frame_count, band_rows, band_cols, channels = f2_hbm.shape
    side = 2 * RADIUS
    subs, across = band_rows // side, band_cols // side
    per_frame = subs * across
    block_count, block_cells = frame_count * per_frame, side * side
    span = 4 * RADIUS
    wside = 2 * RADIUS + 1
    wide = 2 * side
    strips = band_cols // wide
    half_blocks = block_count // 2
    r = lax.axis_index("rows")
    c = lax.axis_index("cols")
    last_r, last_c = row_count - 1, plane_count - 1

    barrier = pltpu.get_barrier_semaphore()
    for k in range(1, row_count):
        pl.semaphore_signal(
            barrier, inc=1, device_id=((r + k) % row_count, c), device_id_type=MESH
        )

    @pl.when(c > 0)
    def _():
        pl.semaphore_signal(barrier, inc=1, device_id=(r, c - 1), device_id_type=MESH)

    @pl.when(c < last_c)
    def _():
        pl.semaphore_signal(barrier, inc=1, device_id=(r, c + 1), device_id_type=MESH)

    has_left = jnp.where(c > 0, 1, 0)
    has_right = jnp.where(c < last_c, 1, 0)
    pl.semaphore_wait(barrier, row_count - 1 + has_left + has_right)

    def strip(at, way):
        p = at + way * (strips - 1 - 2 * at)
        return p, pl.ds(pl.multiple_of(p * wide, wide), wide)

    whole_strip = (0, band_rows)
    last_pieces = [
        (strips - 1, (0, side)),
        (strips, (band_rows - side, side)),
        (strips + 1, (side, band_rows - 2 * side)),
    ]

    def z_copy(b, number, way, rows=whole_strip, own=False):
        _, cols = strip(number if rows == whole_strip else strips - 1, way)
        first, count = rows
        here = f2x.at[b, :, pl.ds(side + first, count), cols]
        return pltpu.make_async_remote_copy(
            src_ref=f2_hbm.at[:, pl.ds(first, count), cols] if own else here,
            dst_ref=here,
            send_sem=zs_sem.at[way, b, number],
            recv_sem=zr_sem.at[b, number],
            device_id=(r, c - 1 + 2 * way),
            device_id_type=MESH,
        )

    def halo_copy(b, at, way, up, own=False):
        _, cols = strip(at, way)
        first = 0 if up else band_rows - side
        into = band_rows + side if up else 0
        if own:
            source = f2_hbm.at[:, pl.ds(first, side), cols]
        else:
            source = f2x.at[b, :, pl.ds(first + side, side), cols]
        lane = 0 if up else 1
        return pltpu.make_async_remote_copy(
            src_ref=source,
            dst_ref=f2x.at[b, :, pl.ds(into, side), cols],
            send_sem=hs_sem.at[lane, b, at],
            recv_sem=hr_sem.at[lane, b, at],
            device_id=(r - 1 if up else r + 1, c),
            device_id_type=MESH,
        )

    def send_halo(b, at, way, up, own=False):
        @pl.when(r > 0 if up else r < last_r)
        def _():
            halo_copy(b, at, way, up, own).start()

    def goes_on(way):
        return (c - 1 + 2 * way >= 0) & (c - 1 + 2 * way <= last_c)

    def f1_copy(index, row, half, bit):
        part = pl.ds(half * half_blocks, half_blocks)
        return pltpu.make_async_remote_copy(
            src_ref=f1a.at[row, part],
            dst_ref=f1a.at[row, part],
            send_sem=fs_sem.at[index],
            recv_sem=fr_sem.at[row, half],
            device_id=(flipped(r, bit), c),
            device_id_type=MESH,
        )

    def tab_copy(k):
        return pltpu.make_async_remote_copy(
            src_ref=tab_made.at[(r + k) % row_count],
            dst_ref=tabv.at[r],
            send_sem=ts_sem.at[k],
            recv_sem=tr_sem.at[k],
            device_id=((r + k) % row_count, c),
            device_id_type=MESH,
        )

    def rep_copy(b, k):
        s = (r + k) % row_count
        return pltpu.make_async_remote_copy(
            src_ref=reps.at[b, s],
            dst_ref=rep_out.at[:, r, b],
            send_sem=rs_sem.at[b, k],
            recv_sem=rr_sem.at[b, k],
            device_id=(s, c),
            device_id_type=MESH,
        )

    def rep_local(b):
        return pltpu.make_async_copy(reps.at[b, r], rep_out.at[:, r, b], rs_sem.at[b, 0])

    x_row, y_row, d_row = flipped(r, 2), flipped(r, 4), flipped(flipped(r, 2), 4)
    f1_first = [(0, r, 0, 2), (1, r, 0, 4), (2, r, 1, 2), (3, r, 1, 4), (4, r, 0, 1), (5, r, 1, 1)]
    f1_second = [
        (6, x_row, 0, 4),
        (7, y_row, 1, 2),
        (8, x_row, 0, 1),
        (9, x_row, 1, 1),
        (10, y_row, 0, 1),
        (11, y_row, 1, 1),
    ]
    f1_third = [(12, d_row, 0, 1), (13, d_row, 1, 1)]

    def whole_part(values, unit):
        return jnp.floor((values + 0.5) * (1.0 / unit))

    def make_tables():
        ids = lax.broadcasted_iota(jnp.int32, (block_count, block_count), 0).astype(jnp.float32)
        lanes = lax.broadcasted_iota(jnp.int32, (block_count, block_count), 1).astype(jnp.float32)
        block = lanes[:1]
        spots = lax.broadcasted_iota(
            jnp.int32, (block_count, tab_made.shape[2]), 1
        ).astype(jnp.float32)
        peers = lax.broadcasted_iota(jnp.int32, (row_count, block_count), 0).astype(jnp.float32)

        def upright(line_values):
            return jnp.sum(jnp.where(ids == lanes, line_values, 0.0), axis=1, keepdims=True)

        tab_made[...] = jnp.zeros(tab_made.shape, tab_made.dtype)
        idx_out[...] = jnp.zeros(idx_out.shape, idx_out.dtype)
        totals = [0.0, 0.0, 0.0]
        for level in range(LEVELS):
            owner = owner_ref[level].astype(jnp.float32)
            tile = tile_ref[level : level + 1].astype(jnp.float32)
            level_across = across >> level
            tiles = (subs >> level) * level_across
            tile = tile - whole_part(tile, tiles) * tiles
            tile_row = whole_part(tile, level_across)
            same = jnp.where((upright(owner) == owner) & (ids < lanes), 1.0, 0.0)
            rank = jnp.sum(same, axis=0, keepdims=True)
            towards = whole_part(owner, plane_count)
            plane = owner - towards * plane_count
            place = (plane * LEVELS + level) * slots + rank
            map_rows = (band_rows >> level) + side
            values = [
                block,
                whole_part(block, per_frame) * map_rows + tile_row * side,
                tile - tile_row * level_across,
            ]
            place = jnp.where(rank < slots, place, -1.0)
            chosen = jnp.where(upright(place) == spots, 1.0, 0.0).astype(jnp.bfloat16)
            for at, value in enumerate(values):
                named = jnp.where(peers == towards, value, 0.0).astype(jnp.bfloat16)
                totals[at] += jnp.dot(named, chosen, preferred_element_type=jnp.float32)
            rank = jnp.minimum(rank, slots - 1.0)
            pair = whole_part(rank, 2)
            source = (owner * (slots // 2) + pair).astype(jnp.int32)
            idx_out[level : level + 1, :block_count] = source
            half = (rank - 2 * pair).astype(jnp.int32)
            idx_out[LEVELS + level : LEVELS + level + 1, :block_count] = half
        for at, total in enumerate(totals):
            total = total.astype(jnp.int32)
            for peer in range(row_count):
                tab_made[peer, at : at + 1, :] = total[peer : peer + 1]

    loc_f2 = pltpu.make_async_copy(f2_hbm, f2x.at[c, :, pl.ds(side, band_rows)], loc_sem.at[0])
    loc_tab = pltpu.make_async_copy(tab_made.at[r], tabv.at[r], loc_sem.at[2])

    def loc_q(k):
        f, at = k // per_frame, k % per_frame
        cut = q_hbm.at[f, at // across, :, at % across]
        return pltpu.make_async_copy(cut, f1a.at[r, k], loc_sem.at[1])

    def start_q(k, carry):
        loc_q(k).start()
        return carry

    for way in range(2):

        @pl.when(goes_on(way))
        def _():
            for at in range(strips - 1):
                z_copy(c, at, way, own=True).start()
            for number, rows in last_pieces:
                z_copy(c, number, way, rows, own=True).start()

    lax.fori_loop(0, block_count, start_q, 0)
    loc_f2.start()
    make_tables()
    pltpu.make_async_copy(f1a.at[r], f1a.at[r], loc_sem.at[1]).wait()
    for item in f1_first:
        f1_copy(*item).start()
    for at in range(strips):
        send_halo(c, at, 0, True, own=True)
        send_halo(c, at, 0, False, own=True)
    for k in range(1, row_count):
        tab_copy(k).start()
    loc_tab.start()

    @pl.when(r == 0)
    def _():
        f2x[:, :, 0:side] = jnp.zeros((plane_count, frame_count, side) + f2x.shape[3:], f2x.dtype)

    @pl.when(r == last_r)
    def _():
        f2x[:, :, band_rows + side :] = jnp.zeros(
            (plane_count, frame_count, side) + f2x.shape[3:], f2x.dtype
        )

    def each_side(step, act):
        def one(way, carry):
            b = c + step * (1 - 2 * way)

            @pl.when((b >= 0) & (b <= last_c))
            def _():
                act(b, way)

            return carry

        lax.fori_loop(0, jnp.where(step > 0, 2, 1), one, 0)

    def take(step, at):
        def act(b, way):
            z_copy(b, at, way).wait_recv()

            @pl.when(goes_on(way))
            def _():
                z_copy(b, at, way).start()

            send_halo(b, at, way, True)
            send_halo(b, at, way, False)

        each_side(step, act)

    def take_last(step):
        def act(b, way):
            for place, (number, rows) in enumerate(last_pieces):
                z_copy(b, number, way, rows).wait_recv()

                @pl.when(goes_on(way))
                def _():
                    z_copy(b, number, way, rows).start()

                if place < 2:
                    send_halo(b, strips - 1, way, place == 0)

        each_side(step, act)

    def take_some(step, low, high):
        def one(at, carry):
            take(step, at)
            return carry

        lax.fori_loop(low, high, one, 0)

    def pool(step, low, high):
        def act(b, way):
            def strip_pool(at, carry):
                @pl.when(r > 0)
                def _():
                    halo_copy(b, at, way, False).wait_recv()

                @pl.when(r < last_r)
                def _():
                    halo_copy(b, at, way, True).wait_recv()

                rows = p1x.shape[2]
                p, cols = strip(at, way)
                half_cols = pl.ds(pl.multiple_of(p * side, side), side)

                def pool_row(t, inner):
                    f, i = t // rows, t % rows
                    pair = f2x[b, f, pl.ds(2 * i, 2), cols].astype(jnp.float32)
                    both = pair[0] + pair[1]
                    for lane in range(channels // 128):
                        tmp[lane, pl.ds(i * wide, wide), :] = both[:, lane * 128 : (lane + 1) * 128]
                    for lane in range(channels // 128):
                        even = tmp[lane, pl.ds(i * wide, side, stride=2), :]
                        odd = tmp[lane, pl.ds(i * wide + 1, side, stride=2), :]
                        p1x[b, f, i, half_cols, lane * 128 : (lane + 1) * 128] = (even + odd) * 0.25
                    return inner

                lax.fori_loop(0, frame_count * rows, pool_row, 0, unroll=4)
                return carry

            lax.fori_loop(low, high, strip_pool, 0)

        each_side(step, act)

    lane_id = lax.broadcasted_iota(jnp.int32, (1, 1, 2 * block_cells), 2)
    query_row = lane_id % block_cells // side
    query_col = lane_id[0] % side
    is_first = lane_id[0] < block_cells
    row_id = lax.broadcasted_iota(jnp.int32, line.shape[2:], 0)
    line[...] = jnp.zeros(line.shape, line.dtype)

    def build(b, level):
        into = (map0, map1)[level]
        width = band_cols >> level
        rows = into.shape[0] // frame_count
        left_b, right_b = jnp.maximum(b - 1, 0), jnp.minimum(b + 1, last_c)

        def build_row(t, carry):
            f, y = t // rows, t % rows
            if level == 0:
                at = y + RADIUS
                left = f2x[left_b, f, at, width - 2 * side :, :].astype(jnp.float32)[side:]
                middle = f2x[b, f, at].astype(jnp.float32)
                right = f2x[right_b, f, at, : 2 * side, :].astype(jnp.float32)[:side]
            else:
                left = p1x[left_b, f, y, width - side :, :]
                middle = p1x[b, f, y]
                right = p1x[right_b, f, y, :side, :]
            left = jnp.where(b > 0, left, 0.0)
            right = jnp.where(b < last_c, right, 0.0)
            whole = jnp.concatenate([left, middle, right], axis=0)
            whole = pltpu.roll(whole, whole.shape[0] - RADIUS, 0)
            into[t] = whole[: width + side].reshape(into.shape[1:])
            return carry

        lax.fori_loop(0, into.shape[0], build_row, 0, unroll=4)

    def score_pair(b, s, level, pair):
        from_map = (map0, map1)[level]
        windows, queries = [], []
        for half in range(2):
            at = (b * LEVELS + level) * slots + 2 * pair + half
            k, row = jnp.clip(tabs[s, 0, at], 0, block_count - 1), jnp.clip(tabs[s, 1, at], 0, from_map.shape[0] - span)
            cells = from_map[pl.ds(row, span), pl.ds(jnp.clip(tabs[s, 2, at], 0, from_map.shape[1] - 2), 2)]
            windows.append(cells.reshape(span * span, channels).astype(jnp.bfloat16))
            queries.append(f1a[s, k].astype(jnp.float32).reshape(block_cells, channels))
        queries = jnp.concatenate(queries, axis=0).astype(jnp.bfloat16)
        first, second = [
            lax.dot_general(
                window, queries, (((1,), (1,)), ((), ())), preferred_element_type=jnp.float32
            )
            for window in windows
        ]
        scores = jnp.where(is_first, first, second).reshape(span, span, 2 * block_cells)
        for bit in (1, 2, 4):
            scores = jnp.where((query_row & bit) != 0, scores[bit:], scores[:-bit])
        flat = scores.reshape(wside * span, 2 * block_cells)
        for bit in (1, 2, 4):
            moved = pltpu.roll(flat, flat.shape[0] - bit, 0)
            flat = jnp.where((query_col & bit) != 0, moved, flat)
        flat = flat * scale
        for a in range(wside):
            line[level, pair, a * wside : (a + 1) * wside, :] = flat[a * span : a * span + wside]
        found = line[level, pair]
        top = jnp.max(jnp.abs(found), axis=0, keepdims=True)
        power = jnp.maximum(jnp.ceil(jnp.log2(top)), -100.0)
        coded = jnp.floor(found * (TOP * jnp.exp2(-power)) + 0.5)
        coded = jnp.where(row_id == wside * wside, power, coded)
        reps[b, s, level, pair] = coded.astype(jnp.int32).astype(jnp.int16)

    def process(b, way):
        for level in range(LEVELS):
            build(b, level)

        def source(k, inner):
            s = (r + k) % row_count
            for level in range(LEVELS):
                for pair in range(slots // 2):
                    score_pair(b, s, level, pair)

            @pl.when(k == 0)
            def _():
                rep_local(b).start()

            @pl.when(k > 0)
            def _():
                rep_copy(b, k).start()

            return inner

        lax.fori_loop(0, row_count, source, 0)

    take_some(1, 0, strips - 1)
    take_last(1)
    for item in f1_second:
        index, row, half, bit = item
        if index in (6, 7, 9, 10):
            f1_copy(*item).wait_recv()
        f1_copy(*item).start()
    if last_c >= 2:
        take_some(2, 0, strips - 1)
    for item in f1_third:
        f1_copy(*item).wait_recv()
        f1_copy(*item).start()
    for bits in ((1,), (1, 2), (1, 4), (1, 2, 4)):
        row = r
        for bit in bits:
            row = flipped(row, bit)
        for half in range(2):
            f1_copy(0, row, half, 1).wait_recv()
    for k in range(1, row_count):
        tab_copy(k).wait_recv()
    loc_tab.wait()
    loc_f2.wait()
    tab_smem = pltpu.make_async_copy(tabv, tabs, tl_sem)
    tab_smem.start()
    tab_smem.wait()
    def stage(step, carry):
        @pl.when(step == 1)
        def _():
            take_last(jnp.int32(2))

        @pl.when(step > 2)
        def _():
            take_some(step, 1, strips - 1)
            take_last(step)

        @pl.when(step >= 2)
        def _():
            take(step + 1, 0)

        pool(step, jnp.where(step == 0, 0, 1), strips)
        pool(step + 1, 0, 1)
        each_side(step, process)
        return carry

    lax.fori_loop(0, last_c + 1, stage, 0)

    def all_sent(b, way):
        @pl.when(goes_on(way))
        def _():
            for at in range(strips - 1):
                z_copy(b, at, way).wait_send()
            for number, rows in last_pieces:
                z_copy(b, number, way, rows).wait_send()

    def halos_sent(b, way):
        for at in range(strips):

            @pl.when(r > 0)
            def _():
                halo_copy(b, at, way, True).wait_send()

            @pl.when(r < last_r)
            def _():
                halo_copy(b, at, way, False).wait_send()

    def step_sent(step, carry):
        each_side(step, all_sent)
        each_side(step, halos_sent)
        return carry

    all_sent(c, 1)
    lax.fori_loop(0, last_c + 1, step_sent, 0)

    def plane_end(b, carry):
        rep_local(b).wait()

        def peer_end(k, inner):
            rep_copy(b, k).wait_send()
            rep_copy(b, k).wait_recv()
            return inner

        lax.fori_loop(1, row_count, peer_end, 0)
        return carry

    lax.fori_loop(0, plane_count, plane_end, 0)
    for item in f1_first + f1_second + f1_third:
        f1_copy(*item).wait_send()
    for k in range(1, row_count):
        tab_copy(k).wait_send()


def join_kernel(group, index_ref, reply_ref, out_ref):
    window_cells = out_ref.shape[0]
    padded_rows, lanes = reply_ref.shape[-2:]
    is_first = lax.broadcasted_iota(jnp.int32, (padded_rows, lanes), 1) < lanes // 2
    base = pl.program_id(0) * group * 2
    for m in range(group):
        for level in range(LEVELS):
            picked = []
            for side in range(2):
                at = base + 2 * m + side
                rows = reply_ref[level, index_ref[level, at]].astype(jnp.int32)
                turn = (index_ref[LEVELS + level, at] + side) % 2 * (lanes // 2)
                picked.append(pltpu.roll(rows.astype(jnp.float32), turn, 1))
            both = jnp.where(is_first, picked[0], picked[1])
            unit = jnp.exp2(both[window_cells : window_cells + 1]) * (1.0 / TOP)
            out_ref[:, m * LEVELS + level, :] = both[:window_cells] * unit


def gathered_body(fmap1, fmap2, target_owner, target_tile):
    side = 2 * RADIUS
    window_cells = (2 * RADIUS + 1) ** 2
    frame_count, band_rows, band_cols, channels = fmap1.shape
    row_count = lax.axis_size("rows")
    plane_count = lax.axis_size("cols")
    device_count = row_count * plane_count
    subs, across = band_rows // side, band_cols // side
    per_frame = subs * across
    block_count = frame_count * per_frame
    block_cells = side * side
    slots = max(2, (2 * block_count + device_count - 1) // device_count)
    queries = fmap1.reshape(frame_count, subs, side, across, side, channels)
    owner = target_owner.transpose(0, 2, 1)
    lanes_used = -(-plane_count * LEVELS * slots // 128) * 128
    table = (row_count, 8, lanes_used)
    padded_rows = -(-(window_cells + 1) // 8) * 8
    pairs = slots // 2
    strips = across // 2
    reply_shape = (LEVELS, row_count, plane_count, pairs, padded_rows, 2 * block_cells)
    ext_rows = band_rows + 2 * side
    dma = pltpu.SemaphoreType.DMA
    replies, index = pl.pallas_call(
        functools.partial(lookup_kernel, (row_count, plane_count, slots, channels**-0.5)),
        out_shape=[
            jax.ShapeDtypeStruct(reply_shape, jnp.int16),
            jax.ShapeDtypeStruct((8, 128), jnp.int32),
        ],
        in_specs=[pl.BlockSpec(memory_space=pl.ANY)] * 2
        + [pl.BlockSpec(memory_space=pltpu.VMEM)] * 2,
        out_specs=[
            pl.BlockSpec(memory_space=pl.ANY),
            pl.BlockSpec(memory_space=pltpu.VMEM),
        ],
        scratch_shapes=[
            pltpu.VMEM((plane_count, frame_count, ext_rows, band_cols, channels), jnp.bfloat16),
            pltpu.VMEM((row_count, block_count, side, side, channels), jnp.bfloat16),
            pltpu.VMEM(table, jnp.int32),
            pltpu.VMEM(table, jnp.int32),
            pltpu.SMEM(table, jnp.int32),
            pltpu.VMEM((frame_count * (band_rows + side), across + 1, side, channels), jnp.float32),
            pltpu.VMEM(
                (frame_count * (band_rows // 2 + side), across // 2 + 1, side, channels),
                jnp.float32,
            ),
            pltpu.VMEM(
                (plane_count, frame_count, ext_rows // 2, band_cols // 2, channels), jnp.float32
            ),
            pltpu.VMEM((channels // 128, ext_rows // 2 * 2 * side, 128), jnp.float32),
            pltpu.VMEM((LEVELS, pairs, padded_rows, 2 * block_cells), jnp.float32),
            pltpu.VMEM(
                (plane_count, row_count, LEVELS, pairs, padded_rows, 2 * block_cells), jnp.int16
            ),
            dma((3,)),
            dma((2, plane_count, strips + 2)),
            dma((plane_count, strips + 2)),
            dma((2, plane_count, strips)),
            dma((2, plane_count, strips)),
            dma((14,)),
            dma((row_count, 2)),
            dma((row_count,)),
            dma((row_count,)),
            dma,
            dma((plane_count, row_count)),
            dma((plane_count, row_count)),
        ],
        compiler_params=pltpu.CompilerParams(
            collective_id=0, has_side_effects=True, vmem_limit_bytes=62 * 2**20
        ),
    )(fmap2, queries, owner, target_tile)
    spots = row_count * plane_count * pairs
    group = 8 // LEVELS
    joined = pl.pallas_call(
        functools.partial(join_kernel, group),
        out_shape=jax.ShapeDtypeStruct(
            (window_cells, block_count // 2 * LEVELS, 2 * block_cells), jnp.float32
        ),
        grid=(block_count // 2 // group,),
        in_specs=[
            pl.BlockSpec(memory_space=pltpu.SMEM),
            pl.BlockSpec((LEVELS, spots, padded_rows, 2 * block_cells), lambda g: (0, 0, 0, 0)),
        ],
        out_specs=pl.BlockSpec(
            (window_cells, group * LEVELS, 2 * block_cells), lambda g: (0, g, 0)
        ),
    )(index, replies.reshape(LEVELS, spots, padded_rows, 2 * block_cells))
    joined = joined.reshape(window_cells, block_count // 2, LEVELS, 2 * block_cells)
    return joined.transpose(2, 0, 1, 3).reshape(LEVELS, window_cells, block_count * block_cells)


def solution(mesh):
    in_specs = (
        P(None, "rows", "cols", None),
        P(None, "rows", "cols", None),
        P(None, ("rows", "cols"), None),
        P(None, ("rows", "cols")),
    )
    out_specs = P(None, None, ("rows", "cols"))
    chosen_body = gathered_body if mesh.shape["rows"] == 8 else body
    return jax.shard_map(
        chosen_body, mesh=mesh, in_specs=in_specs, out_specs=out_specs, check_vma=False
    )
```

```python
import functools

import jax
import jax.numpy as jnp
from jax import lax
from jax.experimental import pallas as pl
from jax.experimental.pallas import tpu as pltpu
from jax.sharding import PartitionSpec as P

RADIUS = 4
LEVELS = 2
STEP_SLOTS = 16


def padded_2(block, sides, width):
    for axis, dim in sides:
        count = lax.axis_size(axis)
        forward = [(i, i + 1) for i in range(count - 1)]
        backward = [(target, source) for source, target in forward]
        low = lax.ppermute(
            lax.slice_in_dim(block, block.shape[dim] - width, None, axis=dim), axis, forward
        )
        high = lax.ppermute(lax.slice_in_dim(block, 0, width, axis=dim), axis, backward)
        block = jnp.concatenate([low, block, high], axis=dim)
    return block


def pool_level(level_map):
    frame_count, rows_in, cols_in, channels = level_map.shape
    pooled = level_map.astype(jnp.float32).reshape(
        frame_count, rows_in // 2, 2, cols_in // 2, 2, channels
    )
    return jnp.mean(pooled, axis=(2, 4)).astype(jnp.bfloat16)


def dispatch_kernel(slot_count, block_ref, query_ref, sent_ref):
    base = pl.program_id(0) * slot_count
    for slot in range(slot_count):
        sent_ref[slot] = query_ref[block_ref[base + slot]]


def correlate_kernel(plan, scale, label_ref, query_ref, map_ref, reply_ref):
    per_frame, col_count, padded_rows, across = plan
    tile_side = 2 * RADIUS
    span_side = 4 * RADIUS
    window_side = 2 * RADIUS + 1
    block_cells = tile_side * tile_side
    base = pl.program_id(0) * STEP_SLOTS
    lane = lax.broadcasted_iota(jnp.int32, (1, 1, 2 * block_cells), 2)
    query_row = lane % block_cells // tile_side
    query_col = lane[0] % tile_side
    is_first = lane[0] < block_cells

    def window(slot):
        label = label_ref[base + slot]
        tile = label % per_frame
        region = label // per_frame
        row = region // col_count * padded_rows + tile // across * tile_side
        col = (region % col_count * across + tile % across) * tile_side
        col = pl.multiple_of(col, tile_side)
        cells = map_ref[pl.ds(row, span_side), pl.ds(col, span_side), :]
        return cells.reshape(span_side * span_side, -1).astype(jnp.bfloat16)

    for pair in range(STEP_SLOTS // 2):
        queries = query_ref[2 * pair : 2 * pair + 2].reshape(2 * block_cells, -1)
        first, second = [
            lax.dot_general(
                window(2 * pair + half),
                queries,
                (((1,), (1,)), ((), ())),
                preferred_element_type=jnp.float32,
            )
            for half in range(2)
        ]
        scores = jnp.where(is_first, first, second)
        scores = scores.reshape(span_side, span_side, 2 * block_cells)
        for bit in (1, 2, 4):
            scores = jnp.where((query_row & bit) != 0, scores[bit:], scores[:-bit])
        flat = scores.reshape(window_side * span_side, 2 * block_cells)
        for bit in (1, 2, 4):
            moved = pltpu.roll(flat, flat.shape[0] - bit, 0)
            flat = jnp.where((query_col & bit) != 0, moved, flat)
        flat = flat * scale
        for a in range(window_side):
            at = (pair * window_side + a) * window_side
            reply_ref[at : at + window_side, :] = flat[
                a * span_side : a * span_side + window_side
            ]


def assemble_kernel(pair_count, source_ref, half_ref, *refs):
    reply_refs, out_ref = refs[:-1], refs[-1]
    window_cells, lanes = out_ref.shape[1], reply_refs[0].shape[1]
    is_first = lax.broadcasted_iota(jnp.int32, (window_cells, lanes), 1) < lanes // 2
    for level in range(LEVELS):

        def step(m, carry, level=level):
            at = 2 * (level * pair_count + m)
            picked = []
            for side in range(2):
                first_row = source_ref[at + side] * window_cells
                rows = reply_refs[level][pl.ds(first_row, window_cells), :]
                moved = pltpu.roll(rows, lanes // 2, 1)
                picked.append(jnp.where(half_ref[at + side] == side, rows, moved))
            spot = pl.ds(pl.multiple_of(m * lanes, lanes), lanes)
            out_ref[level, :, spot] = jnp.where(is_first, picked[0], picked[1])
            return carry

        lax.fori_loop(0, pair_count, step, 0)


def body(fmap1, fmap2, target_owner, target_tile):
    tile_side = 2 * RADIUS
    window_side = 2 * RADIUS + 1
    block_cells = tile_side * tile_side
    frame_count, band_rows, band_cols, channels = fmap1.shape
    row_count = lax.axis_size("rows")
    col_count = lax.axis_size("cols")
    device_count = row_count * col_count
    tiles_across = band_cols // tile_side
    per_frame = band_rows // tile_side * tiles_across
    block_count = frame_count * per_frame
    owner_slots = max(2, (2 * block_count + device_count - 1) // device_count)
    row_slots = -(-owner_slots * col_count // STEP_SLOTS) * STEP_SLOTS
    pair_slots = row_slots // 2
    queries = fmap1.reshape(
        frame_count, band_rows // tile_side, tile_side, tiles_across, tile_side, channels
    )
    queries = queries.transpose(0, 1, 3, 2, 4, 5).reshape(block_count, block_cells, channels)
    owner_ids = target_owner[:, :, 0]
    owner_rows = owner_ids // col_count
    peer_ids = jnp.arange(row_count, dtype=jnp.int32)
    owner_hits = (owner_rows[:, :, None] == peer_ids[None, None, :]).astype(jnp.int32)
    slot_rank = jnp.sum(owner_hits * (jnp.cumsum(owner_hits, axis=1) - 1), axis=2)
    block_ids = jnp.arange(block_count, dtype=jnp.int32)
    label_rows = []
    for level in range(LEVELS):
        tile_count = (band_rows >> level) // tile_side * ((band_cols >> level) // tile_side)
        regions = block_ids // per_frame * col_count + owner_ids[level] % col_count
        label_rows.append(regions * per_frame + target_tile[level] % tile_count)
    rank_ids = jnp.arange(row_slots, dtype=jnp.int32)
    rank_hits = (slot_rank[:, :, None] == rank_ids[None, None, :]).astype(jnp.int32)
    slot_hits = owner_hits[:, :, :, None] * rank_hits[:, :, None, :]

    def by_slot(values):
        table = jnp.sum(slot_hits * values[:, :, None, None], axis=1)
        return table.transpose(1, 0, 2)

    labels_sent = by_slot(jnp.stack(label_rows))
    blocks_sent = by_slot(jnp.broadcast_to(block_ids[None], owner_ids.shape))
    slot_block = (row_slots, block_cells, channels)
    slot_total = row_count * row_slots
    label_part = lax.all_to_all(labels_sent, "rows", split_axis=0, concat_axis=0, tiled=True)
    levels = [fmap2]
    for level in range(1, LEVELS):
        levels.append(pool_level(levels[-1]))
    window_cells = window_side * window_side
    step_block = (STEP_SLOTS, block_cells, channels)
    reply_block = (STEP_SLOTS // 2 * window_cells, 2 * block_cells)
    reply_tables = [None] * LEVELS
    earlier = None
    for level in reversed(range(LEVELS)):
        queries_sent = pl.pallas_call(
            functools.partial(dispatch_kernel, row_slots),
            out_shape=jax.ShapeDtypeStruct((slot_total,) + slot_block[1:], jnp.bfloat16),
            grid_spec=pltpu.PrefetchScalarGridSpec(
                num_scalar_prefetch=1,
                grid=(row_count,),
                in_specs=[pl.BlockSpec(queries.shape, lambda d, *_: (0, 0, 0))],
                out_specs=pl.BlockSpec(slot_block, lambda d, *_: (d, 0, 0)),
            ),
        )(blocks_sent[:, level].reshape(-1), queries)
        query_part = lax.all_to_all(
            queries_sent.reshape((row_count,) + slot_block),
            "rows",
            split_axis=0,
            concat_axis=0,
            tiled=True,
        )
        band = lax.all_gather(levels[level], "cols", axis=2, tiled=True)
        if earlier is not None:
            band = lax.optimization_barrier((band, earlier, query_part))[0]
        padded = padded_2(band, (("rows", 1),), RADIUS).astype(jnp.float32)
        padded = jnp.pad(padded, ((0, 0), (0, 0), (RADIUS, RADIUS), (0, 0)))
        level_map = padded.reshape((-1,) + padded.shape[2:])
        plan = (per_frame, col_count, padded.shape[1], levels[level].shape[2] // tile_side)
        replies = pl.pallas_call(
            functools.partial(correlate_kernel, plan, channels ** (-0.5)),
            out_shape=jax.ShapeDtypeStruct(
                (row_count * pair_slots * window_cells, 2 * block_cells), jnp.float32
            ),
            grid_spec=pltpu.PrefetchScalarGridSpec(
                num_scalar_prefetch=1,
                grid=(slot_total // STEP_SLOTS,),
                in_specs=[
                    pl.BlockSpec(step_block, lambda d, *_: (d, 0, 0)),
                    pl.BlockSpec(
                        level_map.shape, lambda d, *_: (0, 0, 0), pipeline_mode=pl.Buffered(1)
                    ),
                ],
                out_specs=pl.BlockSpec(reply_block, lambda d, *_: (d, 0)),
            ),
        )(
            label_part[:, level].reshape(-1),
            query_part.reshape((slot_total,) + slot_block[1:]),
            level_map,
        )
        returned = lax.all_to_all(
            replies.reshape(row_count, pair_slots * window_cells, 2 * block_cells),
            "rows",
            split_axis=0,
            concat_axis=0,
            tiled=True,
        )
        earlier = returned
        reply_tables[level] = returned.reshape(-1, 2 * block_cells)
    source_ids = owner_rows * pair_slots + slot_rank // 2
    return pl.pallas_call(
        functools.partial(assemble_kernel, block_count // 2),
        out_shape=jax.ShapeDtypeStruct(
            (LEVELS, window_cells, block_count * block_cells), jnp.float32
        ),
        in_specs=[
            pl.BlockSpec(memory_space=pltpu.SMEM),
            pl.BlockSpec(memory_space=pltpu.SMEM),
        ]
        + [pl.BlockSpec(memory_space=pltpu.VMEM)] * LEVELS,
        out_specs=pl.BlockSpec(memory_space=pltpu.VMEM),
    )(source_ids.reshape(-1), (slot_rank % 2).reshape(-1), *reply_tables)


MESH = pl.DeviceIdType.MESH
TOP = 32000.0


def flipped(index, bit):
    return index + bit - 2 * bit * (index // bit % 2)


def lookup_kernel(
    plan,
    f2_hbm,
    q_hbm,
    owner_ref,
    tile_ref,
    rep_out,
    idx_out,
    f2x,
    f1a,
    tab_made,
    tabv,
    tabs,
    map0,
    map1,
    p1x,
    tmp,
    line,
    reps,
    loc_sem,
    zs_sem,
    zr_sem,
    hs_sem,
    hr_sem,
    fs_sem,
    fr_sem,
    ts_sem,
    tr_sem,
    tl_sem,
    rs_sem,
    rr_sem,
):
    row_count, plane_count, slots, scale = plan
    frame_count, band_rows, band_cols, channels = f2_hbm.shape
    side = 2 * RADIUS
    subs, across = band_rows // side, band_cols // side
    per_frame = subs * across
    block_count, block_cells = frame_count * per_frame, side * side
    span = 4 * RADIUS
    wside = 2 * RADIUS + 1
    wide = 2 * side
    strips = band_cols // wide
    half_blocks = block_count // 2
    r = lax.axis_index("rows")
    c = lax.axis_index("cols")
    last_r, last_c = row_count - 1, plane_count - 1

    barrier = pltpu.get_barrier_semaphore()
    for k in range(1, row_count):
        pl.semaphore_signal(
            barrier, inc=1, device_id=((r + k) % row_count, c), device_id_type=MESH
        )

    @pl.when(c > 0)
    def _():
        pl.semaphore_signal(barrier, inc=1, device_id=(r, c - 1), device_id_type=MESH)

    @pl.when(c < last_c)
    def _():
        pl.semaphore_signal(barrier, inc=1, device_id=(r, c + 1), device_id_type=MESH)

    has_left = jnp.where(c > 0, 1, 0)
    has_right = jnp.where(c < last_c, 1, 0)
    pl.semaphore_wait(barrier, row_count - 1 + has_left + has_right)

    def strip(at, way):
        p = at + way * (strips - 1 - 2 * at)
        return p, pl.ds(pl.multiple_of(p * wide, wide), wide)

    whole_strip = (0, band_rows)
    last_pieces = [
        (strips - 1, (0, side)),
        (strips, (band_rows - side, side)),
        (strips + 1, (side, band_rows - 2 * side)),
    ]

    def z_copy(b, number, way, rows=whole_strip, own=False):
        _, cols = strip(number if rows == whole_strip else strips - 1, way)
        first, count = rows
        here = f2x.at[b, :, pl.ds(side + first, count), cols]
        return pltpu.make_async_remote_copy(
            src_ref=f2_hbm.at[:, pl.ds(first, count), cols] if own else here,
            dst_ref=here,
            send_sem=zs_sem.at[way, b, number],
            recv_sem=zr_sem.at[b, number],
            device_id=(r, c - 1 + 2 * way),
            device_id_type=MESH,
        )

    def halo_copy(b, at, way, up, own=False):
        _, cols = strip(at, way)
        first = 0 if up else band_rows - side
        into = band_rows + side if up else 0
        if own:
            source = f2_hbm.at[:, pl.ds(first, side), cols]
        else:
            source = f2x.at[b, :, pl.ds(first + side, side), cols]
        lane = 0 if up else 1
        return pltpu.make_async_remote_copy(
            src_ref=source,
            dst_ref=f2x.at[b, :, pl.ds(into, side), cols],
            send_sem=hs_sem.at[lane, b, at],
            recv_sem=hr_sem.at[lane, b, at],
            device_id=(r - 1 if up else r + 1, c),
            device_id_type=MESH,
        )

    def send_halo(b, at, way, up, own=False):
        @pl.when(r > 0 if up else r < last_r)
        def _():
            halo_copy(b, at, way, up, own).start()

    def goes_on(way):
        return (c - 1 + 2 * way >= 0) & (c - 1 + 2 * way <= last_c)

    def f1_copy(index, row, half, bit):
        part = pl.ds(half * half_blocks, half_blocks)
        return pltpu.make_async_remote_copy(
            src_ref=f1a.at[row, part],
            dst_ref=f1a.at[row, part],
            send_sem=fs_sem.at[index],
            recv_sem=fr_sem.at[row, half],
            device_id=(flipped(r, bit), c),
            device_id_type=MESH,
        )

    def tab_copy(k):
        return pltpu.make_async_remote_copy(
            src_ref=tab_made.at[(r + k) % row_count],
            dst_ref=tabv.at[r],
            send_sem=ts_sem.at[k],
            recv_sem=tr_sem.at[k],
            device_id=((r + k) % row_count, c),
            device_id_type=MESH,
        )

    def rep_copy(b, k):
        s = (r + k) % row_count
        return pltpu.make_async_remote_copy(
            src_ref=reps.at[b, s],
            dst_ref=rep_out.at[:, r, b],
            send_sem=rs_sem.at[b, k],
            recv_sem=rr_sem.at[b, k],
            device_id=(s, c),
            device_id_type=MESH,
        )

    def rep_local(b):
        return pltpu.make_async_copy(reps.at[b, r], rep_out.at[:, r, b], rs_sem.at[b, 0])

    x_row, y_row, d_row = flipped(r, 2), flipped(r, 4), flipped(flipped(r, 2), 4)
    f1_first = [(0, r, 0, 2), (1, r, 0, 4), (2, r, 1, 2), (3, r, 1, 4), (4, r, 0, 1), (5, r, 1, 1)]
    f1_second = [
        (6, x_row, 0, 4),
        (7, y_row, 1, 2),
        (8, x_row, 0, 1),
        (9, x_row, 1, 1),
        (10, y_row, 0, 1),
        (11, y_row, 1, 1),
    ]
    f1_third = [(12, d_row, 0, 1), (13, d_row, 1, 1)]

    def whole_part(values, unit):
        return jnp.floor((values + 0.5) * (1.0 / unit))

    def make_tables():
        ids = lax.broadcasted_iota(jnp.int32, (block_count, block_count), 0).astype(jnp.float32)
        lanes = lax.broadcasted_iota(jnp.int32, (block_count, block_count), 1).astype(jnp.float32)
        block = lanes[:1]
        spots = lax.broadcasted_iota(
            jnp.int32, (block_count, tab_made.shape[2]), 1
        ).astype(jnp.float32)
        peers = lax.broadcasted_iota(jnp.int32, (row_count, block_count), 0).astype(jnp.float32)

        def upright(line_values):
            return jnp.sum(jnp.where(ids == lanes, line_values, 0.0), axis=1, keepdims=True)

        tab_made[...] = jnp.zeros(tab_made.shape, tab_made.dtype)
        idx_out[...] = jnp.zeros(idx_out.shape, idx_out.dtype)
        totals = [0.0, 0.0, 0.0]
        for level in range(LEVELS):
            owner = owner_ref[level].astype(jnp.float32)
            tile = tile_ref[level : level + 1].astype(jnp.float32)
            level_across = across >> level
            tiles = (subs >> level) * level_across
            tile = tile - whole_part(tile, tiles) * tiles
            tile_row = whole_part(tile, level_across)
            same = jnp.where((upright(owner) == owner) & (ids < lanes), 1.0, 0.0)
            rank = jnp.sum(same, axis=0, keepdims=True)
            towards = whole_part(owner, plane_count)
            plane = owner - towards * plane_count
            place = (plane * LEVELS + level) * slots + rank
            map_rows = (band_rows >> level) + side
            values = [
                block,
                whole_part(block, per_frame) * map_rows + tile_row * side,
                tile - tile_row * level_across,
            ]
            place = jnp.where(rank < slots, place, -1.0)
            chosen = jnp.where(upright(place) == spots, 1.0, 0.0).astype(jnp.bfloat16)
            for at, value in enumerate(values):
                named = jnp.where(peers == towards, value, 0.0).astype(jnp.bfloat16)
                totals[at] += jnp.dot(named, chosen, preferred_element_type=jnp.float32)
            rank = jnp.minimum(rank, slots - 1.0)
            pair = whole_part(rank, 2)
            source = (owner * (slots // 2) + pair).astype(jnp.int32)
            idx_out[level : level + 1, :block_count] = source
            half = (rank - 2 * pair).astype(jnp.int32)
            idx_out[LEVELS + level : LEVELS + level + 1, :block_count] = half
        for at, total in enumerate(totals):
            total = total.astype(jnp.int32)
            for peer in range(row_count):
                tab_made[peer, at : at + 1, :] = total[peer : peer + 1]

    loc_f2 = pltpu.make_async_copy(f2_hbm, f2x.at[c, :, pl.ds(side, band_rows)], loc_sem.at[0])
    loc_tab = pltpu.make_async_copy(tab_made.at[r], tabv.at[r], loc_sem.at[2])

    def loc_q(k):
        f, at = k // per_frame, k % per_frame
        cut = q_hbm.at[f, at // across, :, at % across]
        return pltpu.make_async_copy(cut, f1a.at[r, k], loc_sem.at[1])

    def start_q(k, carry):
        loc_q(k).start()
        return carry

    for way in range(2):

        @pl.when(goes_on(way))
        def _():
            for at in range(strips - 1):
                z_copy(c, at, way, own=True).start()
            for number, rows in last_pieces:
                z_copy(c, number, way, rows, own=True).start()

    lax.fori_loop(0, block_count, start_q, 0)
    loc_f2.start()
    make_tables()
    pltpu.make_async_copy(f1a.at[r], f1a.at[r], loc_sem.at[1]).wait()
    for item in f1_first:
        f1_copy(*item).start()
    for at in range(strips):
        send_halo(c, at, 0, True, own=True)
        send_halo(c, at, 0, False, own=True)
    for k in range(1, row_count):
        tab_copy(k).start()
    loc_tab.start()

    @pl.when(r == 0)
    def _():
        f2x[:, :, 0:side] = jnp.zeros((plane_count, frame_count, side) + f2x.shape[3:], f2x.dtype)

    @pl.when(r == last_r)
    def _():
        f2x[:, :, band_rows + side :] = jnp.zeros(
            (plane_count, frame_count, side) + f2x.shape[3:], f2x.dtype
        )

    def each_side(step, act):
        def one(way, carry):
            b = c + step * (1 - 2 * way)

            @pl.when((b >= 0) & (b <= last_c))
            def _():
                act(b, way)

            return carry

        lax.fori_loop(0, jnp.where(step > 0, 2, 1), one, 0)

    def take(step, at, halo=True):
        def act(b, way):
            z_copy(b, at, way).wait_recv()

            @pl.when(goes_on(way))
            def _():
                z_copy(b, at, way).start()

            if halo:
                send_halo(b, at, way, True)
                send_halo(b, at, way, False)

        each_side(step, act)

    def take_last(step, halo=True):
        def act(b, way):
            for place, (number, rows) in enumerate(last_pieces):
                z_copy(b, number, way, rows).wait_recv()

                @pl.when(goes_on(way))
                def _():
                    z_copy(b, number, way, rows).start()

                if halo and place < 2:
                    send_halo(b, strips - 1, way, place == 0)

        each_side(step, act)

    def take_some(step, low, high, halo=True):
        def one(at, carry):
            take(step, at, halo)
            return carry

        lax.fori_loop(low, high, one, 0)

    def pool(step, low, high):
        def act(b, way):
            def strip_pool(at, carry):
                @pl.when(r > 0)
                def _():
                    halo_copy(b, at, way, False).wait_recv()

                @pl.when(r < last_r)
                def _():
                    halo_copy(b, at, way, True).wait_recv()

                rows = p1x.shape[2]
                p, cols = strip(at, way)
                half_cols = pl.ds(pl.multiple_of(p * side, side), side)

                def pool_row(t, inner):
                    f, i = t // rows, t % rows
                    pair = f2x[b, f, pl.ds(2 * i, 2), cols].astype(jnp.float32)
                    both = pair[0] + pair[1]
                    for lane in range(channels // 128):
                        tmp[lane, pl.ds(i * wide, wide), :] = both[:, lane * 128 : (lane + 1) * 128]
                    for lane in range(channels // 128):
                        even = tmp[lane, pl.ds(i * wide, side, stride=2), :]
                        odd = tmp[lane, pl.ds(i * wide + 1, side, stride=2), :]
                        p1x[b, f, i, half_cols, lane * 128 : (lane + 1) * 128] = (even + odd) * 0.25
                    return inner

                lax.fori_loop(0, frame_count * rows, pool_row, 0, unroll=4)
                return carry

            lax.fori_loop(low, high, strip_pool, 0)

        each_side(step, act)

    lane_id = lax.broadcasted_iota(jnp.int32, (1, 1, 2 * block_cells), 2)
    query_row = lane_id % block_cells // side
    query_col = lane_id[0] % side
    is_first = lane_id[0] < block_cells
    row_id = lax.broadcasted_iota(jnp.int32, line.shape[2:], 0)
    line[...] = jnp.zeros(line.shape, line.dtype)

    def build(b, level):
        into = (map0, map1)[level]
        width = band_cols >> level
        rows = into.shape[0] // frame_count
        left_b, right_b = jnp.maximum(b - 1, 0), jnp.minimum(b + 1, last_c)

        def build_row(t, carry):
            f, y = t // rows, t % rows
            if level == 0:
                at = y + RADIUS
                left = f2x[left_b, f, at, width - 2 * side :, :].astype(jnp.float32)[side:]
                middle = f2x[b, f, at].astype(jnp.float32)
                right = f2x[right_b, f, at, : 2 * side, :].astype(jnp.float32)[:side]
            else:
                left = p1x[left_b, f, y, width - side :, :]
                middle = p1x[b, f, y]
                right = p1x[right_b, f, y, :side, :]
            left = jnp.where(b > 0, left, 0.0)
            right = jnp.where(b < last_c, right, 0.0)
            whole = jnp.concatenate([left, middle, right], axis=0)
            whole = pltpu.roll(whole, whole.shape[0] - RADIUS, 0)
            into[t] = whole[: width + side].reshape(into.shape[1:])
            return carry

        lax.fori_loop(0, into.shape[0], build_row, 0, unroll=4)

    def score_pair(b, s, level, pair):
        from_map = (map0, map1)[level]
        windows, queries = [], []
        for half in range(2):
            at = (b * LEVELS + level) * slots + 2 * pair + half
            k, row = jnp.clip(tabs[s, 0, at], 0, block_count - 1), jnp.clip(tabs[s, 1, at], 0, from_map.shape[0] - span)
            cells = from_map[pl.ds(row, span), pl.ds(jnp.clip(tabs[s, 2, at], 0, from_map.shape[1] - 2), 2)]
            windows.append(cells.reshape(span * span, channels).astype(jnp.bfloat16))
            queries.append(f1a[s, k].reshape(block_cells, channels))
        queries = jnp.concatenate(queries, axis=0)
        first, second = [
            lax.dot_general(
                window, queries, (((1,), (1,)), ((), ())), preferred_element_type=jnp.float32
            )
            for window in windows
        ]
        scores = jnp.where(is_first, first, second).reshape(span, span, 2 * block_cells)
        for bit in (1, 2, 4):
            scores = jnp.where((query_row & bit) != 0, scores[bit:], scores[:-bit])
        flat = scores.reshape(wside * span, 2 * block_cells)
        for bit in (1, 2, 4):
            moved = pltpu.roll(flat, flat.shape[0] - bit, 0)
            flat = jnp.where((query_col & bit) != 0, moved, flat)
        flat = flat * scale
        for a in range(wside):
            line[level, pair, a * wside : (a + 1) * wside, :] = flat[a * span : a * span + wside]
        found = line[level, pair]
        top = jnp.max(jnp.abs(found), axis=0, keepdims=True)
        power = jnp.maximum(jnp.ceil(jnp.log2(top)), -100.0)
        coded = jnp.floor(found * (TOP * jnp.exp2(-power)) + 0.5)
        coded = jnp.where(row_id == wside * wside, power, coded)
        reps[b, s, level, pair] = coded.astype(jnp.int32).astype(jnp.int16)

    def process(b, way):
        for level in range(LEVELS):
            build(b, level)

        def source(j, inner):
            flips = (1 - j // 4, (j // 2 + j // 4) % 2, (j + j // 6) % 2)
            s = r
            for flip, bit in zip(flips, (2, 4, 1), strict=True):
                s = s + flip * (bit - 2 * bit * (r // bit % 2))
            k = (s - r + row_count) % row_count
            for level in range(LEVELS):
                for pair in range(slots // 2):
                    score_pair(b, s, level, pair)

            @pl.when(k == 0)
            def _():
                rep_local(b).start()

            @pl.when(k > 0)
            def _():
                rep_copy(b, k).start()

            return inner

        lax.fori_loop(0, row_count, source, 0)

    take_some(1, 0, strips - 1, False)
    take_last(1, False)
    for item in f1_second:
        index, row, half, bit = item
        if index in (6, 7, 9, 10):
            f1_copy(*item).wait_recv()
        f1_copy(*item).start()

    def first_halos(at, carry):
        def act(b, way):
            send_halo(b, at, way, True)
            send_halo(b, at, way, False)

        each_side(1, act)
        return carry

    lax.fori_loop(0, strips, first_halos, 0)
    if last_c >= 2:
        take_some(2, 0, strips - 1)
    for item in f1_third:
        f1_copy(*item).wait_recv()
        f1_copy(*item).start()
    for bits in ((1,), (1, 2), (1, 4), (1, 2, 4)):
        row = r
        for bit in bits:
            row = flipped(row, bit)
        for half in range(2):
            f1_copy(0, row, half, 1).wait_recv()
    for k in range(1, row_count):
        tab_copy(k).wait_recv()
    loc_tab.wait()
    loc_f2.wait()
    tab_smem = pltpu.make_async_copy(tabv, tabs, tl_sem)
    tab_smem.start()
    tab_smem.wait()
    def stage(step, carry):
        @pl.when(step == 1)
        def _():
            take_last(jnp.int32(2))

        @pl.when(step > 2)
        def _():
            take_some(step, 1, strips - 1)
            take_last(step)

        @pl.when(step >= 2)
        def _():
            take(step + 1, 0)

        pool(step, jnp.where(step == 0, 0, 1), strips)
        pool(step + 1, 0, 1)
        each_side(step, process)
        return carry

    lax.fori_loop(0, last_c + 1, stage, 0)

    def all_sent(b, way):
        @pl.when(goes_on(way))
        def _():
            for at in range(strips - 1):
                z_copy(b, at, way).wait_send()
            for number, rows in last_pieces:
                z_copy(b, number, way, rows).wait_send()

    def halos_sent(b, way):
        for at in range(strips):

            @pl.when(r > 0)
            def _():
                halo_copy(b, at, way, True).wait_send()

            @pl.when(r < last_r)
            def _():
                halo_copy(b, at, way, False).wait_send()

    def step_sent(step, carry):
        each_side(step, all_sent)
        each_side(step, halos_sent)
        return carry

    all_sent(c, 1)
    lax.fori_loop(0, last_c + 1, step_sent, 0)

    def plane_end(b, carry):
        rep_local(b).wait()

        def peer_end(k, inner):
            rep_copy(b, k).wait_send()
            rep_copy(b, k).wait_recv()
            return inner

        lax.fori_loop(1, row_count, peer_end, 0)
        return carry

    lax.fori_loop(0, plane_count, plane_end, 0)
    for item in f1_first + f1_second + f1_third:
        f1_copy(*item).wait_send()
    for k in range(1, row_count):
        tab_copy(k).wait_send()


def join_kernel(group, index_ref, reply_ref, out_ref):
    window_cells = out_ref.shape[0]
    padded_rows, lanes = reply_ref.shape[-2:]
    is_first = lax.broadcasted_iota(jnp.int32, (padded_rows, lanes), 1) < lanes // 2
    base = pl.program_id(0) * group * 2
    for m in range(group):
        for level in range(LEVELS):
            picked = []
            for side in range(2):
                at = base + 2 * m + side
                rows = reply_ref[level, index_ref[level, at]].astype(jnp.int32)
                turn = (index_ref[LEVELS + level, at] + side) % 2 * (lanes // 2)
                picked.append(pltpu.roll(rows.astype(jnp.float32), turn, 1))
            both = jnp.where(is_first, picked[0], picked[1])
            unit = jnp.exp2(both[window_cells : window_cells + 1]) * (1.0 / TOP)
            out_ref[:, m * LEVELS + level, :] = both[:window_cells] * unit


def gathered_body(fmap1, fmap2, target_owner, target_tile):
    side = 2 * RADIUS
    window_cells = (2 * RADIUS + 1) ** 2
    frame_count, band_rows, band_cols, channels = fmap1.shape
    row_count = lax.axis_size("rows")
    plane_count = lax.axis_size("cols")
    device_count = row_count * plane_count
    subs, across = band_rows // side, band_cols // side
    per_frame = subs * across
    block_count = frame_count * per_frame
    block_cells = side * side
    slots = max(2, (2 * block_count + device_count - 1) // device_count)
    queries = fmap1.reshape(frame_count, subs, side, across, side, channels)
    owner = target_owner.transpose(0, 2, 1)
    lanes_used = -(-plane_count * LEVELS * slots // 128) * 128
    table = (row_count, 8, lanes_used)
    padded_rows = -(-(window_cells + 1) // 8) * 8
    pairs = slots // 2
    strips = across // 2
    reply_shape = (LEVELS, row_count, plane_count, pairs, padded_rows, 2 * block_cells)
    ext_rows = band_rows + 2 * side
    dma = pltpu.SemaphoreType.DMA
    replies, index = pl.pallas_call(
        functools.partial(lookup_kernel, (row_count, plane_count, slots, channels**-0.5)),
        out_shape=[
            jax.ShapeDtypeStruct(reply_shape, jnp.int16),
            jax.ShapeDtypeStruct((8, 128), jnp.int32),
        ],
        in_specs=[pl.BlockSpec(memory_space=pl.ANY)] * 2
        + [pl.BlockSpec(memory_space=pltpu.VMEM)] * 2,
        out_specs=[
            pl.BlockSpec(memory_space=pl.ANY),
            pl.BlockSpec(memory_space=pltpu.VMEM),
        ],
        scratch_shapes=[
            pltpu.VMEM((plane_count, frame_count, ext_rows, band_cols, channels), jnp.bfloat16),
            pltpu.VMEM((row_count, block_count, side, side, channels), jnp.bfloat16),
            pltpu.VMEM(table, jnp.int32),
            pltpu.VMEM(table, jnp.int32),
            pltpu.SMEM(table, jnp.int32),
            pltpu.VMEM((frame_count * (band_rows + side), across + 1, side, channels), jnp.float32),
            pltpu.VMEM(
                (frame_count * (band_rows // 2 + side), across // 2 + 1, side, channels),
                jnp.float32,
            ),
            pltpu.VMEM(
                (plane_count, frame_count, ext_rows // 2, band_cols // 2, channels), jnp.float32
            ),
            pltpu.VMEM((channels // 128, ext_rows // 2 * 2 * side, 128), jnp.float32),
            pltpu.VMEM((LEVELS, pairs, padded_rows, 2 * block_cells), jnp.float32),
            pltpu.VMEM(
                (plane_count, row_count, LEVELS, pairs, padded_rows, 2 * block_cells), jnp.int16
            ),
            dma((3,)),
            dma((2, plane_count, strips + 2)),
            dma((plane_count, strips + 2)),
            dma((2, plane_count, strips)),
            dma((2, plane_count, strips)),
            dma((14,)),
            dma((row_count, 2)),
            dma((row_count,)),
            dma((row_count,)),
            dma,
            dma((plane_count, row_count)),
            dma((plane_count, row_count)),
        ],
        compiler_params=pltpu.CompilerParams(
            collective_id=0, has_side_effects=True, vmem_limit_bytes=62 * 2**20
        ),
    )(fmap2, queries, owner, target_tile)
    spots = row_count * plane_count * pairs
    group = 8 // LEVELS
    joined = pl.pallas_call(
        functools.partial(join_kernel, group),
        out_shape=jax.ShapeDtypeStruct(
            (window_cells, block_count // 2 * LEVELS, 2 * block_cells), jnp.float32
        ),
        grid=(block_count // 2 // group,),
        in_specs=[
            pl.BlockSpec(memory_space=pltpu.SMEM),
            pl.BlockSpec((LEVELS, spots, padded_rows, 2 * block_cells), lambda g: (0, 0, 0, 0)),
        ],
        out_specs=pl.BlockSpec(
            (window_cells, group * LEVELS, 2 * block_cells), lambda g: (0, g, 0)
        ),
    )(index, replies.reshape(LEVELS, spots, padded_rows, 2 * block_cells))
    joined = joined.reshape(window_cells, block_count // 2, LEVELS, 2 * block_cells)
    return joined.transpose(2, 0, 1, 3).reshape(LEVELS, window_cells, block_count * block_cells)


def solution(mesh):
    in_specs = (
        P(None, "rows", "cols", None),
        P(None, "rows", "cols", None),
        P(None, ("rows", "cols"), None),
        P(None, ("rows", "cols")),
    )
    out_specs = P(None, None, ("rows", "cols"))
    chosen_body = gathered_body if mesh.shape["rows"] == 8 else body
    return jax.shard_map(
        chosen_body, mesh=mesh, in_specs=in_specs, out_specs=out_specs, check_vma=False
    )
```

```python
import functools

import jax
import jax.numpy as jnp
from jax import lax
from jax.experimental import pallas as pl
from jax.experimental.pallas import tpu as pltpu
from jax.sharding import PartitionSpec as P

RADIUS = 4
LEVELS = 2
STEP_SLOTS = 16


def padded_2(block, sides, width):
    for axis, dim in sides:
        count = lax.axis_size(axis)
        forward = [(i, i + 1) for i in range(count - 1)]
        backward = [(target, source) for source, target in forward]
        low = lax.ppermute(
            lax.slice_in_dim(block, block.shape[dim] - width, None, axis=dim), axis, forward
        )
        high = lax.ppermute(lax.slice_in_dim(block, 0, width, axis=dim), axis, backward)
        block = jnp.concatenate([low, block, high], axis=dim)
    return block


def pool_level(level_map):
    frame_count, rows_in, cols_in, channels = level_map.shape
    pooled = level_map.astype(jnp.float32).reshape(
        frame_count, rows_in // 2, 2, cols_in // 2, 2, channels
    )
    return jnp.mean(pooled, axis=(2, 4)).astype(jnp.bfloat16)


def dispatch_kernel(slot_count, block_ref, query_ref, sent_ref):
    base = pl.program_id(0) * slot_count
    for slot in range(slot_count):
        sent_ref[slot] = query_ref[block_ref[base + slot]]


def correlate_kernel(plan, scale, label_ref, query_ref, map_ref, reply_ref):
    per_frame, col_count, padded_rows, across = plan
    tile_side = 2 * RADIUS
    span_side = 4 * RADIUS
    window_side = 2 * RADIUS + 1
    block_cells = tile_side * tile_side
    base = pl.program_id(0) * STEP_SLOTS
    lane = lax.broadcasted_iota(jnp.int32, (1, 1, 2 * block_cells), 2)
    query_row = lane % block_cells // tile_side
    query_col = lane[0] % tile_side
    is_first = lane[0] < block_cells

    def window(slot):
        label = label_ref[base + slot]
        tile = label % per_frame
        region = label // per_frame
        row = region // col_count * padded_rows + tile // across * tile_side
        col = (region % col_count * across + tile % across) * tile_side
        col = pl.multiple_of(col, tile_side)
        cells = map_ref[pl.ds(row, span_side), pl.ds(col, span_side), :]
        return cells.reshape(span_side * span_side, -1).astype(jnp.bfloat16)

    for pair in range(STEP_SLOTS // 2):
        queries = query_ref[2 * pair : 2 * pair + 2].reshape(2 * block_cells, -1)
        first, second = [
            lax.dot_general(
                window(2 * pair + half),
                queries,
                (((1,), (1,)), ((), ())),
                preferred_element_type=jnp.float32,
            )
            for half in range(2)
        ]
        scores = jnp.where(is_first, first, second)
        scores = scores.reshape(span_side, span_side, 2 * block_cells)
        for bit in (1, 2, 4):
            scores = jnp.where((query_row & bit) != 0, scores[bit:], scores[:-bit])
        flat = scores.reshape(window_side * span_side, 2 * block_cells)
        for bit in (1, 2, 4):
            moved = pltpu.roll(flat, flat.shape[0] - bit, 0)
            flat = jnp.where((query_col & bit) != 0, moved, flat)
        flat = flat * scale
        for a in range(window_side):
            at = (pair * window_side + a) * window_side
            reply_ref[at : at + window_side, :] = flat[
                a * span_side : a * span_side + window_side
            ]


def assemble_kernel(pair_count, source_ref, half_ref, *refs):
    reply_refs, out_ref = refs[:-1], refs[-1]
    window_cells, lanes = out_ref.shape[1], reply_refs[0].shape[1]
    is_first = lax.broadcasted_iota(jnp.int32, (window_cells, lanes), 1) < lanes // 2
    for level in range(LEVELS):

        def step(m, carry, level=level):
            at = 2 * (level * pair_count + m)
            picked = []
            for side in range(2):
                first_row = source_ref[at + side] * window_cells
                rows = reply_refs[level][pl.ds(first_row, window_cells), :]
                moved = pltpu.roll(rows, lanes // 2, 1)
                picked.append(jnp.where(half_ref[at + side] == side, rows, moved))
            spot = pl.ds(pl.multiple_of(m * lanes, lanes), lanes)
            out_ref[level, :, spot] = jnp.where(is_first, picked[0], picked[1])
            return carry

        lax.fori_loop(0, pair_count, step, 0)


def body(fmap1, fmap2, target_owner, target_tile):
    tile_side = 2 * RADIUS
    window_side = 2 * RADIUS + 1
    block_cells = tile_side * tile_side
    frame_count, band_rows, band_cols, channels = fmap1.shape
    row_count = lax.axis_size("rows")
    col_count = lax.axis_size("cols")
    device_count = row_count * col_count
    tiles_across = band_cols // tile_side
    per_frame = band_rows // tile_side * tiles_across
    block_count = frame_count * per_frame
    owner_slots = max(2, (2 * block_count + device_count - 1) // device_count)
    row_slots = -(-owner_slots * col_count // STEP_SLOTS) * STEP_SLOTS
    pair_slots = row_slots // 2
    queries = fmap1.reshape(
        frame_count, band_rows // tile_side, tile_side, tiles_across, tile_side, channels
    )
    queries = queries.transpose(0, 1, 3, 2, 4, 5).reshape(block_count, block_cells, channels)
    owner_ids = target_owner[:, :, 0]
    owner_rows = owner_ids // col_count
    peer_ids = jnp.arange(row_count, dtype=jnp.int32)
    owner_hits = (owner_rows[:, :, None] == peer_ids[None, None, :]).astype(jnp.int32)
    slot_rank = jnp.sum(owner_hits * (jnp.cumsum(owner_hits, axis=1) - 1), axis=2)
    block_ids = jnp.arange(block_count, dtype=jnp.int32)
    label_rows = []
    for level in range(LEVELS):
        tile_count = (band_rows >> level) // tile_side * ((band_cols >> level) // tile_side)
        regions = block_ids // per_frame * col_count + owner_ids[level] % col_count
        label_rows.append(regions * per_frame + target_tile[level] % tile_count)
    rank_ids = jnp.arange(row_slots, dtype=jnp.int32)
    rank_hits = (slot_rank[:, :, None] == rank_ids[None, None, :]).astype(jnp.int32)
    slot_hits = owner_hits[:, :, :, None] * rank_hits[:, :, None, :]

    def by_slot(values):
        table = jnp.sum(slot_hits * values[:, :, None, None], axis=1)
        return table.transpose(1, 0, 2)

    labels_sent = by_slot(jnp.stack(label_rows))
    blocks_sent = by_slot(jnp.broadcast_to(block_ids[None], owner_ids.shape))
    slot_block = (row_slots, block_cells, channels)
    slot_total = row_count * row_slots
    label_part = lax.all_to_all(labels_sent, "rows", split_axis=0, concat_axis=0, tiled=True)
    levels = [fmap2]
    for level in range(1, LEVELS):
        levels.append(pool_level(levels[-1]))
    window_cells = window_side * window_side
    step_block = (STEP_SLOTS, block_cells, channels)
    reply_block = (STEP_SLOTS // 2 * window_cells, 2 * block_cells)
    reply_tables = [None] * LEVELS
    earlier = None
    for level in reversed(range(LEVELS)):
        queries_sent = pl.pallas_call(
            functools.partial(dispatch_kernel, row_slots),
            out_shape=jax.ShapeDtypeStruct((slot_total,) + slot_block[1:], jnp.bfloat16),
            grid_spec=pltpu.PrefetchScalarGridSpec(
                num_scalar_prefetch=1,
                grid=(row_count,),
                in_specs=[pl.BlockSpec(queries.shape, lambda d, *_: (0, 0, 0))],
                out_specs=pl.BlockSpec(slot_block, lambda d, *_: (d, 0, 0)),
            ),
        )(blocks_sent[:, level].reshape(-1), queries)
        query_part = lax.all_to_all(
            queries_sent.reshape((row_count,) + slot_block),
            "rows",
            split_axis=0,
            concat_axis=0,
            tiled=True,
        )
        band = lax.all_gather(levels[level], "cols", axis=2, tiled=True)
        if earlier is not None:
            band = lax.optimization_barrier((band, earlier, query_part))[0]
        padded = padded_2(band, (("rows", 1),), RADIUS).astype(jnp.float32)
        padded = jnp.pad(padded, ((0, 0), (0, 0), (RADIUS, RADIUS), (0, 0)))
        level_map = padded.reshape((-1,) + padded.shape[2:])
        plan = (per_frame, col_count, padded.shape[1], levels[level].shape[2] // tile_side)
        replies = pl.pallas_call(
            functools.partial(correlate_kernel, plan, channels ** (-0.5)),
            out_shape=jax.ShapeDtypeStruct(
                (row_count * pair_slots * window_cells, 2 * block_cells), jnp.float32
            ),
            grid_spec=pltpu.PrefetchScalarGridSpec(
                num_scalar_prefetch=1,
                grid=(slot_total // STEP_SLOTS,),
                in_specs=[
                    pl.BlockSpec(step_block, lambda d, *_: (d, 0, 0)),
                    pl.BlockSpec(
                        level_map.shape, lambda d, *_: (0, 0, 0), pipeline_mode=pl.Buffered(1)
                    ),
                ],
                out_specs=pl.BlockSpec(reply_block, lambda d, *_: (d, 0)),
            ),
        )(
            label_part[:, level].reshape(-1),
            query_part.reshape((slot_total,) + slot_block[1:]),
            level_map,
        )
        returned = lax.all_to_all(
            replies.reshape(row_count, pair_slots * window_cells, 2 * block_cells),
            "rows",
            split_axis=0,
            concat_axis=0,
            tiled=True,
        )
        earlier = returned
        reply_tables[level] = returned.reshape(-1, 2 * block_cells)
    source_ids = owner_rows * pair_slots + slot_rank // 2
    return pl.pallas_call(
        functools.partial(assemble_kernel, block_count // 2),
        out_shape=jax.ShapeDtypeStruct(
            (LEVELS, window_cells, block_count * block_cells), jnp.float32
        ),
        in_specs=[
            pl.BlockSpec(memory_space=pltpu.SMEM),
            pl.BlockSpec(memory_space=pltpu.SMEM),
        ]
        + [pl.BlockSpec(memory_space=pltpu.VMEM)] * LEVELS,
        out_specs=pl.BlockSpec(memory_space=pltpu.VMEM),
    )(source_ids.reshape(-1), (slot_rank % 2).reshape(-1), *reply_tables)


MESH = pl.DeviceIdType.MESH
TOP = 32000.0


def flipped(index, bit):
    return index + bit - 2 * bit * (index // bit % 2)


def lookup_kernel(
    plan,
    f2_hbm,
    q_hbm,
    owner_ref,
    tile_ref,
    rep_out,
    idx_out,
    f2x,
    f1a,
    tab_made,
    tabv,
    tabs,
    map0,
    map1,
    p1x,
    tmp,
    line,
    reps,
    loc_sem,
    zs_sem,
    zr_sem,
    hs_sem,
    hr_sem,
    fs_sem,
    fr_sem,
    ts_sem,
    tr_sem,
    tl_sem,
    rs_sem,
    rr_sem,
):
    row_count, plane_count, slots, scale = plan
    frame_count, band_rows, band_cols, channels = f2_hbm.shape
    side = 2 * RADIUS
    subs, across = band_rows // side, band_cols // side
    per_frame = subs * across
    block_count, block_cells = frame_count * per_frame, side * side
    span = 4 * RADIUS
    wside = 2 * RADIUS + 1
    wide = 2 * side
    strips = band_cols // wide
    half_blocks = block_count // 2
    r = lax.axis_index("rows")
    c = lax.axis_index("cols")
    last_r, last_c = row_count - 1, plane_count - 1

    barrier = pltpu.get_barrier_semaphore()
    for k in range(1, row_count):
        pl.semaphore_signal(
            barrier, inc=1, device_id=((r + k) % row_count, c), device_id_type=MESH
        )

    @pl.when(c > 0)
    def _():
        pl.semaphore_signal(barrier, inc=1, device_id=(r, c - 1), device_id_type=MESH)

    @pl.when(c < last_c)
    def _():
        pl.semaphore_signal(barrier, inc=1, device_id=(r, c + 1), device_id_type=MESH)

    has_left = jnp.where(c > 0, 1, 0)
    has_right = jnp.where(c < last_c, 1, 0)
    pl.semaphore_wait(barrier, row_count - 1 + has_left + has_right)

    def strip(at, way):
        p = at + way * (strips - 1 - 2 * at)
        return p, pl.ds(pl.multiple_of(p * wide, wide), wide)

    whole_strip = (0, band_rows)
    last_pieces = [
        (strips - 1, (0, side)),
        (strips, (band_rows - side, side)),
        (strips + 1, (side, band_rows - 2 * side)),
    ]

    def z_copy(b, number, way, rows=whole_strip, own=False):
        _, cols = strip(number if rows == whole_strip else strips - 1, way)
        first, count = rows
        here = f2x.at[b, :, pl.ds(side + first, count), cols]
        return pltpu.make_async_remote_copy(
            src_ref=f2_hbm.at[:, pl.ds(first, count), cols] if own else here,
            dst_ref=here,
            send_sem=zs_sem.at[way, b, number],
            recv_sem=zr_sem.at[b, number],
            device_id=(r, c - 1 + 2 * way),
            device_id_type=MESH,
        )

    def halo_copy(b, at, way, up, own=False):
        _, cols = strip(at, way)
        first = 0 if up else band_rows - side
        into = band_rows + side if up else 0
        if own:
            source = f2_hbm.at[:, pl.ds(first, side), cols]
        else:
            source = f2x.at[b, :, pl.ds(first + side, side), cols]
        lane = 0 if up else 1
        return pltpu.make_async_remote_copy(
            src_ref=source,
            dst_ref=f2x.at[b, :, pl.ds(into, side), cols],
            send_sem=hs_sem.at[lane, b, at],
            recv_sem=hr_sem.at[lane, b, at],
            device_id=(r - 1 if up else r + 1, c),
            device_id_type=MESH,
        )

    def send_halo(b, at, way, up, own=False):
        @pl.when(r > 0 if up else r < last_r)
        def _():
            halo_copy(b, at, way, up, own).start()

    def goes_on(way):
        return (c - 1 + 2 * way >= 0) & (c - 1 + 2 * way <= last_c)

    def f1_copy(index, row, half, bit):
        part = pl.ds(half * half_blocks, half_blocks)
        return pltpu.make_async_remote_copy(
            src_ref=f1a.at[row, part],
            dst_ref=f1a.at[row, part],
            send_sem=fs_sem.at[index],
            recv_sem=fr_sem.at[row, half],
            device_id=(flipped(r, bit), c),
            device_id_type=MESH,
        )

    def tab_copy(k):
        return pltpu.make_async_remote_copy(
            src_ref=tab_made.at[(r + k) % row_count],
            dst_ref=tabv.at[r],
            send_sem=ts_sem.at[k],
            recv_sem=tr_sem.at[k],
            device_id=((r + k) % row_count, c),
            device_id_type=MESH,
        )

    def rep_copy(b, k):
        s = (r + k) % row_count
        return pltpu.make_async_remote_copy(
            src_ref=reps.at[b, s],
            dst_ref=rep_out.at[:, r, b],
            send_sem=rs_sem.at[b, k],
            recv_sem=rr_sem.at[b, k],
            device_id=(s, c),
            device_id_type=MESH,
        )

    def rep_local(b):
        return pltpu.make_async_copy(reps.at[b, r], rep_out.at[:, r, b], rs_sem.at[b, 0])

    x_row, y_row, d_row = flipped(r, 2), flipped(r, 4), flipped(flipped(r, 2), 4)
    f1_first = [(0, r, 0, 2), (1, r, 0, 4), (2, r, 1, 2), (3, r, 1, 4), (4, r, 0, 1), (5, r, 1, 1)]
    f1_second = [
        (6, x_row, 0, 4),
        (7, y_row, 1, 2),
        (8, x_row, 0, 1),
        (9, x_row, 1, 1),
        (10, y_row, 0, 1),
        (11, y_row, 1, 1),
    ]
    f1_third = [(12, d_row, 0, 1), (13, d_row, 1, 1)]

    def whole_part(values, unit):
        return jnp.floor((values + 0.5) * (1.0 / unit))

    def make_tables():
        ids = lax.broadcasted_iota(jnp.int32, (block_count, block_count), 0).astype(jnp.float32)
        lanes = lax.broadcasted_iota(jnp.int32, (block_count, block_count), 1).astype(jnp.float32)
        block = lanes[:1]
        spots = lax.broadcasted_iota(
            jnp.int32, (block_count, tab_made.shape[2]), 1
        ).astype(jnp.float32)
        peers = lax.broadcasted_iota(jnp.int32, (row_count, block_count), 0).astype(jnp.float32)

        def upright(line_values):
            return jnp.sum(jnp.where(ids == lanes, line_values, 0.0), axis=1, keepdims=True)

        tab_made[...] = jnp.zeros(tab_made.shape, tab_made.dtype)
        idx_out[...] = jnp.zeros(idx_out.shape, idx_out.dtype)
        totals = [0.0, 0.0, 0.0]
        for level in range(LEVELS):
            owner = owner_ref[level].astype(jnp.float32)
            tile = tile_ref[level : level + 1].astype(jnp.float32)
            level_across = across >> level
            tiles = (subs >> level) * level_across
            tile = tile - whole_part(tile, tiles) * tiles
            tile_row = whole_part(tile, level_across)
            same = jnp.where((upright(owner) == owner) & (ids < lanes), 1.0, 0.0)
            rank = jnp.sum(same, axis=0, keepdims=True)
            towards = whole_part(owner, plane_count)
            plane = owner - towards * plane_count
            place = (plane * LEVELS + level) * slots + rank
            map_rows = (band_rows >> level) + side
            values = [
                block,
                whole_part(block, per_frame) * map_rows + tile_row * side,
                tile - tile_row * level_across,
            ]
            place = jnp.where(rank < slots, place, -1.0)
            chosen = jnp.where(upright(place) == spots, 1.0, 0.0).astype(jnp.bfloat16)
            for at, value in enumerate(values):
                named = jnp.where(peers == towards, value, 0.0).astype(jnp.bfloat16)
                totals[at] += jnp.dot(named, chosen, preferred_element_type=jnp.float32)
            rank = jnp.minimum(rank, slots - 1.0)
            pair = whole_part(rank, 2)
            source = (owner * (slots // 2) + pair).astype(jnp.int32)
            idx_out[level : level + 1, :block_count] = source
            half = (rank - 2 * pair).astype(jnp.int32)
            idx_out[LEVELS + level : LEVELS + level + 1, :block_count] = half
        for at, total in enumerate(totals):
            total = total.astype(jnp.int32)
            for peer in range(row_count):
                tab_made[peer, at : at + 1, :] = total[peer : peer + 1]

    loc_f2 = pltpu.make_async_copy(f2_hbm, f2x.at[c, :, pl.ds(side, band_rows)], loc_sem.at[0])
    loc_tab = pltpu.make_async_copy(tab_made.at[r], tabv.at[r], loc_sem.at[2])

    def loc_q(k):
        f, at = k // per_frame, k % per_frame
        cut = q_hbm.at[f, at // across, :, at % across]
        return pltpu.make_async_copy(cut, f1a.at[r, k], loc_sem.at[1])

    def start_q(k, carry):
        loc_q(k).start()
        return carry

    for way in range(2):

        @pl.when(goes_on(way))
        def _():
            for at in range(strips - 1):
                z_copy(c, at, way, own=True).start()
            for number, rows in last_pieces:
                z_copy(c, number, way, rows, own=True).start()

    lax.fori_loop(0, block_count, start_q, 0)
    loc_f2.start()
    make_tables()
    pltpu.make_async_copy(f1a.at[r], f1a.at[r], loc_sem.at[1]).wait()
    for item in f1_first:
        f1_copy(*item).start()
    for at in range(strips):
        send_halo(c, at, 0, True, own=True)
        send_halo(c, at, 0, False, own=True)
    for k in range(1, row_count):
        tab_copy(k).start()
    loc_tab.start()

    @pl.when(r == 0)
    def _():
        f2x[:, :, 0:side] = jnp.zeros((plane_count, frame_count, side) + f2x.shape[3:], f2x.dtype)

    @pl.when(r == last_r)
    def _():
        f2x[:, :, band_rows + side :] = jnp.zeros(
            (plane_count, frame_count, side) + f2x.shape[3:], f2x.dtype
        )

    def each_side(step, act):
        def one(way, carry):
            b = c + step * (1 - 2 * way)

            @pl.when((b >= 0) & (b <= last_c))
            def _():
                act(b, way)

            return carry

        lax.fori_loop(0, jnp.where(step > 0, 2, 1), one, 0)

    def take(step, at, halo=True):
        def act(b, way):
            z_copy(b, at, way).wait_recv()

            @pl.when(goes_on(way))
            def _():
                z_copy(b, at, way).start()

            if halo:
                send_halo(b, at, way, True)
                send_halo(b, at, way, False)

        each_side(step, act)

    def take_last(step, halo=True):
        def act(b, way):
            for place, (number, rows) in enumerate(last_pieces):
                z_copy(b, number, way, rows).wait_recv()

                @pl.when(goes_on(way))
                def _():
                    z_copy(b, number, way, rows).start()

                if halo and place < 2:
                    send_halo(b, strips - 1, way, place == 0)

        each_side(step, act)

    def take_some(step, low, high, halo=True):
        def one(at, carry):
            take(step, at, halo)
            return carry

        lax.fori_loop(low, high, one, 0)

    def pool(step, low, high):
        def act(b, way):
            def strip_pool(at, carry):
                @pl.when(r > 0)
                def _():
                    halo_copy(b, at, way, False).wait_recv()

                @pl.when(r < last_r)
                def _():
                    halo_copy(b, at, way, True).wait_recv()

                rows = p1x.shape[2]
                p, cols = strip(at, way)
                half_cols = pl.ds(pl.multiple_of(p * side, side), side)

                def pool_row(t, inner):
                    f, i = t // rows, t % rows
                    pair = f2x[b, f, pl.ds(2 * i, 2), cols].astype(jnp.float32)
                    both = pair[0] + pair[1]
                    for lane in range(channels // 128):
                        tmp[lane, pl.ds(i * wide, wide), :] = both[:, lane * 128 : (lane + 1) * 128]
                    for lane in range(channels // 128):
                        even = tmp[lane, pl.ds(i * wide, side, stride=2), :]
                        odd = tmp[lane, pl.ds(i * wide + 1, side, stride=2), :]
                        p1x[b, f, i, half_cols, lane * 128 : (lane + 1) * 128] = (even + odd) * 0.25
                    return inner

                lax.fori_loop(0, frame_count * rows, pool_row, 0, unroll=4)
                return carry

            lax.fori_loop(low, high, strip_pool, 0)

        each_side(step, act)

    lane_id = lax.broadcasted_iota(jnp.int32, (1, 1, 2 * block_cells), 2)
    query_row = lane_id % block_cells // side
    query_col = lane_id[0] % side
    is_first = lane_id[0] < block_cells
    row_id = lax.broadcasted_iota(jnp.int32, line.shape[2:], 0)
    line[...] = jnp.zeros(line.shape, line.dtype)

    def build(b, level):
        into = (map0, map1)[level]
        width = band_cols >> level
        rows = into.shape[0] // frame_count
        left_b, right_b = jnp.maximum(b - 1, 0), jnp.minimum(b + 1, last_c)

        def build_row(t, carry):
            f, y = t // rows, t % rows
            if level == 0:
                at = y + RADIUS
                left = f2x[left_b, f, at, width - 2 * side :, :].astype(jnp.float32)[side:]
                middle = f2x[b, f, at].astype(jnp.float32)
                right = f2x[right_b, f, at, : 2 * side, :].astype(jnp.float32)[:side]
            else:
                left = p1x[left_b, f, y, width - side :, :]
                middle = p1x[b, f, y]
                right = p1x[right_b, f, y, :side, :]
            left = jnp.where(b > 0, left, 0.0)
            right = jnp.where(b < last_c, right, 0.0)
            whole = jnp.concatenate([left, middle, right], axis=0)
            whole = pltpu.roll(whole, whole.shape[0] - RADIUS, 0)
            into[t] = whole[: width + side].reshape(into.shape[1:])
            return carry

        lax.fori_loop(0, into.shape[0], build_row, 0, unroll=4)

    def score_pair(b, s, level, pair):
        from_map = (map0, map1)[level]
        windows, queries = [], []
        for half in range(2):
            at = (b * LEVELS + level) * slots + 2 * pair + half
            k, row = jnp.clip(tabs[s, 0, at], 0, block_count - 1), jnp.clip(tabs[s, 1, at], 0, from_map.shape[0] - span)
            cells = from_map[pl.ds(row, span), pl.ds(jnp.clip(tabs[s, 2, at], 0, from_map.shape[1] - 2), 2)]
            windows.append(cells.reshape(span * span, channels).astype(jnp.bfloat16))
            queries.append(f1a[s, k].reshape(block_cells, channels))
        queries = jnp.concatenate(queries, axis=0)
        first, second = [
            lax.dot_general(
                window, queries, (((1,), (1,)), ((), ())), preferred_element_type=jnp.float32
            )
            for window in windows
        ]
        scores = jnp.where(is_first, first, second).reshape(span, span, 2 * block_cells)
        for bit in (1, 2, 4):
            scores = jnp.where((query_row & bit) != 0, scores[bit:], scores[:-bit])
        flat = scores.reshape(wside * span, 2 * block_cells)
        for bit in (1, 2, 4):
            moved = pltpu.roll(flat, flat.shape[0] - bit, 0)
            flat = jnp.where((query_col & bit) != 0, moved, flat)
        flat = flat * scale
        for a in range(wside):
            line[level, pair, a * wside : (a + 1) * wside, :] = flat[a * span : a * span + wside]
        found = line[level, pair]
        top = jnp.max(jnp.abs(found), axis=0, keepdims=True)
        power = jnp.maximum(jnp.ceil(jnp.log2(top)), -100.0)
        coded = jnp.floor(found * (TOP * jnp.exp2(-power)) + 0.5)
        coded = jnp.where(row_id == wside * wside, power, coded)
        reps[b, s, level, pair] = coded.astype(jnp.int32).astype(jnp.int16)

    def process(b, way):
        for level in range(LEVELS):
            build(b, level)

        def source(j, inner):
            flips = (1 - j // 4, (j // 2 + j // 4) % 2, (j + j // 6) % 2)
            s = r
            for flip, bit in zip(flips, (2, 4, 1), strict=True):
                s = s + flip * (bit - 2 * bit * (r // bit % 2))
            k = (s - r + row_count) % row_count
            for level in range(LEVELS):
                for pair in range(slots // 2):
                    score_pair(b, s, level, pair)

            @pl.when(k == 0)
            def _():
                rep_local(b).start()

            @pl.when(k > 0)
            def _():
                rep_copy(b, k).start()

            return inner

        lax.fori_loop(0, row_count, source, 0)

    take_some(1, 0, strips - 1, False)
    take_last(1, False)
    for item in f1_second:
        index, row, half, bit = item
        if index in (6, 7, 9, 10):
            f1_copy(*item).wait_recv()
        f1_copy(*item).start()

    def first_halos(at, carry):
        def act(b, way):
            send_halo(b, at, way, True)
            send_halo(b, at, way, False)

        each_side(1, act)
        return carry

    lax.fori_loop(0, strips, first_halos, 0)
    if last_c >= 2:
        take_some(2, 0, strips - 1)
    for item in f1_third:
        f1_copy(*item).wait_recv()
        f1_copy(*item).start()
    for bits in ((1,), (1, 2), (1, 4), (1, 2, 4)):
        row = r
        for bit in bits:
            row = flipped(row, bit)
        for half in range(2):
            f1_copy(0, row, half, 1).wait_recv()
    for k in range(1, row_count):
        tab_copy(k).wait_recv()
    loc_tab.wait()
    loc_f2.wait()
    tab_smem = pltpu.make_async_copy(tabv, tabs, tl_sem)
    tab_smem.start()
    tab_smem.wait()
    def stage(step, carry):
        @pl.when(step == 1)
        def _():
            take_last(jnp.int32(2))

        @pl.when(step > 2)
        def _():
            take_some(step, 1, strips - 1)
            pool(step, 1, strips - 1)
            take_last(step)

        @pl.when(step >= 2)
        def _():
            take(step + 1, 0)

        low = jnp.where(step == 0, 0, jnp.where(step > 2, strips - 1, 1))
        pool(step, low, strips)
        pool(step + 1, 0, 1)
        each_side(step, process)
        return carry

    lax.fori_loop(0, last_c + 1, stage, 0)

    def all_sent(b, way):
        @pl.when(goes_on(way))
        def _():
            for at in range(strips - 1):
                z_copy(b, at, way).wait_send()
            for number, rows in last_pieces:
                z_copy(b, number, way, rows).wait_send()

    def halos_sent(b, way):
        for at in range(strips):

            @pl.when(r > 0)
            def _():
                halo_copy(b, at, way, True).wait_send()

            @pl.when(r < last_r)
            def _():
                halo_copy(b, at, way, False).wait_send()

    def step_sent(step, carry):
        each_side(step, all_sent)
        each_side(step, halos_sent)
        return carry

    all_sent(c, 1)
    lax.fori_loop(0, last_c + 1, step_sent, 0)

    def plane_end(b, carry):
        rep_local(b).wait()

        def peer_end(k, inner):
            rep_copy(b, k).wait_send()
            rep_copy(b, k).wait_recv()
            return inner

        lax.fori_loop(1, row_count, peer_end, 0)
        return carry

    lax.fori_loop(0, plane_count, plane_end, 0)
    for item in f1_first + f1_second + f1_third:
        f1_copy(*item).wait_send()
    for k in range(1, row_count):
        tab_copy(k).wait_send()


def join_kernel(group, index_ref, reply_ref, out_ref):
    window_cells = out_ref.shape[0]
    padded_rows, lanes = reply_ref.shape[-2:]
    is_first = lax.broadcasted_iota(jnp.int32, (padded_rows, lanes), 1) < lanes // 2
    base = pl.program_id(0) * group * 2
    for m in range(group):
        for level in range(LEVELS):
            picked = []
            for side in range(2):
                at = base + 2 * m + side
                rows = reply_ref[level, index_ref[level, at]].astype(jnp.int32)
                turn = (index_ref[LEVELS + level, at] + side) % 2 * (lanes // 2)
                picked.append(pltpu.roll(rows.astype(jnp.float32), turn, 1))
            both = jnp.where(is_first, picked[0], picked[1])
            unit = jnp.exp2(both[window_cells : window_cells + 1]) * (1.0 / TOP)
            out_ref[:, m * LEVELS + level, :] = both[:window_cells] * unit


def gathered_body(fmap1, fmap2, target_owner, target_tile):
    side = 2 * RADIUS
    window_cells = (2 * RADIUS + 1) ** 2
    frame_count, band_rows, band_cols, channels = fmap1.shape
    row_count = lax.axis_size("rows")
    plane_count = lax.axis_size("cols")
    device_count = row_count * plane_count
    subs, across = band_rows // side, band_cols // side
    per_frame = subs * across
    block_count = frame_count * per_frame
    block_cells = side * side
    slots = max(2, (2 * block_count + device_count - 1) // device_count)
    queries = fmap1.reshape(frame_count, subs, side, across, side, channels)
    owner = target_owner.transpose(0, 2, 1)
    lanes_used = -(-plane_count * LEVELS * slots // 128) * 128
    table = (row_count, 8, lanes_used)
    padded_rows = -(-(window_cells + 1) // 8) * 8
    pairs = slots // 2
    strips = across // 2
    reply_shape = (LEVELS, row_count, plane_count, pairs, padded_rows, 2 * block_cells)
    ext_rows = band_rows + 2 * side
    dma = pltpu.SemaphoreType.DMA
    replies, index = pl.pallas_call(
        functools.partial(lookup_kernel, (row_count, plane_count, slots, channels**-0.5)),
        out_shape=[
            jax.ShapeDtypeStruct(reply_shape, jnp.int16),
            jax.ShapeDtypeStruct((8, 128), jnp.int32),
        ],
        in_specs=[pl.BlockSpec(memory_space=pl.ANY)] * 2
        + [pl.BlockSpec(memory_space=pltpu.VMEM)] * 2,
        out_specs=[
            pl.BlockSpec(memory_space=pl.ANY),
            pl.BlockSpec(memory_space=pltpu.VMEM),
        ],
        scratch_shapes=[
            pltpu.VMEM((plane_count, frame_count, ext_rows, band_cols, channels), jnp.bfloat16),
            pltpu.VMEM((row_count, block_count, side, side, channels), jnp.bfloat16),
            pltpu.VMEM(table, jnp.int32),
            pltpu.VMEM(table, jnp.int32),
            pltpu.SMEM(table, jnp.int32),
            pltpu.VMEM((frame_count * (band_rows + side), across + 1, side, channels), jnp.float32),
            pltpu.VMEM(
                (frame_count * (band_rows // 2 + side), across // 2 + 1, side, channels),
                jnp.float32,
            ),
            pltpu.VMEM(
                (plane_count, frame_count, ext_rows // 2, band_cols // 2, channels), jnp.float32
            ),
            pltpu.VMEM((channels // 128, ext_rows // 2 * 2 * side, 128), jnp.float32),
            pltpu.VMEM((LEVELS, pairs, padded_rows, 2 * block_cells), jnp.float32),
            pltpu.VMEM(
                (plane_count, row_count, LEVELS, pairs, padded_rows, 2 * block_cells), jnp.int16
            ),
            dma((3,)),
            dma((2, plane_count, strips + 2)),
            dma((plane_count, strips + 2)),
            dma((2, plane_count, strips)),
            dma((2, plane_count, strips)),
            dma((14,)),
            dma((row_count, 2)),
            dma((row_count,)),
            dma((row_count,)),
            dma,
            dma((plane_count, row_count)),
            dma((plane_count, row_count)),
        ],
        compiler_params=pltpu.CompilerParams(
            collective_id=0, has_side_effects=True, vmem_limit_bytes=62 * 2**20
        ),
    )(fmap2, queries, owner, target_tile)
    spots = row_count * plane_count * pairs
    group = 8 // LEVELS
    joined = pl.pallas_call(
        functools.partial(join_kernel, group),
        out_shape=jax.ShapeDtypeStruct(
            (window_cells, block_count // 2 * LEVELS, 2 * block_cells), jnp.float32
        ),
        grid=(block_count // 2 // group,),
        in_specs=[
            pl.BlockSpec(memory_space=pltpu.SMEM),
            pl.BlockSpec((LEVELS, spots, padded_rows, 2 * block_cells), lambda g: (0, 0, 0, 0)),
        ],
        out_specs=pl.BlockSpec(
            (window_cells, group * LEVELS, 2 * block_cells), lambda g: (0, g, 0)
        ),
    )(index, replies.reshape(LEVELS, spots, padded_rows, 2 * block_cells))
    joined = joined.reshape(window_cells, block_count // 2, LEVELS, 2 * block_cells)
    return joined.transpose(2, 0, 1, 3).reshape(LEVELS, window_cells, block_count * block_cells)


def solution(mesh):
    in_specs = (
        P(None, "rows", "cols", None),
        P(None, "rows", "cols", None),
        P(None, ("rows", "cols"), None),
        P(None, ("rows", "cols")),
    )
    out_specs = P(None, None, ("rows", "cols"))
    chosen_body = gathered_body if mesh.shape["rows"] == 8 else body
    return jax.shard_map(
        chosen_body, mesh=mesh, in_specs=in_specs, out_specs=out_specs, check_vma=False
    )
```
